256 devices in a mesh: gz: 2 (over core), gx: 8 (over y, x_hi), gy: 16 (over z, x_lo).
Axes of the slice: x: 4 (x_hi: 2, x_lo: 2; x = x_hi * 2 + x_lo), y: 4, z: 8, core: 2. Of those that a mesh axis runs over, the one named last changes fastest.
Arguments:
- queries: bfloat16 [2, 16384, 128], P('gz', 'gx'), may hold values from -6 to 6
- keys: bfloat16 [2, 16384, 128], P('gz', 'gy'), may hold values from -6 to 6
- values: bfloat16 [2, 16384, 128], P('gz', 'gy'), may hold values from -6 to 6
- w_out: bfloat16 [256, 2048], replicated, may hold values from -0.375 to 0.375
Outputs:
- mixed: bfloat16 [16384, 2048], P(('gx', 'gy'), 'gz')
The draws below stay inside these ranges and needn't reach their ends.
All inputs are finite; a program needn't handle non-finite values.
Results may differ from the reference program's by a relative error of at most 0.02.
Values may be sent and summed in bfloat16 or wider, within the bound.
A program may use at most 64 MiB of HBM per device.

```python
import math
import jax
import jax.numpy as jnp
from jax import lax

HEAD_DIM = 128
D = 2048
SWEEPS = 3
HEADS = 2
SEQ = 16384


def base_draw(key):
    return jnp.clip(1.75 * jax.random.normal(key, (HEADS, SEQ, HEAD_DIM), jnp.float32), -6.0, 6.0)


def draw_queries(key, part):
    result = base_draw(jax.random.fold_in(key, 1))
    return result.astype(jnp.bfloat16)


def draw_keys(key, part):
    result = base_draw(jax.random.fold_in(key, 2))
    return result.astype(jnp.bfloat16)


def level_of(stream_key, shape, cuts, smallest, largest):
    gain, own = 1.0, jax.random.fold_in(stream_key, 6)
    for position, parts in cuts:
        heights = jnp.exp(jax.random.uniform(jax.random.fold_in(own, position), (parts,), jnp.float32, smallest / len(cuts), largest / len(cuts)))
        gain = gain * jnp.repeat(heights, shape[position] // parts).reshape([-1 if axis == position else 1 for axis in range(len(shape))])
    return gain


def centred(own_key, extent, deviation, most, pieces=(), kind=jnp.bfloat16):
    gain = level_of(own_key, extent, pieces, -0.22, 0.18) if pieces else 1.0
    drawn = jax.random.normal(own_key, extent, jnp.float32) * deviation * gain
    return jnp.minimum(jnp.maximum(drawn, -most), most).astype(kind)


def setup_inputs(seed: int = 0) -> dict:
    arg_keys = jax.random.split(jax.random.key(seed), 5)
    queries = draw_queries(jax.random.fold_in(arg_keys[4], 71), 0)
    keys = draw_keys(jax.random.fold_in(arg_keys[4], 71), 0)
    values = centred(arg_keys[2], (HEADS, SEQ, HEAD_DIM), 1.0, 6.0, ((0, 2), (1, 16)))
    w_out = centred(arg_keys[3], (HEADS * HEAD_DIM, D), (HEADS * HEAD_DIM) ** -0.5, 0.375)
    return {"queries": queries, "keys": keys, "values": values, "w_out": w_out}


def log_total(shifted, along):
    biggest = lax.optimization_barrier(jnp.max(shifted, axis=along, keepdims=True))
    summed = lax.optimization_barrier(jnp.sum(jnp.exp(shifted - biggest), axis=along, keepdims=True))
    return jnp.squeeze(biggest + jnp.log(summed), axis=along)

def one_head(operands):
    query_rows, key_rows, value_rows = operands
    scores = jnp.dot(query_rows, key_rows.T, preferred_element_type=jnp.float32) * (1.0 / math.sqrt(HEAD_DIM))
    col_pot = jnp.zeros((SEQ,), jnp.float32)
    for sweep_index in range(SWEEPS):
        row_pot = -log_total(scores + col_pot[None, :], 1)
        col_pot = -log_total(scores + row_pot[:, None], 0)
    row_pot = -log_total(scores + col_pot[None, :], 1)
    weights = jnp.exp(scores + row_pot[:, None] + col_pot[None, :]).astype(jnp.bfloat16)
    return jnp.dot(weights, value_rows, preferred_element_type=jnp.float32).astype(jnp.bfloat16)

def reference(queries, keys, values, w_out):
    head_out = lax.map(one_head, (queries, keys, values))
    flat_heads = jnp.transpose(head_out, (1, 0, 2)).reshape(SEQ, HEADS * HEAD_DIM)
    return jnp.dot(flat_heads, w_out, preferred_element_type=jnp.float32).astype(jnp.bfloat16)
```

```python
import functools
import math

import jax
import jax.numpy as jnp
from jax import lax
from jax.experimental import pallas as pl
from jax.experimental.pallas import tpu as pltpu
from jax.sharding import PartitionSpec as P

SWEEPS = 3
LANES = 128
MESH = pl.DeviceIdType.MESH
F32 = jnp.float32
BF16 = jnp.bfloat16


def far_first(count):
    return sorted(range(count), key=lambda d: -min(d, count - d))


def split_lhs(x):
    rows = jnp.broadcast_to(x, (16, x.shape[1]))
    hi = rows.astype(BF16).astype(F32)
    rest = rows - hi
    mid = rest.astype(BF16).astype(F32)
    lo = rest - mid
    at = lax.broadcasted_iota(jnp.int32, rows.shape, 0)
    parts = jnp.where(at == 0, hi, jnp.where(at == 1, mid, jnp.where(at == 2, lo, 0.0)))
    return parts.astype(BF16)


def kernel(
    sizes,
    q_hbm,
    k_hbm,
    v_hbm,
    w_hbm,
    out_ref,
    q_ref,
    k_ref,
    v_ref,
    w_ref,
    s_ref,
    f_ref,
    lhs_row,
    lhs_col,
    val_lhs,
    cmax_ref,
    row_send,
    row_recv,
    col_send,
    col_recv,
    row_vec,
    col_vec,
    out_send,
    out_recv,
    head_send,
    head_recv,
    load_sem,
    row_ssem,
    row_rsem,
    col_ssem,
    col_rsem,
    out_ssem,
    out_rsem,
    head_ssem,
    head_rsem,
):
    nx, ny = sizes
    rows, width = q_ref.shape
    cols = k_ref.shape[0]
    row_tiles, col_tiles = rows // LANES, cols // LANES
    nz = ny // 2
    gz, gx, gy = lax.axis_index("gz"), lax.axis_index("gx"), lax.axis_index("gy")
    z, xl = gy // 2, lax.rem(gy, 2)
    y, xh = gx // 2, lax.rem(gx, 2)
    scale = math.log2(math.e) / math.sqrt(width)

    row_peers = [(dz, dx) for dz in far_first(nz) for dx in (1, 0) if (dz, dx) != (0, 0)]
    col_peers = [(dy, dx) for dy in far_first(nx // 2) for dx in (1, 0) if (dy, dx) != (0, 0)]

    def row_peer(dz, dx):
        return lax.rem(z + dz, nz) * 2 + lax.rem(xl + dx, 2)

    def col_peer(dy, dx):
        return lax.rem(y + dy, nx // 2) * 2 + lax.rem(xh + dx, 2)

    mine = w_ref.shape[1]
    loads = [
        pltpu.make_async_copy(q_hbm, q_ref, load_sem.at[0]),
        pltpu.make_async_copy(k_hbm, k_ref, load_sem.at[1]),
        pltpu.make_async_copy(v_hbm, v_ref, load_sem.at[2]),
        pltpu.make_async_copy(
            w_hbm.at[:, pl.ds(pl.multiple_of(gz * mine, LANES), mine)], w_ref, load_sem.at[3]
        ),
    ]
    for load in loads:
        load.start()

    barrier = pltpu.get_barrier_semaphore()
    for dz, dx in row_peers:
        pl.semaphore_signal(
            barrier, inc=1, device_id={"gy": row_peer(dz, dx)}, device_id_type=MESH
        )
    for dy, dx in col_peers:
        pl.semaphore_signal(
            barrier, inc=1, device_id={"gx": col_peer(dy, dx)}, device_id_type=MESH
        )
    pl.semaphore_signal(barrier, inc=1, device_id={"gz": 1 - gz}, device_id_type=MESH)

    def send_rows(turn):
        copies = []
        for dz, dx in row_peers:
            slot = dz * 2 + dx
            copy = pltpu.make_async_remote_copy(
                src_ref=row_send.at[turn],
                dst_ref=row_recv.at[turn, slot],
                send_sem=row_ssem.at[turn, slot],
                recv_sem=row_rsem.at[turn, slot],
                device_id={"gy": row_peer(dz, dx)},
                device_id_type=MESH,
            )
            copy.start()
            copies.append((slot, copy))
        return copies

    def send_cols(turn):
        copies = []
        for dy, dx in col_peers:
            slot = dy * 2 + dx
            copy = pltpu.make_async_remote_copy(
                src_ref=col_send.at[turn],
                dst_ref=col_recv.at[turn, slot],
                send_sem=col_ssem.at[turn, slot],
                recv_sem=col_rsem.at[turn, slot],
                device_id={"gx": col_peer(dy, dx)},
                device_id_type=MESH,
            )
            copy.start()
            copies.append((slot, copy))
        return copies

    def log_total(own, received):
        biggest = own
        for other in received:
            biggest = jnp.maximum(biggest, other)
        total = jnp.exp2(own - biggest)
        for other in received:
            total = total + jnp.exp2(other - biggest)
        return biggest + jnp.log2(total)

    def plain_total(own, received):
        total = own
        for other in received:
            total = total + other
        return total

    started = []

    loads[0].wait()
    loads[1].wait()
    block = min(256, rows)
    for b in range(rows // block):
        lanes = slice(b * block, (b + 1) * block)
        scores = scale * lax.dot_general(
            k_ref[...], q_ref[lanes, :], (((1,), (1,)), ((), ())), preferred_element_type=F32
        )
        s_ref[:, lanes] = scores
        biggest = jnp.max(scores, axis=0, keepdims=True)
        summed = jnp.sum(jnp.exp2(s_ref[:, lanes] - biggest), axis=0, keepdims=True)
        local = biggest + jnp.log2(summed)
        for t in range(block // LANES):
            row_send[0, pl.ds(b * (block // LANES) + t, 1), :] = local[
                :, t * LANES : (t + 1) * LANES
            ]

    pl.semaphore_wait(barrier, len(row_peers) + len(col_peers) + 1)
    copies = send_rows(0)
    started += copies
    for _, copy in copies:
        copy.wait_recv()
    row_vec[...] = -log_total(row_send[0], [row_recv[0, slot] for slot, _ in copies])

    eye = lax.broadcasted_iota(jnp.int32, (LANES, LANES), 0) == lax.broadcasted_iota(
        jnp.int32, (LANES, LANES), 1
    )

    def across(column):
        return jnp.sum(
            jnp.where(eye, jnp.broadcast_to(column, (LANES, LANES)), 0.0), axis=0, keepdims=True
        )

    tiles = [slice(t * LANES, (t + 1) * LANES) for t in range(row_tiles)]
    for jb in range(col_tiles):
        down = slice(jb * LANES, (jb + 1) * LANES)
        biggest = s_ref[down, tiles[0]] + row_vec[0:1, :]
        for t in range(1, row_tiles):
            biggest = jnp.maximum(biggest, s_ref[down, tiles[t]] + row_vec[t : t + 1, :])
        biggest = jnp.max(biggest, axis=1, keepdims=True)
        wide = jnp.broadcast_to(biggest, (LANES, LANES))
        summed = jnp.zeros((LANES, LANES), F32)
        for t in range(row_tiles):
            part = jnp.exp2(s_ref[down, tiles[t]] + row_vec[t : t + 1, :] - wide)
            f_ref[down, tiles[t]] = part.astype(BF16)
            summed = summed + part
        summed = jnp.sum(summed, axis=1, keepdims=True)
        cmax_ref[pl.ds(jb, 1), :] = across(biggest)
        col_send[0, pl.ds(jb, 1), :] = across(biggest + jnp.log2(summed))

    copies = send_cols(0)
    started += copies
    loads[2].wait()
    loads[3].wait()
    for t in range(col_tiles):
        down = slice(t * LANES, (t + 1) * LANES)
        val_lhs[0:width, down] = v_ref[down, :].astype(F32).T.astype(BF16)
    for _, copy in copies:
        copy.wait_recv()
    total = log_total(col_send[0], [col_recv[0, slot] for slot, _ in copies])
    col_vec[...] = jnp.exp2(cmax_ref[...] - total)

    def row_step(turn):
        for t in range(col_tiles):
            lhs_row[:, t * LANES : (t + 1) * LANES] = split_lhs(col_vec[t : t + 1, :])
        sums = jnp.sum(
            lax.dot_general(
                lhs_row[...], f_ref[...], (((1,), (0,)), ((), ())), preferred_element_type=F32
            ),
            axis=0,
            keepdims=True,
        )
        for t in range(row_tiles):
            row_send[turn, pl.ds(t, 1), :] = sums[:, t * LANES : (t + 1) * LANES]
        copies = send_rows(turn)
        for _, copy in copies:
            copy.wait_recv()
        row_vec[...] = 1.0 / plain_total(
            row_send[turn], [row_recv[turn, slot] for slot, _ in copies]
        )
        return copies

    def col_step(turn):
        for t in range(row_tiles):
            lhs_col[:, t * LANES : (t + 1) * LANES] = split_lhs(row_vec[t : t + 1, :])
        sums = jnp.sum(
            lax.dot_general(
                lhs_col[...], f_ref[...], (((1,), (1,)), ((), ())), preferred_element_type=F32
            ),
            axis=0,
            keepdims=True,
        )
        for t in range(col_tiles):
            col_send[turn, pl.ds(t, 1), :] = (
                sums[:, t * LANES : (t + 1) * LANES] * col_vec[t : t + 1, :]
            )
        copies = send_cols(turn)
        for _, copy in copies:
            copy.wait_recv()
        col_vec[...] = col_vec[...] / plain_total(
            col_send[turn], [col_recv[turn, slot] for slot, _ in copies]
        )
        return copies

    for turn in range(1, SWEEPS):
        started += row_step(turn)
        started += col_step(turn)

    for t in range(col_tiles):
        down = slice(t * LANES, (t + 1) * LANES)
        val_lhs[0:width, down] = (val_lhs[0:width, down].astype(F32) * col_vec[t : t + 1, :]).astype(
            BF16
        )
        val_lhs[width : width + 16, down] = split_lhs(col_vec[t : t + 1, :])
    tail = lax.broadcasted_iota(jnp.int32, (16, LANES), 0)
    sends = []
    for dz in far_first(nz):
        there = lax.rem(z + dz, nz)
        part = jnp.dot(
            val_lhs[...],
            f_ref[:, pl.ds(pl.multiple_of(there * 2 * LANES, 2 * LANES), 2 * LANES)],
            preferred_element_type=F32,
        )
        for x in range(2):
            piece = part[:, x * LANES : (x + 1) * LANES]
            out_send[dz, x, 0:width, :] = piece[0:width].astype(BF16)
            weight = jnp.sum(piece[width:], axis=0, keepdims=True)
            high = weight.astype(BF16).astype(F32)
            out_send[dz, x, width : width + 16, :] = jnp.where(
                tail == 0, high, jnp.where(tail == 1, weight - high, 0.0)
            ).astype(BF16)
        for dx in (1, 0):
            if (dz, dx) != (0, 0):
                copy = pltpu.make_async_remote_copy(
                    src_ref=out_send.at[dz, lax.rem(xl + dx, 2)],
                    dst_ref=out_recv.at[dz, dx],
                    send_sem=out_ssem.at[dz, dx],
                    recv_sem=out_rsem.at[dz, dx],
                    device_id={"gy": row_peer(dz, dx)},
                    device_id_type=MESH,
                )
                copy.start()
                sends.append((dz, dx, copy))
    total = out_send[0, xl].astype(F32)
    for dz, dx, copy in reversed(sends):
        copy.wait_recv()
        total = total + out_recv[dz, dx].astype(F32)
    weight = jnp.sum(total[width:], axis=0, keepdims=True)
    head = (total[0:width] / weight).T.astype(BF16)
    head_send[...] = head
    swap = pltpu.make_async_remote_copy(
        src_ref=head_send,
        dst_ref=head_recv,
        send_sem=head_ssem,
        recv_sem=head_rsem,
        device_id={"gz": 1 - gz},
        device_id_type=MESH,
    )
    swap.start()

    def w_rows(which):
        return w_ref[pl.ds(pl.multiple_of(which * width, width), width), :]

    mixed = jnp.dot(head_send[...], w_rows(gz), preferred_element_type=F32)
    swap.wait_recv()
    mixed = mixed + jnp.dot(head_recv[...], w_rows(1 - gz), preferred_element_type=F32)
    out_ref[...] = mixed.astype(BF16)

    for _, copy in started:
        copy.wait_send()
    for _, _, copy in sends:
        copy.wait_send()
    swap.wait_send()


def solution(mesh):
    nx, ny = mesh.shape["gx"], mesh.shape["gy"]

    def body(queries, keys, values, w_out):
        _, rows, width = queries.shape
        cols = keys.shape[1]
        model = w_out.shape[1] // 2
        row_tiles, col_tiles = rows // LANES, cols // LANES
        anywhere = pl.BlockSpec(memory_space=pl.ANY)
        dma = pltpu.SemaphoreType.DMA
        return pl.pallas_call(
            functools.partial(kernel, (nx, ny)),
            out_shape=jax.ShapeDtypeStruct((rows // ny, model), BF16),
            in_specs=[anywhere] * 4,
            out_specs=pl.BlockSpec(memory_space=pltpu.VMEM),
            scratch_shapes=[
                pltpu.VMEM((rows, width), BF16),
                pltpu.VMEM((cols, width), BF16),
                pltpu.VMEM((cols, width), BF16),
                pltpu.VMEM((2 * width, model), BF16),
                pltpu.VMEM((cols, rows), F32),
                pltpu.VMEM((cols, rows), BF16),
                pltpu.VMEM((16, cols), BF16),
                pltpu.VMEM((16, rows), BF16),
                pltpu.VMEM((width + 16, cols), BF16),
                pltpu.VMEM((col_tiles, LANES), F32),
                pltpu.VMEM((SWEEPS, row_tiles, LANES), F32),
                pltpu.VMEM((SWEEPS, ny, row_tiles, LANES), F32),
                pltpu.VMEM((SWEEPS, col_tiles, LANES), F32),
                pltpu.VMEM((SWEEPS, nx, col_tiles, LANES), F32),
                pltpu.VMEM((row_tiles, LANES), F32),
                pltpu.VMEM((col_tiles, LANES), F32),
                pltpu.VMEM((ny // 2, 2, width + 16, LANES), BF16),
                pltpu.VMEM((ny // 2, 2, width + 16, LANES), BF16),
                pltpu.VMEM((LANES, width), BF16),
                pltpu.VMEM((LANES, width), BF16),
                dma((4,)),
                dma((SWEEPS, ny)),
                dma((SWEEPS, ny)),
                dma((SWEEPS, nx)),
                dma((SWEEPS, nx)),
                dma((ny // 2, 2)),
                dma((ny // 2, 2)),
                dma,
                dma,
            ],
            compiler_params=pltpu.CompilerParams(
                collective_id=0, has_side_effects=True, vmem_limit_bytes=56 * 1024 * 1024
            ),
        )(queries.reshape(rows, width), keys.reshape(cols, width), values.reshape(cols, width), w_out)

    return jax.shard_map(
        body,
        mesh=mesh,
        in_specs=(P("gz", "gx", None), P("gz", "gy", None), P("gz", "gy", None), P()),
        out_specs=P(("gx", "gy"), "gz"),
        check_vma=False,
    )
```

```python
import functools
import math

import jax
import jax.numpy as jnp
from jax import lax
from jax.experimental import pallas as pl
from jax.experimental.pallas import tpu as pltpu
from jax.sharding import PartitionSpec as P

SWEEPS = 3
LANES = 128
MESH = pl.DeviceIdType.MESH
F32 = jnp.float32
BF16 = jnp.bfloat16


def far_first(count):
    return sorted(range(count), key=lambda d: -min(d, count - d))


def split_lhs(x):
    rows = jnp.broadcast_to(x, (16, x.shape[1]))
    hi = rows.astype(BF16).astype(F32)
    rest = rows - hi
    mid = rest.astype(BF16).astype(F32)
    lo = rest - mid
    at = lax.broadcasted_iota(jnp.int32, rows.shape, 0)
    parts = jnp.where(at == 0, hi, jnp.where(at == 1, mid, jnp.where(at == 2, lo, 0.0)))
    return parts.astype(BF16)


def kernel(
    sizes,
    q_hbm,
    k_hbm,
    v_hbm,
    out_ref,
    q_ref,
    k_ref,
    v_ref,
    k_parts,
    s_ref,
    f_ref,
    g_ref,
    lhs_row,
    lhs_col,
    val_lhs,
    cmax_ref,
    row_send,
    row_recv,
    sum_send,
    sum_recv,
    col_send,
    col_recv,
    row_vec,
    col_vec,
    out_send,
    out_recv,
    head_send,
    head_recv,
    load_sem,
    row_ssem,
    row_rsem,
    col_ssem,
    col_rsem,
    out_sem,
    head_sem,
):
    nx, ny = sizes
    rows, width = q_ref.shape
    cols = k_ref.shape[0]
    row_tiles, col_tiles = rows // LANES, cols // LANES
    nz = ny // 2
    gz, gx, gy = lax.axis_index("gz"), lax.axis_index("gx"), lax.axis_index("gy")
    z, xl = gy // 2, lax.rem(gy, 2)
    y, xh = gx // 2, lax.rem(gx, 2)
    scale = math.log2(math.e) / math.sqrt(width)

    row_peers = [(dz, dx) for dz in far_first(nz) for dx in (1, 0) if (dz, dx) != (0, 0)]
    col_peers = [(dy, dx) for dy in far_first(nx // 2) for dx in (1, 0) if (dy, dx) != (0, 0)]

    def row_peer(dz, dx):
        return lax.rem(z + dz, nz) * 2 + lax.rem(xl + dx, 2)

    def col_peer(dy, dx):
        return lax.rem(y + dy, nx // 2) * 2 + lax.rem(xh + dx, 2)

    loads = [
        pltpu.make_async_copy(q_hbm, q_ref, load_sem.at[0]),
        pltpu.make_async_copy(k_hbm, k_ref, load_sem.at[1]),
        pltpu.make_async_copy(v_hbm, v_ref, load_sem.at[2]),
    ]
    for load in loads:
        load.start()

    barrier = pltpu.get_barrier_semaphore()
    for dz, dx in row_peers:
        pl.semaphore_signal(
            barrier, inc=1, device_id={"gy": row_peer(dz, dx)}, device_id_type=MESH
        )
    for dy, dx in col_peers:
        pl.semaphore_signal(
            barrier, inc=1, device_id={"gx": col_peer(dy, dx)}, device_id_type=MESH
        )
    pl.semaphore_signal(barrier, inc=1, device_id={"gz": 1 - gz}, device_id_type=MESH)

    def send_all(source, target, ssem, rsem, peers):
        for slot, device in peers:
            pltpu.make_async_remote_copy(
                src_ref=source,
                dst_ref=target.at[slot],
                send_sem=ssem,
                recv_sem=rsem,
                device_id=device,
                device_id_type=MESH,
            ).start()

    def wait_all(target, sem):
        everything = target.at[pl.ds(1, target.shape[0] - 1)]
        pltpu.make_async_copy(everything, everything, sem).wait()

    row_to = [(dz * 2 + dx, {"gy": row_peer(dz, dx)}) for dz, dx in row_peers]
    col_to = [(dy * 2 + dx, {"gx": col_peer(dy, dx)}) for dy, dx in col_peers]

    def log_total(own, received):
        biggest = own
        for other in received:
            biggest = jnp.maximum(biggest, other)
        total = jnp.exp2(own - biggest)
        for other in received:
            total = total + jnp.exp2(other - biggest)
        return biggest + jnp.log2(total)

    def plain_total(own, received):
        total = own
        for other in received:
            total = total + other
        return total

    loads[1].wait()
    scaled = scale * k_ref[...].astype(F32)
    high = scaled.astype(BF16)
    k_parts[:, 0:width] = high
    k_parts[:, width:] = (scaled - high.astype(F32)).astype(BF16)
    loads[0].wait()
    block = 2 * LANES
    for b in range(rows // block):
        lanes = slice(b * block, (b + 1) * block)
        q_block = q_ref[lanes, :]
        scores = lax.dot_general(
            k_parts[...],
            jnp.concatenate([q_block, q_block], axis=1),
            (((1,), (1,)), ((), ())),
            preferred_element_type=F32,
        )
        s_ref[:, lanes] = scores
        biggest, summed = None, None
        for jb in range(col_tiles):
            part = scores[jb * LANES : (jb + 1) * LANES].reshape(LANES // 8, 8, block)
            top = jnp.max(part, axis=0)
            total = jnp.sum(jnp.exp2(part - top[None]), axis=0)
            if biggest is None:
                biggest, summed = top, total
            else:
                larger = jnp.maximum(biggest, top)
                summed = summed * jnp.exp2(biggest - larger) + total * jnp.exp2(top - larger)
                biggest = larger
        top = jnp.max(biggest, axis=0, keepdims=True)
        summed = jnp.sum(summed * jnp.exp2(biggest - top), axis=0, keepdims=True)
        local = top + jnp.log2(summed)
        for t in range(block // LANES):
            row_send[pl.ds(b * (block // LANES) + t, 1), :] = local[:, t * LANES : (t + 1) * LANES]

    pl.semaphore_wait(barrier, len(row_peers) + len(col_peers) + 1)
    send_all(row_send, row_recv, row_ssem.at[0], row_rsem.at[0], row_to)
    wait_all(row_recv, row_rsem.at[0])
    row_vec[...] = -log_total(row_send[...], [row_recv[slot] for slot in range(1, ny)])

    eye = lax.broadcasted_iota(jnp.int32, (LANES, LANES), 0) == lax.broadcasted_iota(
        jnp.int32, (LANES, LANES), 1
    )

    def across(column):
        return jnp.sum(
            jnp.where(eye, jnp.broadcast_to(column, (LANES, LANES)), 0.0), axis=0, keepdims=True
        )

    tiles = [slice(t * LANES, (t + 1) * LANES) for t in range(row_tiles)]
    for jb in range(col_tiles):
        down = slice(jb * LANES, (jb + 1) * LANES)
        biggest = None
        for t in range(row_tiles):
            shifted = s_ref[down, tiles[t]] + row_vec[t : t + 1, :]
            s_ref[down, tiles[t]] = shifted
            biggest = shifted if biggest is None else jnp.maximum(biggest, shifted)
        biggest = jnp.max(biggest, axis=1, keepdims=True)
        wide = jnp.broadcast_to(biggest, (LANES, LANES))
        summed = jnp.zeros((LANES, LANES), F32)
        for t in range(row_tiles):
            part = jnp.exp2(s_ref[down, tiles[t]] - wide)
            f_ref[down, tiles[t]] = part.astype(BF16)
            summed = summed + part
        summed = jnp.sum(summed, axis=1, keepdims=True)
        cmax_ref[pl.ds(jb, 1), :] = across(biggest)
        col_send[0, pl.ds(jb, 1), :] = across(biggest + jnp.log2(summed))

    send_all(col_send.at[0], col_recv.at[0], col_ssem.at[0], col_rsem.at[0], col_to)
    loads[2].wait()
    for t in range(col_tiles):
        down = slice(t * LANES, (t + 1) * LANES)
        val_lhs[0:width, down] = v_ref[down, :].astype(F32).T.astype(BF16)
        for i in range(row_tiles):
            g_ref[tiles[i], down] = f_ref[down, tiles[i]].T
    wait_all(col_recv.at[0], col_rsem.at[0])
    total = log_total(col_send[0], [col_recv[0, slot] for slot in range(1, nx)])
    col_vec[...] = jnp.exp2(cmax_ref[...] - total)

    def row_step(turn):
        for t in range(col_tiles):
            lhs_row[:, t * LANES : (t + 1) * LANES] = split_lhs(col_vec[t : t + 1, :])
        sums = jnp.sum(
            lax.dot_general(
                lhs_row[...], f_ref[...], (((1,), (0,)), ((), ())), preferred_element_type=F32
            ),
            axis=0,
            keepdims=True,
        )
        for t in range(row_tiles):
            row_vec[pl.ds(t, 1), :] = sums[:, t * LANES : (t + 1) * LANES]
        own = row_vec[...].astype(BF16)
        sum_send[turn - 1] = own
        send_all(
            sum_send.at[turn - 1], sum_recv.at[turn - 1], row_ssem.at[turn], row_rsem.at[turn], row_to
        )
        wait_all(sum_recv.at[turn - 1], row_rsem.at[turn])
        row_vec[...] = 1.0 / plain_total(
            own.astype(F32), [sum_recv[turn - 1, slot].astype(F32) for slot in range(1, ny)]
        )

    def col_step(turn):
        for t in range(row_tiles):
            lhs_col[:, t * LANES : (t + 1) * LANES] = split_lhs(row_vec[t : t + 1, :])
        sums = jnp.sum(
            lax.dot_general(
                lhs_col[...], g_ref[...], (((1,), (0,)), ((), ())), preferred_element_type=F32
            ),
            axis=0,
            keepdims=True,
        )
        for t in range(col_tiles):
            col_send[turn, pl.ds(t, 1), :] = (
                sums[:, t * LANES : (t + 1) * LANES] * col_vec[t : t + 1, :]
            )
        send_all(
            col_send.at[turn], col_recv.at[turn], col_ssem.at[turn], col_rsem.at[turn], col_to
        )
        wait_all(col_recv.at[turn], col_rsem.at[turn])
        col_vec[...] = col_vec[...] / plain_total(
            col_send[turn], [col_recv[turn, slot] for slot in range(1, nx)]
        )

    for turn in range(1, SWEEPS):
        row_step(turn)
        col_step(turn)

    for t in range(col_tiles):
        down = slice(t * LANES, (t + 1) * LANES)
        val_lhs[0:width, down] = (val_lhs[0:width, down].astype(F32) * col_vec[t : t + 1, :]).astype(
            BF16
        )
        val_lhs[width : width + 16, down] = split_lhs(col_vec[t : t + 1, :])
    tail = lax.broadcasted_iota(jnp.int32, (16, LANES), 0)

    def product(dz):
        there = lax.rem(z + dz, nz)
        return jnp.dot(
            val_lhs[...],
            f_ref[:, pl.ds(pl.multiple_of(there * 2 * LANES, 2 * LANES), 2 * LANES)],
            preferred_element_type=F32,
        )

    order = far_first(nz)
    ahead = product(order[0])
    for n, dz in enumerate(order):
        part = ahead
        if n + 1 < nz:
            ahead = product(order[n + 1])
        for x in range(2):
            piece = part[:, x * LANES : (x + 1) * LANES]
            out_send[dz, x, 0:width, :] = piece[0:width].astype(BF16)
            weight = jnp.sum(piece[width:], axis=0, keepdims=True)
            high = weight.astype(BF16).astype(F32)
            out_send[dz, x, width : width + 16, :] = jnp.where(
                tail == 0, high, jnp.where(tail == 1, weight - high, 0.0)
            ).astype(BF16)
        for dx in (1, 0):
            if (dz, dx) != (0, 0):
                pltpu.make_async_remote_copy(
                    src_ref=out_send.at[dz, lax.rem(xl + dx, 2)],
                    dst_ref=out_recv.at[dz * 2 + dx],
                    send_sem=out_sem.at[0],
                    recv_sem=out_sem.at[1],
                    device_id={"gy": row_peer(dz, dx)},
                    device_id_type=MESH,
                ).start()
    wait_all(out_recv, out_sem.at[1])
    total = out_send[0, xl].astype(F32)
    for slot in range(1, ny):
        total = total + out_recv[slot].astype(F32)
    weight = jnp.sum(total[width:], axis=0, keepdims=True)
    head = (total[0:width] / weight).T.astype(BF16)
    head_send[...] = head
    swap = pltpu.make_async_remote_copy(
        src_ref=head_send,
        dst_ref=head_recv,
        send_sem=head_sem.at[0],
        recv_sem=head_sem.at[1],
        device_id={"gz": 1 - gz},
        device_id_type=MESH,
    )
    swap.start()
    out_ref[:, pl.ds(pl.multiple_of(gz * width, width), width)] = head
    wait_all(row_recv, row_ssem.at[0])
    wait_all(col_recv.at[0], col_ssem.at[0])
    for turn in range(1, SWEEPS):
        wait_all(sum_recv.at[turn - 1], row_ssem.at[turn])
        wait_all(col_recv.at[turn], col_ssem.at[turn])
    wait_all(out_recv, out_sem.at[0])
    swap.wait()
    out_ref[:, pl.ds(pl.multiple_of((1 - gz) * width, width), width)] = head_recv[...]


def solution(mesh):
    nx, ny = mesh.shape["gx"], mesh.shape["gy"]

    def body(queries, keys, values, w_out):
        _, rows, width = queries.shape
        cols = keys.shape[1]
        columns = w_out.shape[1] // lax.axis_size("gz")
        row_tiles, col_tiles = rows // LANES, cols // LANES
        anywhere = pl.BlockSpec(memory_space=pl.ANY)
        dma = pltpu.SemaphoreType.DMA
        heads = pl.pallas_call(
            functools.partial(kernel, (nx, ny)),
            out_shape=jax.ShapeDtypeStruct((rows // ny, 2 * width), BF16),
            in_specs=[anywhere] * 3,
            out_specs=pl.BlockSpec(memory_space=pltpu.VMEM),
            scratch_shapes=[
                pltpu.VMEM((rows, width), BF16),
                pltpu.VMEM((cols, width), BF16),
                pltpu.VMEM((cols, width), BF16),
                pltpu.VMEM((cols, 2 * width), BF16),
                pltpu.VMEM((cols, rows), F32),
                pltpu.VMEM((cols, rows), BF16),
                pltpu.VMEM((rows, cols), BF16),
                pltpu.VMEM((16, cols), BF16),
                pltpu.VMEM((16, rows), BF16),
                pltpu.VMEM((width + 16, cols), BF16),
                pltpu.VMEM((col_tiles, LANES), F32),
                pltpu.VMEM((row_tiles, LANES), F32),
                pltpu.VMEM((ny, row_tiles, LANES), F32),
                pltpu.VMEM((SWEEPS - 1, row_tiles, LANES), BF16),
                pltpu.VMEM((SWEEPS - 1, ny, row_tiles, LANES), BF16),
                pltpu.VMEM((SWEEPS, col_tiles, LANES), F32),
                pltpu.VMEM((SWEEPS, nx, col_tiles, LANES), F32),
                pltpu.VMEM((row_tiles, LANES), F32),
                pltpu.VMEM((col_tiles, LANES), F32),
                pltpu.VMEM((ny // 2, 2, width + 16, LANES), BF16),
                pltpu.VMEM((ny, width + 16, LANES), BF16),
                pltpu.VMEM((LANES, width), BF16),
                pltpu.VMEM((LANES, width), BF16),
                dma((3,)),
                dma((SWEEPS,)),
                dma((SWEEPS,)),
                dma((SWEEPS,)),
                dma((SWEEPS,)),
                dma((2,)),
                dma((2,)),
            ],
            compiler_params=pltpu.CompilerParams(
                collective_id=0, has_side_effects=True, vmem_limit_bytes=56 * 1024 * 1024
            ),
        )(queries.reshape(rows, width), keys.reshape(cols, width), values.reshape(cols, width))
        w_columns = lax.dynamic_slice_in_dim(
            w_out, lax.axis_index("gz") * columns, columns, 1
        )
        return jnp.dot(heads, w_columns, preferred_element_type=F32).astype(BF16)

    return jax.shard_map(
        body,
        mesh=mesh,
        in_specs=(P("gz", "gx", None), P("gz", "gy", None), P("gz", "gy", None), P()),
        out_specs=P(("gx", "gy"), "gz"),
        check_vma=False,
    )
```

```python
import functools
import math

import jax
import jax.numpy as jnp
from jax import lax
from jax.experimental import pallas as pl
from jax.experimental.pallas import tpu as pltpu
from jax.sharding import PartitionSpec as P

SWEEPS = 3
LANES = 128
MESH = pl.DeviceIdType.MESH
F32 = jnp.float32
BF16 = jnp.bfloat16


def far_first(count):
    return sorted(range(count), key=lambda d: -min(d, count - d))


def split_lhs(x):
    rows = jnp.broadcast_to(x, (16, x.shape[1]))
    hi = rows.astype(BF16).astype(F32)
    rest = rows - hi
    mid = rest.astype(BF16).astype(F32)
    lo = rest - mid
    at = lax.broadcasted_iota(jnp.int32, rows.shape, 0)
    parts = jnp.where(at == 0, hi, jnp.where(at == 1, mid, jnp.where(at == 2, lo, 0.0)))
    return parts.astype(BF16)


def kernel(
    sizes,
    q_hbm,
    k_hbm,
    v_hbm,
    out_ref,
    q_ref,
    k_ref,
    v_ref,
    k_parts,
    s_ref,
    f_ref,
    g_ref,
    lhs_row,
    lhs_col,
    val_lhs,
    k2_ref,
    v2_ref,
    pair_ref,
    wide_ref,
    row_log,
    log_send,
    log_recv,
    part_send,
    part_recv,
    side_recv,
    cmax_ref,
    row_send,
    row_recv,
    sum_send,
    sum_recv,
    col_send,
    col_recv,
    row_vec,
    col_vec,
    out_send,
    out_recv,
    head_send,
    head_recv,
    load_sem,
    row_ssem,
    row_rsem,
    col_ssem,
    col_rsem,
    out_sem,
    head_sem,
    pair_ssem,
    pair_rsem,
    side_sem,
):
    nx, ny = sizes
    rows, width = q_ref.shape
    cols = k_ref.shape[0]
    row_tiles, col_tiles = rows // LANES, cols // LANES
    nz = ny // 2
    gz, gx, gy = lax.axis_index("gz"), lax.axis_index("gx"), lax.axis_index("gy")
    z, xl = gy // 2, lax.rem(gy, 2)
    y, xh = gx // 2, lax.rem(gx, 2)
    scale = math.log2(math.e) / math.sqrt(width)

    row_peers = [(dz, dx) for dz in far_first(nz) for dx in (1, 0) if (dz, dx) != (0, 0)]
    col_peers = [(dy, dx) for dy in far_first(nx // 2) for dx in (1, 0) if (dy, dx) != (0, 0)]

    def row_peer(dz, dx):
        return lax.rem(z + dz, nz) * 2 + lax.rem(xl + dx, 2)

    def col_peer(dy, dx):
        return lax.rem(y + dy, nx // 2) * 2 + lax.rem(xh + dx, 2)

    loads = [
        pltpu.make_async_copy(q_hbm, q_ref, load_sem.at[0]),
        pltpu.make_async_copy(k_hbm, k_ref, load_sem.at[1]),
        pltpu.make_async_copy(v_hbm, v_ref, load_sem.at[2]),
    ]
    for load in loads:
        load.start()

    barrier = pltpu.get_barrier_semaphore()
    for dz, dx in row_peers:
        pl.semaphore_signal(
            barrier, inc=1, device_id={"gy": row_peer(dz, dx)}, device_id_type=MESH
        )
    for dy, dx in col_peers:
        pl.semaphore_signal(
            barrier, inc=1, device_id={"gx": col_peer(dy, dx)}, device_id_type=MESH
        )
    pl.semaphore_signal(barrier, inc=1, device_id={"gz": 1 - gz}, device_id_type=MESH)
    beside = z * 2 + 1 - xl
    for dy, dx in col_peers:
        pl.semaphore_signal(
            barrier,
            inc=1,
            device_id={"gx": col_peer(dy, dx), "gy": beside},
            device_id_type=MESH,
        )

    def send_all(source, target, ssem, rsem, peers):
        for slot, device in peers:
            pltpu.make_async_remote_copy(
                src_ref=source,
                dst_ref=target.at[slot],
                send_sem=ssem,
                recv_sem=rsem,
                device_id=device,
                device_id_type=MESH,
            ).start()

    def wait_all(target, sem):
        everything = target.at[pl.ds(1, target.shape[0] - 1)]
        pltpu.make_async_copy(everything, everything, sem).wait()

    row_to = [(dz * 2 + dx, {"gy": row_peer(dz, dx)}) for dz, dx in row_peers]
    col_to = [(dy * 2 + dx, {"gx": col_peer(dy, dx)}) for dy, dx in col_peers]
    side_to = [
        (dy * 2 + dx, {"gx": col_peer(dy, dx), "gy": beside}) for dy, dx in [*col_peers, (0, 0)]
    ]

    def to_pair(source, target, number):
        return pltpu.make_async_remote_copy(
            src_ref=source,
            dst_ref=target,
            send_sem=pair_ssem.at[number],
            recv_sem=pair_rsem.at[number],
            device_id={"gy": beside},
            device_id_type=MESH,
        )

    pair_copies = [
        to_pair(k_ref, k2_ref, 0),
        to_pair(v_ref, v2_ref, 1),
        to_pair(log_send, log_recv, 2),
        to_pair(part_send, part_recv, 3),
    ]
    order = far_first(nz)

    def log_total(own, received):
        biggest = own
        for other in received:
            biggest = jnp.maximum(biggest, other)
        total = jnp.exp2(own - biggest)
        for other in received:
            total = total + jnp.exp2(other - biggest)
        return biggest + jnp.log2(total)

    def plain_total(own, received):
        total = own
        for other in received:
            total = total + other
        return total

    loads[1].wait()
    scaled = scale * k_ref[...].astype(F32)
    high = scaled.astype(BF16)
    k_parts[:, 0:width] = high
    k_parts[:, width:] = (scaled - high.astype(F32)).astype(BF16)
    loads[0].wait()
    block = 2 * LANES
    for b in range(rows // block):
        lanes = slice(b * block, (b + 1) * block)
        q_block = q_ref[lanes, :]
        scores = lax.dot_general(
            k_parts[...],
            jnp.concatenate([q_block, q_block], axis=1),
            (((1,), (1,)), ((), ())),
            preferred_element_type=F32,
        )
        s_ref[:, lanes] = scores
        biggest, summed = None, None
        for jb in range(col_tiles):
            part = scores[jb * LANES : (jb + 1) * LANES].reshape(LANES // 8, 8, block)
            top = jnp.max(part, axis=0)
            total = jnp.sum(jnp.exp2(part - top[None]), axis=0)
            if biggest is None:
                biggest, summed = top, total
            else:
                larger = jnp.maximum(biggest, top)
                summed = summed * jnp.exp2(biggest - larger) + total * jnp.exp2(top - larger)
                biggest = larger
        top = jnp.max(biggest, axis=0, keepdims=True)
        summed = jnp.sum(summed * jnp.exp2(biggest - top), axis=0, keepdims=True)
        local = top + jnp.log2(summed)
        for t in range(block // LANES):
            row_send[pl.ds(b * (block // LANES) + t, 1), :] = local[:, t * LANES : (t + 1) * LANES]

    pl.semaphore_wait(barrier, len(row_peers) + 2 * len(col_peers) + 1)
    send_all(row_send, row_recv, row_ssem.at[0], row_rsem.at[0], row_to)
    pair_copies[0].start()
    wait_all(row_recv, row_rsem.at[0])
    loads[2].wait()
    pair_copies[1].start()
    row_log[...] = -log_total(row_send[...], [row_recv[slot] for slot in range(1, ny)])

    eye = lax.broadcasted_iota(jnp.int32, (LANES, LANES), 0) == lax.broadcasted_iota(
        jnp.int32, (LANES, LANES), 1
    )

    def across(column):
        return jnp.sum(
            jnp.where(eye, jnp.broadcast_to(column, (LANES, LANES)), 0.0), axis=0, keepdims=True
        )

    tiles = [slice(t * LANES, (t + 1) * LANES) for t in range(row_tiles)]
    for jb in range(col_tiles):
        down = slice(jb * LANES, (jb + 1) * LANES)
        biggest = None
        for t in range(row_tiles):
            shifted = s_ref[down, tiles[t]] + row_log[t : t + 1, :]
            s_ref[down, tiles[t]] = shifted
            biggest = shifted if biggest is None else jnp.maximum(biggest, shifted)
        biggest = jnp.max(biggest, axis=1, keepdims=True)
        wide = jnp.broadcast_to(biggest, (LANES, LANES))
        summed = jnp.zeros((LANES, LANES), F32)
        for t in range(row_tiles):
            part = jnp.exp2(s_ref[down, tiles[t]] - wide)
            f_ref[down, tiles[t]] = part.astype(BF16)
            summed = summed + part
        summed = jnp.sum(summed, axis=1, keepdims=True)
        cmax_ref[pl.ds(jb, 1), :] = across(biggest)
        col_send[0, pl.ds(jb, 1), :] = across(biggest + jnp.log2(summed))

    send_all(col_send.at[0], col_recv.at[0], col_ssem.at[0], col_rsem.at[0], col_to)
    for t in range(col_tiles):
        down = slice(t * LANES, (t + 1) * LANES)
        val_lhs[0:width, down] = v_ref[down, :].astype(F32).T.astype(BF16)
        for i in range(row_tiles):
            g_ref[tiles[i], down] = f_ref[down, tiles[i]].T
    wait_all(col_recv.at[0], col_rsem.at[0])
    total = log_total(col_send[0], [col_recv[0, slot] for slot in range(1, nx)])
    log_send[...] = -total
    pair_copies[2].start()
    col_vec[...] = jnp.exp2(cmax_ref[...] - total)

    def for_pair():
        pair_copies[0].wait_recv()
        scaled = scale * k2_ref[...].astype(F32)
        high = scaled.astype(BF16)
        k_parts[:, 0:width] = high
        k_parts[:, width:] = (scaled - high.astype(F32)).astype(BF16)
        pair_copies[1].wait_recv()
        for t in range(col_tiles):
            down = slice(t * LANES, (t + 1) * LANES)
            val_lhs[0:width, cols + t * LANES : cols + (t + 1) * LANES] = (
                v2_ref[down, :].astype(F32).T.astype(BF16)
            )
        pair_copies[2].wait_recv()
        for t in range(col_tiles):
            line = jnp.broadcast_to(log_recv[t : t + 1, :], (LANES, LANES))
            column = jnp.sum(jnp.where(eye, line, 0.0), axis=1, keepdims=True)
            wide_ref[t * LANES : (t + 1) * LANES, :] = jnp.broadcast_to(column, (LANES, LANES))
        for m in range(nz // 2):
            chunks = [lax.rem(z + dz, nz) * 2 + xl for dz in order[2 * m : 2 * m + 2]]
            q_block = jnp.concatenate(
                [q_ref[pl.ds(pl.multiple_of(c * LANES, LANES), LANES), :] for c in chunks], axis=0
            )
            scores = lax.dot_general(
                k_parts[...],
                jnp.concatenate([q_block, q_block], axis=1),
                (((1,), (1,)), ((), ())),
                preferred_element_type=F32,
            )
            for n, c in enumerate(chunks):
                across_lanes = slice((2 * m + n) * LANES, (2 * m + n + 1) * LANES)
                part = scores[:, n * LANES : (n + 1) * LANES] + wide_ref[...]
                pair_ref[cols:, across_lanes] = jnp.exp2(part + row_log[pl.ds(c, 1), :]).astype(BF16)

    def own_half():
        for n, dz in enumerate(order):
            c = lax.rem(z + dz, nz) * 2 + xl
            pair_ref[0:cols, n * LANES : (n + 1) * LANES] = f_ref[
                :, pl.ds(pl.multiple_of(c * LANES, LANES), LANES)
            ]

    def row_step(turn):
        for t in range(col_tiles):
            lhs_row[:, t * LANES : (t + 1) * LANES] = split_lhs(col_vec[t : t + 1, :])
        sums = jnp.sum(
            lax.dot_general(
                lhs_row[...], f_ref[...], (((1,), (0,)), ((), ())), preferred_element_type=F32
            ),
            axis=0,
            keepdims=True,
        )
        for t in range(row_tiles):
            row_vec[pl.ds(t, 1), :] = sums[:, t * LANES : (t + 1) * LANES]
        own = row_vec[...].astype(BF16)
        sum_send[turn - 1] = own
        send_all(
            sum_send.at[turn - 1], sum_recv.at[turn - 1], row_ssem.at[turn], row_rsem.at[turn], row_to
        )
        if turn == 1:
            for_pair()
        wait_all(sum_recv.at[turn - 1], row_rsem.at[turn])
        row_vec[...] = 1.0 / plain_total(
            own.astype(F32), [sum_recv[turn - 1, slot].astype(F32) for slot in range(1, ny)]
        )

    def col_step(turn):
        for t in range(row_tiles):
            lhs_col[:, t * LANES : (t + 1) * LANES] = split_lhs(row_vec[t : t + 1, :])
        sums = jnp.sum(
            lax.dot_general(
                lhs_col[...], g_ref[...], (((1,), (0,)), ((), ())), preferred_element_type=F32
            ),
            axis=0,
            keepdims=True,
        )
        for t in range(col_tiles):
            col_send[turn, pl.ds(t, 1), :] = (
                sums[:, t * LANES : (t + 1) * LANES] * col_vec[t : t + 1, :]
            )
        send_all(
            col_send.at[turn], col_recv.at[turn], col_ssem.at[turn], col_rsem.at[turn], col_to
        )
        if turn == 1:
            own_half()
        if turn == SWEEPS - 1:
            send_all(col_send.at[turn], side_recv, side_sem.at[0], side_sem.at[1], side_to)
        wait_all(col_recv.at[turn], col_rsem.at[turn])
        inverse = 1.0 / plain_total(
            col_send[turn], [col_recv[turn, slot] for slot in range(1, nx)]
        )
        col_vec[...] = col_vec[...] * inverse
        if turn == 1:
            part_send[...] = inverse
            pair_copies[3].start()

    for turn in range(1, SWEEPS):
        row_step(turn)
        col_step(turn)

    pltpu.make_async_copy(side_recv, side_recv, side_sem.at[1]).wait()
    pair_copies[3].wait_recv()
    side = part_recv[...] / plain_total(side_recv[0], [side_recv[slot] for slot in range(1, nx)])
    for t in range(2 * col_tiles):
        lanes = slice(t * LANES, (t + 1) * LANES)
        if t < col_tiles:
            line = col_vec[t : t + 1, :]
        else:
            line = side[t - col_tiles : t - col_tiles + 1, :]
        val_lhs[0:width, lanes] = (val_lhs[0:width, lanes].astype(F32) * line).astype(BF16)
        val_lhs[width : width + 16, lanes] = split_lhs(line)
    tail = lax.broadcasted_iota(jnp.int32, (16, LANES), 0)

    def product(m):
        return jnp.dot(
            val_lhs[...],
            pair_ref[:, m * 2 * LANES : (m + 1) * 2 * LANES],
            preferred_element_type=F32,
        )

    ahead = product(0)
    for m in range(nz // 2):
        both = ahead
        if m + 1 < nz // 2:
            ahead = product(m + 1)
        for x in range(2):
            dz = order[2 * m + x]
            piece = both[:, x * LANES : (x + 1) * LANES]
            out_send[dz, 0:width, :] = piece[0:width].astype(BF16)
            weight = jnp.sum(piece[width:], axis=0, keepdims=True)
            high = weight.astype(BF16).astype(F32)
            out_send[dz, width : width + 16, :] = jnp.where(
                tail == 0, high, jnp.where(tail == 1, weight - high, 0.0)
            ).astype(BF16)
            if dz != 0:
                pltpu.make_async_remote_copy(
                    src_ref=out_send.at[dz],
                    dst_ref=out_recv.at[dz],
                    send_sem=out_sem.at[0],
                    recv_sem=out_sem.at[1],
                    device_id={"gy": row_peer(dz, 0)},
                    device_id_type=MESH,
                ).start()
    wait_all(out_recv, out_sem.at[1])
    total = out_send[0].astype(F32)
    for slot in range(1, nz):
        total = total + out_recv[slot].astype(F32)
    weight = jnp.sum(total[width:], axis=0, keepdims=True)
    head = (total[0:width] / weight).T.astype(BF16)
    head_send[...] = head
    swap = pltpu.make_async_remote_copy(
        src_ref=head_send,
        dst_ref=head_recv,
        send_sem=head_sem.at[0],
        recv_sem=head_sem.at[1],
        device_id={"gz": 1 - gz},
        device_id_type=MESH,
    )
    swap.start()
    out_ref[:, pl.ds(pl.multiple_of(gz * width, width), width)] = head
    wait_all(row_recv, row_ssem.at[0])
    wait_all(col_recv.at[0], col_ssem.at[0])
    for turn in range(1, SWEEPS):
        wait_all(sum_recv.at[turn - 1], row_ssem.at[turn])
        wait_all(col_recv.at[turn], col_ssem.at[turn])
    wait_all(out_recv, out_sem.at[0])
    pltpu.make_async_copy(side_recv, side_recv, side_sem.at[0]).wait()
    for copy in pair_copies:
        copy.wait_send()
    swap.wait()
    out_ref[:, pl.ds(pl.multiple_of((1 - gz) * width, width), width)] = head_recv[...]


def solution(mesh):
    nx, ny = mesh.shape["gx"], mesh.shape["gy"]

    def body(queries, keys, values, w_out):
        _, rows, width = queries.shape
        cols = keys.shape[1]
        columns = w_out.shape[1] // lax.axis_size("gz")
        row_tiles, col_tiles = rows // LANES, cols // LANES
        anywhere = pl.BlockSpec(memory_space=pl.ANY)
        dma = pltpu.SemaphoreType.DMA
        heads = pl.pallas_call(
            functools.partial(kernel, (nx, ny)),
            out_shape=jax.ShapeDtypeStruct((rows // ny, 2 * width), BF16),
            in_specs=[anywhere] * 3,
            out_specs=pl.BlockSpec(memory_space=pltpu.VMEM),
            scratch_shapes=[
                pltpu.VMEM((rows, width), BF16),
                pltpu.VMEM((cols, width), BF16),
                pltpu.VMEM((cols, width), BF16),
                pltpu.VMEM((cols, 2 * width), BF16),
                pltpu.VMEM((cols, rows), F32),
                pltpu.VMEM((cols, rows), BF16),
                pltpu.VMEM((rows, cols), BF16),
                pltpu.VMEM((16, cols), BF16),
                pltpu.VMEM((16, rows), BF16),
                pltpu.VMEM((width + 16, 2 * cols), BF16),
                pltpu.VMEM((cols, width), BF16),
                pltpu.VMEM((cols, width), BF16),
                pltpu.VMEM((2 * cols, rows // 2), BF16),
                pltpu.VMEM((cols, LANES), F32),
                pltpu.VMEM((row_tiles, LANES), F32),
                pltpu.VMEM((col_tiles, LANES), F32),
                pltpu.VMEM((col_tiles, LANES), F32),
                pltpu.VMEM((col_tiles, LANES), F32),
                pltpu.VMEM((col_tiles, LANES), F32),
                pltpu.VMEM((nx, col_tiles, LANES), F32),
                pltpu.VMEM((col_tiles, LANES), F32),
                pltpu.VMEM((row_tiles, LANES), F32),
                pltpu.VMEM((ny, row_tiles, LANES), F32),
                pltpu.VMEM((SWEEPS - 1, row_tiles, LANES), BF16),
                pltpu.VMEM((SWEEPS - 1, ny, row_tiles, LANES), BF16),
                pltpu.VMEM((SWEEPS, col_tiles, LANES), F32),
                pltpu.VMEM((SWEEPS, nx, col_tiles, LANES), F32),
                pltpu.VMEM((row_tiles, LANES), F32),
                pltpu.VMEM((col_tiles, LANES), F32),
                pltpu.VMEM((ny // 2, width + 16, LANES), BF16),
                pltpu.VMEM((ny // 2, width + 16, LANES), BF16),
                pltpu.VMEM((LANES, width), BF16),
                pltpu.VMEM((LANES, width), BF16),
                dma((3,)),
                dma((SWEEPS,)),
                dma((SWEEPS,)),
                dma((SWEEPS,)),
                dma((SWEEPS,)),
                dma((2,)),
                dma((2,)),
                dma((4,)),
                dma((4,)),
                dma((2,)),
            ],
            compiler_params=pltpu.CompilerParams(
                collective_id=0, has_side_effects=True, vmem_limit_bytes=56 * 1024 * 1024
            ),
        )(queries.reshape(rows, width), keys.reshape(cols, width), values.reshape(cols, width))
        w_columns = lax.dynamic_slice_in_dim(
            w_out, lax.axis_index("gz") * columns, columns, 1
        )
        return jnp.dot(heads, w_columns, preferred_element_type=F32).astype(BF16)

    return jax.shard_map(
        body,
        mesh=mesh,
        in_specs=(P("gz", "gx", None), P("gz", "gy", None), P("gz", "gy", None), P()),
        out_specs=P(("gx", "gy"), "gz"),
        check_vma=False,
    )
```

```python
import functools
import math

import jax
import jax.numpy as jnp
from jax import lax
from jax.experimental import pallas as pl
from jax.experimental.pallas import tpu as pltpu
from jax.sharding import PartitionSpec as P

SWEEPS = 3
LANES = 128
MESH = pl.DeviceIdType.MESH
F32 = jnp.float32
BF16 = jnp.bfloat16


def far_first(count):
    return sorted(range(count), key=lambda d: -min(d, count - d))


def split_lhs(x):
    rows = jnp.broadcast_to(x, (16, x.shape[1]))
    hi = rows.astype(BF16).astype(F32)
    rest = rows - hi
    mid = rest.astype(BF16).astype(F32)
    lo = rest - mid
    at = lax.broadcasted_iota(jnp.int32, rows.shape, 0)
    parts = jnp.where(at == 0, hi, jnp.where(at == 1, mid, jnp.where(at == 2, lo, 0.0)))
    return parts.astype(BF16)


def kernel(
    sizes,
    q_hbm,
    k_hbm,
    v_hbm,
    out_ref,
    q_ref,
    k_ref,
    v_ref,
    k_parts,
    s_ref,
    f_ref,
    g_ref,
    lhs_row,
    lhs_col,
    val_lhs,
    k2_ref,
    v2_ref,
    pair_ref,
    wide_ref,
    row_log,
    log_send,
    log_recv,
    part_send,
    part_recv,
    side_recv,
    cmax_ref,
    row_send,
    row_recv,
    sum_send,
    sum_recv,
    col_send,
    col_recv,
    row_vec,
    col_vec,
    out_send,
    out_recv,
    head_send,
    head_recv,
    load_sem,
    row_ssem,
    row_rsem,
    col_ssem,
    col_rsem,
    out_sem,
    head_sem,
    pair_ssem,
    pair_rsem,
    side_sem,
):
    nx, ny = sizes
    rows, width = q_ref.shape
    cols = k_ref.shape[0]
    row_tiles, col_tiles = rows // LANES, cols // LANES
    nz = ny // 2
    gz, gx, gy = lax.axis_index("gz"), lax.axis_index("gx"), lax.axis_index("gy")
    z, xl = gy // 2, lax.rem(gy, 2)
    y, xh = gx // 2, lax.rem(gx, 2)
    scale = math.log2(math.e) / math.sqrt(width)

    row_peers = [(dz, dx) for dz in far_first(nz) for dx in (1, 0) if (dz, dx) != (0, 0)]
    col_peers = [(dy, dx) for dy in far_first(nx // 2) for dx in (1, 0) if (dy, dx) != (0, 0)]

    def row_peer(dz, dx):
        return lax.rem(z + dz, nz) * 2 + lax.rem(xl + dx, 2)

    def col_peer(dy, dx):
        return lax.rem(y + dy, nx // 2) * 2 + lax.rem(xh + dx, 2)

    loads = [
        pltpu.make_async_copy(q_hbm, q_ref, load_sem.at[0]),
        pltpu.make_async_copy(k_hbm, k_ref, load_sem.at[1]),
        pltpu.make_async_copy(v_hbm, v_ref, load_sem.at[2]),
    ]
    for load in loads:
        load.start()

    barrier = pltpu.get_barrier_semaphore()
    for dz, dx in row_peers:
        pl.semaphore_signal(
            barrier, inc=1, device_id={"gy": row_peer(dz, dx)}, device_id_type=MESH
        )
    for dy, dx in col_peers:
        pl.semaphore_signal(
            barrier, inc=1, device_id={"gx": col_peer(dy, dx)}, device_id_type=MESH
        )
    pl.semaphore_signal(barrier, inc=1, device_id={"gz": 1 - gz}, device_id_type=MESH)
    beside = z * 2 + 1 - xl
    for dy, dx in col_peers:
        pl.semaphore_signal(
            barrier,
            inc=1,
            device_id={"gx": col_peer(dy, dx), "gy": beside},
            device_id_type=MESH,
        )

    def send_all(source, target, ssem, rsem, peers):
        for slot, device in peers:
            pltpu.make_async_remote_copy(
                src_ref=source,
                dst_ref=target.at[slot],
                send_sem=ssem,
                recv_sem=rsem,
                device_id=device,
                device_id_type=MESH,
            ).start()

    def wait_all(target, sem):
        everything = target.at[pl.ds(1, target.shape[0] - 1)]
        pltpu.make_async_copy(everything, everything, sem).wait()

    row_to = [(dz * 2 + dx, {"gy": row_peer(dz, dx)}) for dz, dx in row_peers]
    col_to = [(dy * 2 + dx, {"gx": col_peer(dy, dx)}) for dy, dx in col_peers]
    side_to = [
        (dy * 2 + dx, {"gx": col_peer(dy, dx), "gy": beside}) for dy, dx in [*col_peers, (0, 0)]
    ]

    def to_pair(source, target, number):
        return pltpu.make_async_remote_copy(
            src_ref=source,
            dst_ref=target,
            send_sem=pair_ssem.at[number],
            recv_sem=pair_rsem.at[number],
            device_id={"gy": beside},
            device_id_type=MESH,
        )

    pair_copies = [
        to_pair(k_ref, k2_ref, 0),
        to_pair(v_ref, v2_ref, 1),
        to_pair(log_send, log_recv, 2),
        to_pair(part_send, part_recv, 3),
    ]
    order = far_first(nz)

    def log_total(own, received):
        biggest = own
        for other in received:
            biggest = jnp.maximum(biggest, other)
        total = jnp.exp2(own - biggest)
        for other in received:
            total = total + jnp.exp2(other - biggest)
        return biggest + jnp.log2(total)

    def plain_total(own, received):
        total = own
        for other in received:
            total = total + other
        return total

    loads[1].wait()
    scaled = scale * k_ref[...].astype(F32)
    high = scaled.astype(BF16)
    k_parts[:, 0:width] = high
    k_parts[:, width:] = (scaled - high.astype(F32)).astype(BF16)
    loads[0].wait()
    block = 2 * LANES
    for b in range(rows // block):
        lanes = slice(b * block, (b + 1) * block)
        q_block = q_ref[lanes, :]
        scores = lax.dot_general(
            k_parts[...],
            jnp.concatenate([q_block, q_block], axis=1),
            (((1,), (1,)), ((), ())),
            preferred_element_type=F32,
        )
        s_ref[:, lanes] = scores
        biggest, summed = None, None
        for jb in range(col_tiles):
            part = scores[jb * LANES : (jb + 1) * LANES].reshape(LANES // 8, 8, block)
            top = jnp.max(part, axis=0)
            total = jnp.sum(jnp.exp2(part - top[None]), axis=0)
            if biggest is None:
                biggest, summed = top, total
            else:
                larger = jnp.maximum(biggest, top)
                summed = summed * jnp.exp2(biggest - larger) + total * jnp.exp2(top - larger)
                biggest = larger
        top = jnp.max(biggest, axis=0, keepdims=True)
        summed = jnp.sum(summed * jnp.exp2(biggest - top), axis=0, keepdims=True)
        local = top + jnp.log2(summed)
        for t in range(block // LANES):
            row_send[pl.ds(b * (block // LANES) + t, 1), :] = local[:, t * LANES : (t + 1) * LANES]

    pl.semaphore_wait(barrier, len(row_peers) + 2 * len(col_peers) + 1)
    send_all(row_send, row_recv, row_ssem.at[0], row_rsem.at[0], row_to)
    pair_copies[0].start()
    loads[2].wait()
    pair_copies[1].start()
    wait_all(row_recv, row_rsem.at[0])
    row_log[...] = -log_total(row_send[...], [row_recv[slot] for slot in range(1, ny)])

    eye = lax.broadcasted_iota(jnp.int32, (LANES, LANES), 0) == lax.broadcasted_iota(
        jnp.int32, (LANES, LANES), 1
    )

    def across(column):
        return jnp.sum(
            jnp.where(eye, jnp.broadcast_to(column, (LANES, LANES)), 0.0), axis=0, keepdims=True
        )

    tiles = [slice(t * LANES, (t + 1) * LANES) for t in range(row_tiles)]
    for jb in range(col_tiles):
        down = slice(jb * LANES, (jb + 1) * LANES)
        biggest = None
        for t in range(row_tiles):
            shifted = s_ref[down, tiles[t]] + row_log[t : t + 1, :]
            s_ref[down, tiles[t]] = shifted
            biggest = shifted if biggest is None else jnp.maximum(biggest, shifted)
        biggest = jnp.max(biggest, axis=1, keepdims=True)
        wide = jnp.broadcast_to(biggest, (LANES, LANES))
        summed = jnp.zeros((LANES, LANES), F32)
        for t in range(row_tiles):
            part = jnp.exp2(s_ref[down, tiles[t]] - wide)
            f_ref[down, tiles[t]] = part.astype(BF16)
            summed = summed + part
        summed = jnp.sum(summed, axis=1, keepdims=True)
        cmax_ref[pl.ds(jb, 1), :] = across(biggest)
        col_send[0, pl.ds(jb, 1), :] = across(biggest + jnp.log2(summed))

    send_all(col_send.at[0], col_recv.at[0], col_ssem.at[0], col_rsem.at[0], col_to)
    for t in range(col_tiles):
        down = slice(t * LANES, (t + 1) * LANES)
        val_lhs[0:width, down] = v_ref[down, :].astype(F32).T.astype(BF16)
        for i in range(row_tiles):
            g_ref[tiles[i], down] = f_ref[down, tiles[i]].T
    wait_all(col_recv.at[0], col_rsem.at[0])
    total = log_total(col_send[0], [col_recv[0, slot] for slot in range(1, nx)])
    log_send[...] = -total
    pair_copies[2].start()
    col_vec[...] = jnp.exp2(cmax_ref[...] - total)

    def for_pair():
        pair_copies[0].wait_recv()
        scaled = scale * k2_ref[...].astype(F32)
        high = scaled.astype(BF16)
        k_parts[:, 0:width] = high
        k_parts[:, width:] = (scaled - high.astype(F32)).astype(BF16)
        pair_copies[1].wait_recv()
        for t in range(col_tiles):
            down = slice(t * LANES, (t + 1) * LANES)
            val_lhs[0:width, cols + t * LANES : cols + (t + 1) * LANES] = (
                v2_ref[down, :].astype(F32).T.astype(BF16)
            )
        pair_copies[2].wait_recv()
        for t in range(col_tiles):
            line = jnp.broadcast_to(log_recv[t : t + 1, :], (LANES, LANES))
            column = jnp.sum(jnp.where(eye, line, 0.0), axis=1, keepdims=True)
            wide_ref[t * LANES : (t + 1) * LANES, :] = jnp.broadcast_to(column, (LANES, LANES))
        for m in range(nz // 2):
            chunks = [lax.rem(z + dz, nz) * 2 + xl for dz in order[2 * m : 2 * m + 2]]
            q_block = jnp.concatenate(
                [q_ref[pl.ds(pl.multiple_of(c * LANES, LANES), LANES), :] for c in chunks], axis=0
            )
            scores = lax.dot_general(
                k_parts[...],
                jnp.concatenate([q_block, q_block], axis=1),
                (((1,), (1,)), ((), ())),
                preferred_element_type=F32,
            )
            for n, c in enumerate(chunks):
                across_lanes = slice((2 * m + n) * LANES, (2 * m + n + 1) * LANES)
                part = scores[:, n * LANES : (n + 1) * LANES] + wide_ref[...]
                pair_ref[cols:, across_lanes] = jnp.exp2(part + row_log[pl.ds(c, 1), :]).astype(BF16)

    def own_half():
        for n, dz in enumerate(order):
            c = lax.rem(z + dz, nz) * 2 + xl
            pair_ref[0:cols, n * LANES : (n + 1) * LANES] = f_ref[
                :, pl.ds(pl.multiple_of(c * LANES, LANES), LANES)
            ]

    def row_step(turn):
        for t in range(col_tiles):
            lhs_row[:, t * LANES : (t + 1) * LANES] = split_lhs(col_vec[t : t + 1, :])
        sums = jnp.sum(
            lax.dot_general(
                lhs_row[...], f_ref[...], (((1,), (0,)), ((), ())), preferred_element_type=F32
            ),
            axis=0,
            keepdims=True,
        )
        for t in range(row_tiles):
            row_vec[pl.ds(t, 1), :] = sums[:, t * LANES : (t + 1) * LANES]
        own = row_vec[...].astype(BF16)
        sum_send[turn - 1] = own
        send_all(
            sum_send.at[turn - 1], sum_recv.at[turn - 1], row_ssem.at[turn], row_rsem.at[turn], row_to
        )
        if turn == 1:
            for_pair()
        wait_all(sum_recv.at[turn - 1], row_rsem.at[turn])
        row_vec[...] = 1.0 / plain_total(
            own.astype(F32), [sum_recv[turn - 1, slot].astype(F32) for slot in range(1, ny)]
        )

    def col_step(turn):
        for t in range(row_tiles):
            lhs_col[:, t * LANES : (t + 1) * LANES] = split_lhs(row_vec[t : t + 1, :])
        sums = jnp.sum(
            lax.dot_general(
                lhs_col[...], g_ref[...], (((1,), (0,)), ((), ())), preferred_element_type=F32
            ),
            axis=0,
            keepdims=True,
        )
        for t in range(col_tiles):
            col_send[turn, pl.ds(t, 1), :] = (
                sums[:, t * LANES : (t + 1) * LANES] * col_vec[t : t + 1, :]
            )
        send_all(
            col_send.at[turn], col_recv.at[turn], col_ssem.at[turn], col_rsem.at[turn], col_to
        )
        if turn == 1:
            own_half()
        if turn == SWEEPS - 1:
            send_all(col_send.at[turn], side_recv, side_sem.at[0], side_sem.at[1], side_to)
        wait_all(col_recv.at[turn], col_rsem.at[turn])
        inverse = 1.0 / plain_total(
            col_send[turn], [col_recv[turn, slot] for slot in range(1, nx)]
        )
        col_vec[...] = col_vec[...] * inverse
        if turn == 1:
            part_send[...] = inverse
            pair_copies[3].start()

    for turn in range(1, SWEEPS):
        row_step(turn)
        col_step(turn)

    pltpu.make_async_copy(side_recv, side_recv, side_sem.at[1]).wait()
    pair_copies[3].wait_recv()
    side = part_recv[...] / plain_total(side_recv[0], [side_recv[slot] for slot in range(1, nx)])
    for t in range(2 * col_tiles):
        lanes = slice(t * LANES, (t + 1) * LANES)
        if t < col_tiles:
            line = col_vec[t : t + 1, :]
        else:
            line = side[t - col_tiles : t - col_tiles + 1, :]
        val_lhs[0:width, lanes] = (val_lhs[0:width, lanes].astype(F32) * line).astype(BF16)
        val_lhs[width : width + 16, lanes] = split_lhs(line)
    tail = lax.broadcasted_iota(jnp.int32, (16, LANES), 0)

    def product(m):
        return jnp.dot(
            val_lhs[...],
            pair_ref[:, m * 2 * LANES : (m + 1) * 2 * LANES],
            preferred_element_type=F32,
        )

    ahead = product(0)
    for m in range(nz // 2):
        both = ahead
        if m + 1 < nz // 2:
            ahead = product(m + 1)
        for x in range(2):
            dz = order[2 * m + x]
            piece = both[:, x * LANES : (x + 1) * LANES]
            out_send[dz, 0:width, :] = piece[0:width].astype(BF16)
            weight = jnp.sum(piece[width:], axis=0, keepdims=True)
            high = weight.astype(BF16).astype(F32)
            out_send[dz, width : width + 16, :] = jnp.where(
                tail == 0, high, jnp.where(tail == 1, weight - high, 0.0)
            ).astype(BF16)
            if dz != 0:
                pltpu.make_async_remote_copy(
                    src_ref=out_send.at[dz],
                    dst_ref=out_recv.at[dz],
                    send_sem=out_sem.at[0],
                    recv_sem=out_sem.at[1],
                    device_id={"gy": row_peer(dz, 0)},
                    device_id_type=MESH,
                ).start()
    wait_all(out_recv, out_sem.at[1])
    total = out_send[0].astype(F32)
    for slot in range(1, nz):
        total = total + out_recv[slot].astype(F32)
    weight = jnp.sum(total[width:], axis=0, keepdims=True)
    head = (total[0:width] / weight).T.astype(BF16)
    head_send[...] = head
    swap = pltpu.make_async_remote_copy(
        src_ref=head_send,
        dst_ref=head_recv,
        send_sem=head_sem.at[0],
        recv_sem=head_sem.at[1],
        device_id={"gz": 1 - gz},
        device_id_type=MESH,
    )
    swap.start()
    out_ref[:, pl.ds(pl.multiple_of(gz * width, width), width)] = head
    wait_all(row_recv, row_ssem.at[0])
    wait_all(col_recv.at[0], col_ssem.at[0])
    for turn in range(1, SWEEPS):
        wait_all(sum_recv.at[turn - 1], row_ssem.at[turn])
        wait_all(col_recv.at[turn], col_ssem.at[turn])
    wait_all(out_recv, out_sem.at[0])
    pltpu.make_async_copy(side_recv, side_recv, side_sem.at[0]).wait()
    for copy in pair_copies:
        copy.wait_send()
    swap.wait()
    out_ref[:, pl.ds(pl.multiple_of((1 - gz) * width, width), width)] = head_recv[...]


def solution(mesh):
    nx, ny = mesh.shape["gx"], mesh.shape["gy"]

    def body(queries, keys, values, w_out):
        _, rows, width = queries.shape
        cols = keys.shape[1]
        columns = w_out.shape[1] // lax.axis_size("gz")
        row_tiles, col_tiles = rows // LANES, cols // LANES
        anywhere = pl.BlockSpec(memory_space=pltpu.HBM)
        dma = pltpu.SemaphoreType.DMA
        heads = pl.pallas_call(
            functools.partial(kernel, (nx, ny)),
            out_shape=jax.ShapeDtypeStruct((rows // ny, 2 * width), BF16),
            in_specs=[anywhere] * 3,
            out_specs=pl.BlockSpec(memory_space=pltpu.VMEM),
            scratch_shapes=[
                pltpu.VMEM((rows, width), BF16),
                pltpu.VMEM((cols, width), BF16),
                pltpu.VMEM((cols, width), BF16),
                pltpu.VMEM((cols, 2 * width), BF16),
                pltpu.VMEM((cols, rows), F32),
                pltpu.VMEM((cols, rows), BF16),
                pltpu.VMEM((rows, cols), BF16),
                pltpu.VMEM((16, cols), BF16),
                pltpu.VMEM((16, rows), BF16),
                pltpu.VMEM((width + 16, 2 * cols), BF16),
                pltpu.VMEM((cols, width), BF16),
                pltpu.VMEM((cols, width), BF16),
                pltpu.VMEM((2 * cols, rows // 2), BF16),
                pltpu.VMEM((cols, LANES), F32),
                pltpu.VMEM((row_tiles, LANES), F32),
                pltpu.VMEM((col_tiles, LANES), F32),
                pltpu.VMEM((col_tiles, LANES), F32),
                pltpu.VMEM((col_tiles, LANES), F32),
                pltpu.VMEM((col_tiles, LANES), F32),
                pltpu.VMEM((nx, col_tiles, LANES), F32),
                pltpu.VMEM((col_tiles, LANES), F32),
                pltpu.VMEM((row_tiles, LANES), F32),
                pltpu.VMEM((ny, row_tiles, LANES), F32),
                pltpu.VMEM((SWEEPS - 1, row_tiles, LANES), BF16),
                pltpu.VMEM((SWEEPS - 1, ny, row_tiles, LANES), BF16),
                pltpu.VMEM((SWEEPS, col_tiles, LANES), F32),
                pltpu.VMEM((SWEEPS, nx, col_tiles, LANES), F32),
                pltpu.VMEM((row_tiles, LANES), F32),
                pltpu.VMEM((col_tiles, LANES), F32),
                pltpu.VMEM((ny // 2, width + 16, LANES), BF16),
                pltpu.VMEM((ny // 2, width + 16, LANES), BF16),
                pltpu.VMEM((LANES, width), BF16),
                pltpu.VMEM((LANES, width), BF16),
                dma((3,)),
                dma((SWEEPS,)),
                dma((SWEEPS,)),
                dma((SWEEPS,)),
                dma((SWEEPS,)),
                dma((2,)),
                dma((2,)),
                dma((4,)),
                dma((4,)),
                dma((2,)),
            ],
            compiler_params=pltpu.CompilerParams(
                collective_id=0, has_side_effects=True, vmem_limit_bytes=44 * 1024 * 1024
            ),
        )(*(pltpu.with_memory_space_constraint(x, pltpu.HBM) for x in (queries.reshape(rows, width), keys.reshape(cols, width), values.reshape(cols, width))))
        w_columns = lax.dynamic_slice_in_dim(
            w_out, lax.axis_index("gz") * columns, columns, 1
        )
        return jnp.dot(heads, w_columns, preferred_element_type=F32).astype(BF16)

    return jax.shard_map(
        body,
        mesh=mesh,
        in_specs=(P("gz", "gx", None), P("gz", "gy", None), P("gz", "gy", None), P()),
        out_specs=P(("gx", "gy"), "gz"),
        check_vma=False,
    )
```

```python
import functools
import math

import jax
import jax.numpy as jnp
from jax import lax
from jax.experimental import pallas as pl
from jax.experimental.pallas import tpu as pltpu
from jax.sharding import PartitionSpec as P

SWEEPS = 3
LANES = 128
MESH = pl.DeviceIdType.MESH
F32 = jnp.float32
BF16 = jnp.bfloat16


def far_first(count):
    return sorted(range(count), key=lambda d: -min(d, count - d))


def split_lhs(x):
    rows = jnp.broadcast_to(x, (16, x.shape[1]))
    hi = rows.astype(BF16).astype(F32)
    rest = rows - hi
    mid = rest.astype(BF16).astype(F32)
    lo = rest - mid
    at = lax.broadcasted_iota(jnp.int32, rows.shape, 0)
    parts = jnp.where(at == 0, hi, jnp.where(at == 1, mid, jnp.where(at == 2, lo, 0.0)))
    return parts.astype(BF16)


def kernel(
    sizes,
    q_hbm,
    k_hbm,
    v_hbm,
    out_ref,
    q_ref,
    k_ref,
    v_ref,
    k_parts,
    s_ref,
    f_ref,
    g_ref,
    lhs_row,
    lhs_col,
    val_lhs,
    k2_ref,
    v2_ref,
    pair_ref,
    wide_ref,
    row_log,
    log_send,
    log_recv,
    part_send,
    part_recv,
    side_recv,
    cmax_ref,
    row_send,
    row_recv,
    sum_send,
    sum_recv,
    col_send,
    col_recv,
    row_vec,
    col_vec,
    out_send,
    out_recv,
    head_send,
    head_recv,
    load_sem,
    row_ssem,
    row_rsem,
    col_ssem,
    col_rsem,
    out_sem,
    head_sem,
    pair_ssem,
    pair_rsem,
    side_sem,
):
    nx, ny = sizes
    rows, width = q_ref.shape
    cols = k_ref.shape[0]
    row_tiles, col_tiles = rows // LANES, cols // LANES
    nz = ny // 2
    gz, gx, gy = lax.axis_index("gz"), lax.axis_index("gx"), lax.axis_index("gy")
    z, xl = gy // 2, lax.rem(gy, 2)
    y, xh = gx // 2, lax.rem(gx, 2)
    scale = math.log2(math.e) / math.sqrt(width)

    row_peers = [(dz, dx) for dz in far_first(nz) for dx in (1, 0) if (dz, dx) != (0, 0)]
    col_peers = [(dy, dx) for dy in far_first(nx // 2) for dx in (1, 0) if (dy, dx) != (0, 0)]

    def row_peer(dz, dx):
        return lax.rem(z + dz, nz) * 2 + lax.rem(xl + dx, 2)

    def col_peer(dy, dx):
        return lax.rem(y + dy, nx // 2) * 2 + lax.rem(xh + dx, 2)

    loads = [
        pltpu.make_async_copy(q_hbm, q_ref, load_sem.at[0]),
        pltpu.make_async_copy(k_hbm, k_ref, load_sem.at[1]),
        pltpu.make_async_copy(v_hbm, v_ref, load_sem.at[2]),
    ]
    for load in loads:
        load.start()

    barrier = pltpu.get_barrier_semaphore()
    for dz, dx in row_peers:
        pl.semaphore_signal(
            barrier, inc=1, device_id={"gy": row_peer(dz, dx)}, device_id_type=MESH
        )
    for dy, dx in col_peers:
        pl.semaphore_signal(
            barrier, inc=1, device_id={"gx": col_peer(dy, dx)}, device_id_type=MESH
        )
    pl.semaphore_signal(barrier, inc=1, device_id={"gz": 1 - gz}, device_id_type=MESH)
    beside = z * 2 + 1 - xl
    for dy, dx in col_peers:
        pl.semaphore_signal(
            barrier,
            inc=1,
            device_id={"gx": col_peer(dy, dx), "gy": beside},
            device_id_type=MESH,
        )

    def send_all(source, target, ssem, rsem, peers):
        for slot, device in peers:
            pltpu.make_async_remote_copy(
                src_ref=source,
                dst_ref=target.at[slot],
                send_sem=ssem,
                recv_sem=rsem,
                device_id=device,
                device_id_type=MESH,
            ).start()

    def wait_all(target, sem):
        everything = target.at[pl.ds(1, target.shape[0] - 1)]
        pltpu.make_async_copy(everything, everything, sem).wait()

    row_to = [(dz * 2 + dx, {"gy": row_peer(dz, dx)}) for dz, dx in row_peers]
    col_to = [(dy * 2 + dx, {"gx": col_peer(dy, dx)}) for dy, dx in col_peers]
    side_to = [
        (dy * 2 + dx, {"gx": col_peer(dy, dx), "gy": beside}) for dy, dx in [*col_peers, (0, 0)]
    ]

    def to_pair(source, target, number):
        return pltpu.make_async_remote_copy(
            src_ref=source,
            dst_ref=target,
            send_sem=pair_ssem.at[number],
            recv_sem=pair_rsem.at[number],
            device_id={"gy": beside},
            device_id_type=MESH,
        )

    half = cols // 2
    halves = [pl.ds(0, half), pl.ds(half, half)]
    pair_keys = [to_pair(k_ref.at[h], k2_ref.at[h], n) for n, h in enumerate(halves)]
    pair_values = [to_pair(v_ref.at[h], v2_ref.at[h], 2 + n) for n, h in enumerate(halves)]
    pair_log = to_pair(log_send, log_recv, 4)
    pair_part = to_pair(part_send, part_recv, 5)
    order = far_first(nz)

    def log_total(own, received):
        biggest = own
        for other in received:
            biggest = jnp.maximum(biggest, other)
        total = jnp.exp2(own - biggest)
        for other in received:
            total = total + jnp.exp2(other - biggest)
        return biggest + jnp.log2(total)

    def plain_total(own, received):
        total = own
        for other in received:
            total = total + other
        return total

    loads[1].wait()
    scaled = scale * k_ref[...].astype(F32)
    high = scaled.astype(BF16)
    k_parts[:, 0:width] = high
    k_parts[:, width:] = (scaled - high.astype(F32)).astype(BF16)
    loads[0].wait()
    block = 2 * LANES
    for b in range(rows // block):
        lanes = slice(b * block, (b + 1) * block)
        q_block = q_ref[lanes, :]
        scores = lax.dot_general(
            k_parts[...],
            jnp.concatenate([q_block, q_block], axis=1),
            (((1,), (1,)), ((), ())),
            preferred_element_type=F32,
        )
        s_ref[:, lanes] = scores
        biggest, summed = None, None
        for jb in range(col_tiles):
            part = scores[jb * LANES : (jb + 1) * LANES].reshape(LANES // 8, 8, block)
            top = jnp.max(part, axis=0)
            total = jnp.sum(jnp.exp2(part - top[None]), axis=0)
            if biggest is None:
                biggest, summed = top, total
            else:
                larger = jnp.maximum(biggest, top)
                summed = summed * jnp.exp2(biggest - larger) + total * jnp.exp2(top - larger)
                biggest = larger
        top = jnp.max(biggest, axis=0, keepdims=True)
        summed = jnp.sum(summed * jnp.exp2(biggest - top), axis=0, keepdims=True)
        local = top + jnp.log2(summed)
        for t in range(block // LANES):
            row_send[pl.ds(b * (block // LANES) + t, 1), :] = local[:, t * LANES : (t + 1) * LANES]

    pl.semaphore_wait(barrier, len(row_peers) + 2 * len(col_peers) + 1)
    send_all(row_send, row_recv, row_ssem.at[0], row_rsem.at[0], row_to)
    pair_keys[0].start()
    loads[2].wait()
    wait_all(row_recv, row_rsem.at[0])
    row_log[...] = -log_total(row_send[...], [row_recv[slot] for slot in range(1, ny)])

    eye = lax.broadcasted_iota(jnp.int32, (LANES, LANES), 0) == lax.broadcasted_iota(
        jnp.int32, (LANES, LANES), 1
    )

    def across(column):
        return jnp.sum(
            jnp.where(eye, jnp.broadcast_to(column, (LANES, LANES)), 0.0), axis=0, keepdims=True
        )

    tiles = [slice(t * LANES, (t + 1) * LANES) for t in range(row_tiles)]
    for jb in range(col_tiles):
        down = slice(jb * LANES, (jb + 1) * LANES)
        biggest = None
        for t in range(row_tiles):
            shifted = s_ref[down, tiles[t]] + row_log[t : t + 1, :]
            s_ref[down, tiles[t]] = shifted
            biggest = shifted if biggest is None else jnp.maximum(biggest, shifted)
        biggest = jnp.max(biggest, axis=1, keepdims=True)
        wide = jnp.broadcast_to(biggest, (LANES, LANES))
        summed = jnp.zeros((LANES, LANES), F32)
        for t in range(row_tiles):
            part = jnp.exp2(s_ref[down, tiles[t]] - wide)
            f_ref[down, tiles[t]] = part.astype(BF16)
            summed = summed + part
        summed = jnp.sum(summed, axis=1, keepdims=True)
        cmax_ref[pl.ds(jb, 1), :] = across(biggest)
        col_send[0, pl.ds(jb, 1), :] = across(biggest + jnp.log2(summed))

    send_all(col_send.at[0], col_recv.at[0], col_ssem.at[0], col_rsem.at[0], col_to)
    pair_keys[1].start()
    for t in range(col_tiles):
        down = slice(t * LANES, (t + 1) * LANES)
        val_lhs[0:width, down] = v_ref[down, :].astype(F32).T.astype(BF16)
        for i in range(row_tiles):
            g_ref[tiles[i], down] = f_ref[down, tiles[i]].T
    wait_all(col_recv.at[0], col_rsem.at[0])
    total = log_total(col_send[0], [col_recv[0, slot] for slot in range(1, nx)])
    log_send[...] = -total
    pair_log.start()
    col_vec[...] = jnp.exp2(cmax_ref[...] - total)

    def for_pair():
        pair_keys[0].wait_recv()
        pair_keys[1].wait_recv()
        scaled = scale * k2_ref[...].astype(F32)
        high = scaled.astype(BF16)
        k_parts[:, 0:width] = high
        k_parts[:, width:] = (scaled - high.astype(F32)).astype(BF16)
        pair_log.wait_recv()
        for t in range(col_tiles):
            line = jnp.broadcast_to(log_recv[t : t + 1, :], (LANES, LANES))
            column = jnp.sum(jnp.where(eye, line, 0.0), axis=1, keepdims=True)
            wide_ref[t * LANES : (t + 1) * LANES, :] = jnp.broadcast_to(column, (LANES, LANES))
        for m in range(nz // 2):
            chunks = [lax.rem(z + dz, nz) * 2 + xl for dz in order[2 * m : 2 * m + 2]]
            q_block = jnp.concatenate(
                [q_ref[pl.ds(pl.multiple_of(c * LANES, LANES), LANES), :] for c in chunks], axis=0
            )
            scores = lax.dot_general(
                k_parts[...],
                jnp.concatenate([q_block, q_block], axis=1),
                (((1,), (1,)), ((), ())),
                preferred_element_type=F32,
            )
            for n, c in enumerate(chunks):
                across_lanes = slice((2 * m + n) * LANES, (2 * m + n + 1) * LANES)
                part = scores[:, n * LANES : (n + 1) * LANES] + wide_ref[...]
                pair_ref[cols:, across_lanes] = jnp.exp2(part + row_log[pl.ds(c, 1), :]).astype(BF16)

    def values_of_pair():
        pair_values[0].wait_recv()
        pair_values[1].wait_recv()
        for t in range(col_tiles):
            down = slice(t * LANES, (t + 1) * LANES)
            val_lhs[0:width, cols + t * LANES : cols + (t + 1) * LANES] = (
                v2_ref[down, :].astype(F32).T.astype(BF16)
            )

    def own_half():
        for n, dz in enumerate(order):
            c = lax.rem(z + dz, nz) * 2 + xl
            pair_ref[0:cols, n * LANES : (n + 1) * LANES] = f_ref[
                :, pl.ds(pl.multiple_of(c * LANES, LANES), LANES)
            ]

    def row_step(turn):
        for t in range(col_tiles):
            lhs_row[:, t * LANES : (t + 1) * LANES] = split_lhs(col_vec[t : t + 1, :])
        sums = jnp.sum(
            lax.dot_general(
                lhs_row[...], f_ref[...], (((1,), (0,)), ((), ())), preferred_element_type=F32
            ),
            axis=0,
            keepdims=True,
        )
        for t in range(row_tiles):
            row_vec[pl.ds(t, 1), :] = sums[:, t * LANES : (t + 1) * LANES]
        own = row_vec[...].astype(BF16)
        sum_send[turn - 1] = own
        send_all(
            sum_send.at[turn - 1], sum_recv.at[turn - 1], row_ssem.at[turn], row_rsem.at[turn], row_to
        )
        if turn == 1:
            pair_values[0].start()
            for_pair()
        else:
            values_of_pair()
        wait_all(sum_recv.at[turn - 1], row_rsem.at[turn])
        row_vec[...] = 1.0 / plain_total(
            own.astype(F32), [sum_recv[turn - 1, slot].astype(F32) for slot in range(1, ny)]
        )

    def col_step(turn):
        for t in range(row_tiles):
            lhs_col[:, t * LANES : (t + 1) * LANES] = split_lhs(row_vec[t : t + 1, :])
        sums = jnp.sum(
            lax.dot_general(
                lhs_col[...], g_ref[...], (((1,), (0,)), ((), ())), preferred_element_type=F32
            ),
            axis=0,
            keepdims=True,
        )
        for t in range(col_tiles):
            col_send[turn, pl.ds(t, 1), :] = (
                sums[:, t * LANES : (t + 1) * LANES] * col_vec[t : t + 1, :]
            )
        send_all(
            col_send.at[turn], col_recv.at[turn], col_ssem.at[turn], col_rsem.at[turn], col_to
        )
        if turn == 1:
            pair_values[1].start()
            own_half()
        if turn == SWEEPS - 1:
            send_all(col_send.at[turn], side_recv, side_sem.at[0], side_sem.at[1], side_to)
        wait_all(col_recv.at[turn], col_rsem.at[turn])
        inverse = 1.0 / plain_total(
            col_send[turn], [col_recv[turn, slot] for slot in range(1, nx)]
        )
        col_vec[...] = col_vec[...] * inverse
        if turn == 1:
            part_send[...] = inverse
            pair_part.start()

    for turn in range(1, SWEEPS):
        row_step(turn)
        col_step(turn)

    pltpu.make_async_copy(side_recv, side_recv, side_sem.at[1]).wait()
    pair_part.wait_recv()
    side = part_recv[...] / plain_total(side_recv[0], [side_recv[slot] for slot in range(1, nx)])
    for t in range(2 * col_tiles):
        lanes = slice(t * LANES, (t + 1) * LANES)
        if t < col_tiles:
            line = col_vec[t : t + 1, :]
        else:
            line = side[t - col_tiles : t - col_tiles + 1, :]
        val_lhs[0:width, lanes] = (val_lhs[0:width, lanes].astype(F32) * line).astype(BF16)
        val_lhs[width : width + 16, lanes] = split_lhs(line)
    tail = lax.broadcasted_iota(jnp.int32, (16, LANES), 0)

    def product(m):
        return jnp.dot(
            val_lhs[...],
            pair_ref[:, m * 2 * LANES : (m + 1) * 2 * LANES],
            preferred_element_type=F32,
        )

    ahead = product(0)
    for m in range(nz // 2):
        both = ahead
        if m + 1 < nz // 2:
            ahead = product(m + 1)
        for x in range(2):
            dz = order[2 * m + x]
            piece = both[:, x * LANES : (x + 1) * LANES]
            out_send[dz, 0:width, :] = piece[0:width].astype(BF16)
            weight = jnp.sum(piece[width:], axis=0, keepdims=True)
            high = weight.astype(BF16).astype(F32)
            out_send[dz, width : width + 16, :] = jnp.where(
                tail == 0, high, jnp.where(tail == 1, weight - high, 0.0)
            ).astype(BF16)
            if dz != 0:
                pltpu.make_async_remote_copy(
                    src_ref=out_send.at[dz],
                    dst_ref=out_recv.at[dz],
                    send_sem=out_sem.at[0],
                    recv_sem=out_sem.at[1],
                    device_id={"gy": row_peer(dz, 0)},
                    device_id_type=MESH,
                ).start()
    wait_all(out_recv, out_sem.at[1])
    total = out_send[0].astype(F32)
    for slot in range(1, nz):
        total = total + out_recv[slot].astype(F32)
    weight = jnp.sum(total[width:], axis=0, keepdims=True)
    head = (total[0:width] / weight).T.astype(BF16)
    head_send[...] = head
    swap = pltpu.make_async_remote_copy(
        src_ref=head_send,
        dst_ref=head_recv,
        send_sem=head_sem.at[0],
        recv_sem=head_sem.at[1],
        device_id={"gz": 1 - gz},
        device_id_type=MESH,
    )
    swap.start()
    out_ref[:, pl.ds(pl.multiple_of(gz * width, width), width)] = head
    wait_all(row_recv, row_ssem.at[0])
    wait_all(col_recv.at[0], col_ssem.at[0])
    for turn in range(1, SWEEPS):
        wait_all(sum_recv.at[turn - 1], row_ssem.at[turn])
        wait_all(col_recv.at[turn], col_ssem.at[turn])
    wait_all(out_recv, out_sem.at[0])
    pltpu.make_async_copy(side_recv, side_recv, side_sem.at[0]).wait()
    for copy in [*pair_keys, *pair_values, pair_log, pair_part]:
        copy.wait_send()
    swap.wait()
    out_ref[:, pl.ds(pl.multiple_of((1 - gz) * width, width), width)] = head_recv[...]


def solution(mesh):
    nx, ny = mesh.shape["gx"], mesh.shape["gy"]

    def body(queries, keys, values, w_out):
        _, rows, width = queries.shape
        cols = keys.shape[1]
        columns = w_out.shape[1] // lax.axis_size("gz")
        row_tiles, col_tiles = rows // LANES, cols // LANES
        anywhere = pl.BlockSpec(memory_space=pltpu.HBM)
        dma = pltpu.SemaphoreType.DMA
        heads = pl.pallas_call(
            functools.partial(kernel, (nx, ny)),
            out_shape=jax.ShapeDtypeStruct((rows // ny, 2 * width), BF16),
            in_specs=[anywhere] * 3,
            out_specs=pl.BlockSpec(memory_space=pltpu.VMEM),
            scratch_shapes=[
                pltpu.VMEM((rows, width), BF16),
                pltpu.VMEM((cols, width), BF16),
                pltpu.VMEM((cols, width), BF16),
                pltpu.VMEM((cols, 2 * width), BF16),
                pltpu.VMEM((cols, rows), F32),
                pltpu.VMEM((cols, rows), BF16),
                pltpu.VMEM((rows, cols), BF16),
                pltpu.VMEM((16, cols), BF16),
                pltpu.VMEM((16, rows), BF16),
                pltpu.VMEM((width + 16, 2 * cols), BF16),
                pltpu.VMEM((cols, width), BF16),
                pltpu.VMEM((cols, width), BF16),
                pltpu.VMEM((2 * cols, rows // 2), BF16),
                pltpu.VMEM((cols, LANES), F32),
                pltpu.VMEM((row_tiles, LANES), F32),
                pltpu.VMEM((col_tiles, LANES), F32),
                pltpu.VMEM((col_tiles, LANES), F32),
                pltpu.VMEM((col_tiles, LANES), F32),
                pltpu.VMEM((col_tiles, LANES), F32),
                pltpu.VMEM((nx, col_tiles, LANES), F32),
                pltpu.VMEM((col_tiles, LANES), F32),
                pltpu.VMEM((row_tiles, LANES), F32),
                pltpu.VMEM((ny, row_tiles, LANES), F32),
                pltpu.VMEM((SWEEPS - 1, row_tiles, LANES), BF16),
                pltpu.VMEM((SWEEPS - 1, ny, row_tiles, LANES), BF16),
                pltpu.VMEM((SWEEPS, col_tiles, LANES), F32),
                pltpu.VMEM((SWEEPS, nx, col_tiles, LANES), F32),
                pltpu.VMEM((row_tiles, LANES), F32),
                pltpu.VMEM((col_tiles, LANES), F32),
                pltpu.VMEM((ny // 2, width + 16, LANES), BF16),
                pltpu.VMEM((ny // 2, width + 16, LANES), BF16),
                pltpu.VMEM((LANES, width), BF16),
                pltpu.VMEM((LANES, width), BF16),
                dma((3,)),
                dma((SWEEPS,)),
                dma((SWEEPS,)),
                dma((SWEEPS,)),
                dma((SWEEPS,)),
                dma((2,)),
                dma((2,)),
                dma((6,)),
                dma((6,)),
                dma((2,)),
            ],
            compiler_params=pltpu.CompilerParams(
                collective_id=0, has_side_effects=True, vmem_limit_bytes=44 * 1024 * 1024
            ),
        )(
            *(
                pltpu.with_memory_space_constraint(x.reshape(-1, width), pltpu.HBM)
                for x in (queries, keys, values)
            )
        )
        w_columns = lax.dynamic_slice_in_dim(
            w_out, lax.axis_index("gz") * columns, columns, 1
        )
        return jnp.dot(heads, w_columns, preferred_element_type=F32).astype(BF16)

    return jax.shard_map(
        body,
        mesh=mesh,
        in_specs=(P("gz", "gx", None), P("gz", "gy", None), P("gz", "gy", None), P()),
        out_specs=P(("gx", "gy"), "gz"),
        check_vma=False,
    )
```

```python
import functools
import math

import jax
import jax.numpy as jnp
from jax import lax
from jax.experimental import pallas as pl
from jax.experimental.pallas import tpu as pltpu
from jax.sharding import PartitionSpec as P

SWEEPS = 3
LANES = 128
MESH = pl.DeviceIdType.MESH
F32 = jnp.float32
BF16 = jnp.bfloat16


def far_first(count):
    return sorted(range(count), key=lambda d: -min(d, count - d))


def split_lhs(x):
    rows = jnp.broadcast_to(x, (16, x.shape[1]))
    hi = rows.astype(BF16).astype(F32)
    rest = rows - hi
    mid = rest.astype(BF16).astype(F32)
    lo = rest - mid
    at = lax.broadcasted_iota(jnp.int32, rows.shape, 0)
    parts = jnp.where(at == 0, hi, jnp.where(at == 1, mid, jnp.where(at == 2, lo, 0.0)))
    return parts.astype(BF16)


def kernel(
    sizes,
    q_hbm,
    k_hbm,
    v_hbm,
    out_ref,
    q_ref,
    k_ref,
    v_ref,
    k_parts,
    s_ref,
    f_ref,
    g_ref,
    lhs_row,
    lhs_col,
    val_lhs,
    k2_ref,
    v2_ref,
    pair_ref,
    wide_ref,
    row_log,
    log_send,
    log_recv,
    part_send,
    part_recv,
    side_recv,
    cmax_ref,
    row_send,
    row_recv,
    sum_send,
    sum_recv,
    col_send,
    col_recv,
    row_vec,
    col_vec,
    out_send,
    out_recv,
    head_send,
    head_recv,
    load_sem,
    row_ssem,
    row_rsem,
    col_ssem,
    col_rsem,
    out_sem,
    head_sem,
    pair_ssem,
    pair_rsem,
    side_sem,
):
    nx, ny = sizes
    rows, width = q_ref.shape
    cols = k_ref.shape[0]
    row_tiles, col_tiles = rows // LANES, cols // LANES
    nz = ny // 2
    gz, gx, gy = lax.axis_index("gz"), lax.axis_index("gx"), lax.axis_index("gy")
    z, xl = gy // 2, lax.rem(gy, 2)
    y, xh = gx // 2, lax.rem(gx, 2)
    scale = math.log2(math.e) / math.sqrt(width)

    row_peers = [(dz, dx) for dz in far_first(nz) for dx in (1, 0) if (dz, dx) != (0, 0)]
    col_peers = [(dy, dx) for dy in far_first(nx // 2) for dx in (1, 0) if (dy, dx) != (0, 0)]

    def row_peer(dz, dx):
        return lax.rem(z + dz, nz) * 2 + lax.rem(xl + dx, 2)

    def col_peer(dy, dx):
        return lax.rem(y + dy, nx // 2) * 2 + lax.rem(xh + dx, 2)

    loads = [
        pltpu.make_async_copy(q_hbm, q_ref, load_sem.at[0]),
        pltpu.make_async_copy(k_hbm, k_parts.at[:, pl.ds(0, width)], load_sem.at[1]),
        pltpu.make_async_copy(v_hbm, v_ref, load_sem.at[2]),
        pltpu.make_async_copy(k_hbm, k_parts.at[:, pl.ds(width, width)], load_sem.at[3]),
        pltpu.make_async_copy(k_hbm, k_ref, load_sem.at[4]),
    ]
    for n in (1, 3, 0, 4, 2):
        loads[n].start()

    barrier = pltpu.get_barrier_semaphore()
    for dz, dx in row_peers:
        pl.semaphore_signal(
            barrier, inc=1, device_id={"gy": row_peer(dz, dx)}, device_id_type=MESH
        )
    for dy, dx in col_peers:
        pl.semaphore_signal(
            barrier, inc=1, device_id={"gx": col_peer(dy, dx)}, device_id_type=MESH
        )
    pl.semaphore_signal(barrier, inc=1, device_id={"gz": 1 - gz}, device_id_type=MESH)
    beside = z * 2 + 1 - xl
    for dy, dx in col_peers:
        pl.semaphore_signal(
            barrier,
            inc=1,
            device_id={"gx": col_peer(dy, dx), "gy": beside},
            device_id_type=MESH,
        )

    def send_all(source, target, ssem, rsem, peers):
        for slot, device in peers:
            pltpu.make_async_remote_copy(
                src_ref=source,
                dst_ref=target.at[slot],
                send_sem=ssem,
                recv_sem=rsem,
                device_id=device,
                device_id_type=MESH,
            ).start()

    def wait_all(target, sem):
        everything = target.at[pl.ds(1, target.shape[0] - 1)]
        pltpu.make_async_copy(everything, everything, sem).wait()

    row_to = [(dz * 2 + dx, {"gy": row_peer(dz, dx)}) for dz, dx in row_peers]
    col_to = [(dy * 2 + dx, {"gx": col_peer(dy, dx)}) for dy, dx in col_peers]
    side_to = [
        (dy * 2 + dx, {"gx": col_peer(dy, dx), "gy": beside}) for dy, dx in [*col_peers, (0, 0)]
    ]

    def to_pair(source, target, number):
        return pltpu.make_async_remote_copy(
            src_ref=source,
            dst_ref=target,
            send_sem=pair_ssem.at[number],
            recv_sem=pair_rsem.at[number],
            device_id={"gy": beside},
            device_id_type=MESH,
        )

    half = cols // 2
    halves = [pl.ds(0, half), pl.ds(half, half)]
    pair_keys = [to_pair(k_ref.at[h], k2_ref.at[h], n) for n, h in enumerate(halves)]
    pair_values = [to_pair(v_ref.at[h], v2_ref.at[h], 2 + n) for n, h in enumerate(halves)]
    pair_log = to_pair(log_send, log_recv, 4)
    pair_part = to_pair(part_send, part_recv, 5)

    def ranked(n):
        return jnp.where(n < nz // 2, n, nz + nz // 2 - 1 - n)

    targets = [ranked(jnp.where(n >= ranked(z), n + 1, n)) for n in range(nz - 1)] + [z]

    def log_total(own, received):
        biggest = own
        for other in received:
            biggest = jnp.maximum(biggest, other)
        total = jnp.exp2(own - biggest)
        for other in received:
            total = total + jnp.exp2(other - biggest)
        return biggest + jnp.log2(total)

    def plain_total(own, received):
        total = own
        for other in received:
            total = total + other
        return total

    loads[1].wait()
    loads[3].wait()
    loads[0].wait()

    def scaled_parts(x):
        scaled = scale * x.astype(F32)
        high = scaled.astype(BF16)
        return jnp.concatenate([high, (scaled - high.astype(F32)).astype(BF16)], axis=1)

    block = 2 * LANES
    for b in range(rows // block):
        lanes = slice(b * block, (b + 1) * block)
        scores = lax.dot_general(
            k_parts[...],
            scaled_parts(q_ref[lanes, :]),
            (((1,), (1,)), ((), ())),
            preferred_element_type=F32,
        )
        s_ref[:, lanes] = scores
        biggest, summed = None, None
        for jb in range(col_tiles):
            part = scores[jb * LANES : (jb + 1) * LANES].reshape(LANES // 8, 8, block)
            top = jnp.max(part, axis=0)
            total = jnp.sum(jnp.exp2(part - top[None]), axis=0)
            if biggest is None:
                biggest, summed = top, total
            else:
                larger = jnp.maximum(biggest, top)
                summed = summed * jnp.exp2(biggest - larger) + total * jnp.exp2(top - larger)
                biggest = larger
        top = jnp.max(biggest, axis=0, keepdims=True)
        summed = jnp.sum(summed * jnp.exp2(biggest - top), axis=0, keepdims=True)
        local = top + jnp.log2(summed)
        for t in range(block // LANES):
            row_send[pl.ds(b * (block // LANES) + t, 1), :] = local[:, t * LANES : (t + 1) * LANES]

    pl.semaphore_wait(barrier, len(row_peers) + 2 * len(col_peers) + 1)
    send_all(row_send, row_recv, row_ssem.at[0], row_rsem.at[0], row_to)
    loads[4].wait()
    pair_keys[0].start()
    loads[2].wait()
    wait_all(row_recv, row_rsem.at[0])
    row_log[...] = -log_total(row_send[...], [row_recv[slot] for slot in range(1, ny)])

    eye = lax.broadcasted_iota(jnp.int32, (LANES, LANES), 0) == lax.broadcasted_iota(
        jnp.int32, (LANES, LANES), 1
    )

    def across(column):
        return jnp.sum(
            jnp.where(eye, jnp.broadcast_to(column, (LANES, LANES)), 0.0), axis=0, keepdims=True
        )

    tiles = [slice(t * LANES, (t + 1) * LANES) for t in range(row_tiles)]
    for jb in range(col_tiles):
        down = slice(jb * LANES, (jb + 1) * LANES)
        biggest = None
        for t in range(row_tiles):
            shifted = s_ref[down, tiles[t]] + row_log[t : t + 1, :]
            s_ref[down, tiles[t]] = shifted
            biggest = shifted if biggest is None else jnp.maximum(biggest, shifted)
        biggest = jnp.max(biggest, axis=1, keepdims=True)
        wide = jnp.broadcast_to(biggest, (LANES, LANES))
        summed = jnp.zeros((LANES, LANES), F32)
        for t in range(row_tiles):
            part = jnp.exp2(s_ref[down, tiles[t]] - wide)
            f_ref[down, tiles[t]] = part.astype(BF16)
            summed = summed + part
        summed = jnp.sum(summed, axis=1, keepdims=True)
        cmax_ref[pl.ds(jb, 1), :] = across(biggest)
        col_send[0, pl.ds(jb, 1), :] = across(biggest + jnp.log2(summed))

    send_all(col_send.at[0], col_recv.at[0], col_ssem.at[0], col_rsem.at[0], col_to)
    pair_keys[1].start()
    for t in range(col_tiles):
        down = slice(t * LANES, (t + 1) * LANES)
        val_lhs[0:width, down] = v_ref[down, :].astype(F32).T.astype(BF16)
        for i in range(row_tiles):
            g_ref[tiles[i], down] = f_ref[down, tiles[i]].T
    wait_all(col_recv.at[0], col_rsem.at[0])
    total = log_total(col_send[0], [col_recv[0, slot] for slot in range(1, nx)])
    log_send[...] = -total
    pair_log.start()
    col_vec[...] = jnp.exp2(cmax_ref[...] - total)

    def for_pair():
        pair_keys[0].wait_recv()
        pair_keys[1].wait_recv()
        k_parts[:, 0:width] = k2_ref[...]
        k_parts[:, width:] = k2_ref[...]
        pair_log.wait_recv()
        for t in range(col_tiles):
            line = jnp.broadcast_to(log_recv[t : t + 1, :], (LANES, LANES))
            column = jnp.sum(jnp.where(eye, line, 0.0), axis=1, keepdims=True)
            wide_ref[t * LANES : (t + 1) * LANES, :] = jnp.broadcast_to(column, (LANES, LANES))
        for m in range(nz // 2):
            chunks = [to * 2 + xl for to in targets[2 * m : 2 * m + 2]]
            q_block = jnp.concatenate(
                [q_ref[pl.ds(pl.multiple_of(c * LANES, LANES), LANES), :] for c in chunks], axis=0
            )
            scores = lax.dot_general(
                k_parts[...],
                scaled_parts(q_block),
                (((1,), (1,)), ((), ())),
                preferred_element_type=F32,
            )
            for n, c in enumerate(chunks):
                across_lanes = slice((2 * m + n) * LANES, (2 * m + n + 1) * LANES)
                part = scores[:, n * LANES : (n + 1) * LANES] + wide_ref[...]
                pair_ref[cols:, across_lanes] = jnp.exp2(part + row_log[pl.ds(c, 1), :]).astype(BF16)

    def values_of_pair():
        pair_values[0].wait_recv()
        pair_values[1].wait_recv()
        for t in range(col_tiles):
            down = slice(t * LANES, (t + 1) * LANES)
            val_lhs[0:width, cols + t * LANES : cols + (t + 1) * LANES] = (
                v2_ref[down, :].astype(F32).T.astype(BF16)
            )

    def own_half():
        for n, to in enumerate(targets):
            c = to * 2 + xl
            pair_ref[0:cols, n * LANES : (n + 1) * LANES] = f_ref[
                :, pl.ds(pl.multiple_of(c * LANES, LANES), LANES)
            ]

    def row_step(turn):
        for t in range(col_tiles):
            lhs_row[:, t * LANES : (t + 1) * LANES] = split_lhs(col_vec[t : t + 1, :])
        sums = jnp.sum(
            lax.dot_general(
                lhs_row[...], f_ref[...], (((1,), (0,)), ((), ())), preferred_element_type=F32
            ),
            axis=0,
            keepdims=True,
        )
        for t in range(row_tiles):
            row_vec[pl.ds(t, 1), :] = sums[:, t * LANES : (t + 1) * LANES]
        own = row_vec[...].astype(BF16)
        sum_send[turn - 1] = own
        send_all(
            sum_send.at[turn - 1], sum_recv.at[turn - 1], row_ssem.at[turn], row_rsem.at[turn], row_to
        )
        if turn == 1:
            pair_values[0].start()
            for_pair()
        else:
            values_of_pair()
        wait_all(sum_recv.at[turn - 1], row_rsem.at[turn])
        row_vec[...] = 1.0 / plain_total(
            own.astype(F32), [sum_recv[turn - 1, slot].astype(F32) for slot in range(1, ny)]
        )

    def col_step(turn):
        for t in range(row_tiles):
            lhs_col[:, t * LANES : (t + 1) * LANES] = split_lhs(row_vec[t : t + 1, :])
        sums = jnp.sum(
            lax.dot_general(
                lhs_col[...], g_ref[...], (((1,), (0,)), ((), ())), preferred_element_type=F32
            ),
            axis=0,
            keepdims=True,
        )
        for t in range(col_tiles):
            col_send[turn, pl.ds(t, 1), :] = (
                sums[:, t * LANES : (t + 1) * LANES] * col_vec[t : t + 1, :]
            )
        send_all(
            col_send.at[turn], col_recv.at[turn], col_ssem.at[turn], col_rsem.at[turn], col_to
        )
        if turn == 1:
            pair_values[1].start()
            own_half()
        if turn == SWEEPS - 1:
            send_all(col_send.at[turn], side_recv, side_sem.at[0], side_sem.at[1], side_to)
        wait_all(col_recv.at[turn], col_rsem.at[turn])
        inverse = 1.0 / plain_total(
            col_send[turn], [col_recv[turn, slot] for slot in range(1, nx)]
        )
        col_vec[...] = col_vec[...] * inverse
        if turn == 1:
            part_send[...] = inverse
            pair_part.start()

    for turn in range(1, SWEEPS):
        row_step(turn)
        col_step(turn)

    pltpu.make_async_copy(side_recv, side_recv, side_sem.at[1]).wait()
    pair_part.wait_recv()
    side = part_recv[...] / plain_total(side_recv[0], [side_recv[slot] for slot in range(1, nx)])
    for t in range(2 * col_tiles):
        lanes = slice(t * LANES, (t + 1) * LANES)
        if t < col_tiles:
            line = col_vec[t : t + 1, :]
        else:
            line = side[t - col_tiles : t - col_tiles + 1, :]
        val_lhs[0:width, lanes] = (val_lhs[0:width, lanes].astype(F32) * line).astype(BF16)
        val_lhs[width : width + 16, lanes] = split_lhs(line)
    tail = lax.broadcasted_iota(jnp.int32, (16, LANES), 0)

    def product(m):
        return jnp.dot(
            val_lhs[...],
            pair_ref[:, m * 2 * LANES : (m + 1) * 2 * LANES],
            preferred_element_type=F32,
        )

    ahead = product(0)
    for m in range(nz // 2):
        both = ahead
        if m + 1 < nz // 2:
            ahead = product(m + 1)
        for x in range(2):
            n = 2 * m + x
            piece = both[:, x * LANES : (x + 1) * LANES]
            out_send[n, 0:width, :] = piece[0:width].astype(BF16)
            weight = jnp.sum(piece[width:], axis=0, keepdims=True)
            high = weight.astype(BF16).astype(F32)
            out_send[n, width : width + 16, :] = jnp.where(
                tail == 0, high, jnp.where(tail == 1, weight - high, 0.0)
            ).astype(BF16)
            if n != nz - 1:
                pltpu.make_async_remote_copy(
                    src_ref=out_send.at[n],
                    dst_ref=out_recv.at[lax.rem(z - targets[n] + nz, nz)],
                    send_sem=out_sem.at[0],
                    recv_sem=out_sem.at[1],
                    device_id={"gy": targets[n] * 2 + xl},
                    device_id_type=MESH,
                ).start()
    wait_all(out_recv, out_sem.at[1])
    total = out_send[nz - 1].astype(F32)
    for slot in range(1, nz):
        total = total + out_recv[slot].astype(F32)
    weight = jnp.sum(total[width:], axis=0, keepdims=True)
    head = (total[0:width] / weight).T.astype(BF16)
    head_send[...] = head
    swap = pltpu.make_async_remote_copy(
        src_ref=head_send,
        dst_ref=head_recv,
        send_sem=head_sem.at[0],
        recv_sem=head_sem.at[1],
        device_id={"gz": 1 - gz},
        device_id_type=MESH,
    )
    swap.start()
    out_ref[:, pl.ds(pl.multiple_of(gz * width, width), width)] = head
    wait_all(row_recv, row_ssem.at[0])
    wait_all(col_recv.at[0], col_ssem.at[0])
    for turn in range(1, SWEEPS):
        wait_all(sum_recv.at[turn - 1], row_ssem.at[turn])
        wait_all(col_recv.at[turn], col_ssem.at[turn])
    wait_all(out_recv, out_sem.at[0])
    pltpu.make_async_copy(side_recv, side_recv, side_sem.at[0]).wait()
    for copy in [*pair_keys, *pair_values, pair_log, pair_part]:
        copy.wait_send()
    swap.wait()
    out_ref[:, pl.ds(pl.multiple_of((1 - gz) * width, width), width)] = head_recv[...]


def solution(mesh):
    nx, ny = mesh.shape["gx"], mesh.shape["gy"]

    def body(queries, keys, values, w_out):
        _, rows, width = queries.shape
        cols = keys.shape[1]
        columns = w_out.shape[1] // lax.axis_size("gz")
        row_tiles, col_tiles = rows // LANES, cols // LANES
        anywhere = pl.BlockSpec(memory_space=pltpu.HBM)
        dma = pltpu.SemaphoreType.DMA
        heads = pl.pallas_call(
            functools.partial(kernel, (nx, ny)),
            out_shape=jax.ShapeDtypeStruct((rows // ny, 2 * width), BF16),
            in_specs=[anywhere] * 3,
            out_specs=pl.BlockSpec(memory_space=pltpu.VMEM),
            scratch_shapes=[
                pltpu.VMEM((rows, width), BF16),
                pltpu.VMEM((cols, width), BF16),
                pltpu.VMEM((cols, width), BF16),
                pltpu.VMEM((cols, 2 * width), BF16),
                pltpu.VMEM((cols, rows), F32),
                pltpu.VMEM((cols, rows), BF16),
                pltpu.VMEM((rows, cols), BF16),
                pltpu.VMEM((16, cols), BF16),
                pltpu.VMEM((16, rows), BF16),
                pltpu.VMEM((width + 16, 2 * cols), BF16),
                pltpu.VMEM((cols, width), BF16),
                pltpu.VMEM((cols, width), BF16),
                pltpu.VMEM((2 * cols, rows // 2), BF16),
                pltpu.VMEM((cols, LANES), F32),
                pltpu.VMEM((row_tiles, LANES), F32),
                pltpu.VMEM((col_tiles, LANES), F32),
                pltpu.VMEM((col_tiles, LANES), F32),
                pltpu.VMEM((col_tiles, LANES), F32),
                pltpu.VMEM((col_tiles, LANES), F32),
                pltpu.VMEM((nx, col_tiles, LANES), F32),
                pltpu.VMEM((col_tiles, LANES), F32),
                pltpu.VMEM((row_tiles, LANES), F32),
                pltpu.VMEM((ny, row_tiles, LANES), F32),
                pltpu.VMEM((SWEEPS - 1, row_tiles, LANES), BF16),
                pltpu.VMEM((SWEEPS - 1, ny, row_tiles, LANES), BF16),
                pltpu.VMEM((SWEEPS, col_tiles, LANES), F32),
                pltpu.VMEM((SWEEPS, nx, col_tiles, LANES), F32),
                pltpu.VMEM((row_tiles, LANES), F32),
                pltpu.VMEM((col_tiles, LANES), F32),
                pltpu.VMEM((ny // 2, width + 16, LANES), BF16),
                pltpu.VMEM((ny // 2, width + 16, LANES), BF16),
                pltpu.VMEM((LANES, width), BF16),
                pltpu.VMEM((LANES, width), BF16),
                dma((5,)),
                dma((SWEEPS,)),
                dma((SWEEPS,)),
                dma((SWEEPS,)),
                dma((SWEEPS,)),
                dma((2,)),
                dma((2,)),
                dma((6,)),
                dma((6,)),
                dma((2,)),
            ],
            compiler_params=pltpu.CompilerParams(
                collective_id=0, has_side_effects=True, vmem_limit_bytes=44 * 1024 * 1024
            ),
        )(
            *(
                pltpu.with_memory_space_constraint(x.reshape(-1, width), pltpu.HBM)
                for x in (queries, keys, values)
            )
        )
        w_columns = lax.dynamic_slice_in_dim(
            w_out, lax.axis_index("gz") * columns, columns, 1
        )
        return jnp.dot(heads, w_columns, preferred_element_type=F32).astype(BF16)

    return jax.shard_map(
        body,
        mesh=mesh,
        in_specs=(P("gz", "gx", None), P("gz", "gy", None), P("gz", "gy", None), P()),
        out_specs=P(("gx", "gy"), "gz"),
        check_vma=False,
    )
```

```python
import functools
import math

import jax
import jax.numpy as jnp
from jax import lax
from jax.experimental import pallas as pl
from jax.experimental.pallas import tpu as pltpu
from jax.sharding import PartitionSpec as P

SWEEPS = 3
LANES = 128
MESH = pl.DeviceIdType.MESH
F32 = jnp.float32
BF16 = jnp.bfloat16


def far_first(count):
    return sorted(range(count), key=lambda d: -min(d, count - d))


def split_lhs(x):
    rows = jnp.broadcast_to(x, (16, x.shape[1]))
    hi = rows.astype(BF16).astype(F32)
    rest = rows - hi
    mid = rest.astype(BF16).astype(F32)
    lo = rest - mid
    at = lax.broadcasted_iota(jnp.int32, rows.shape, 0)
    parts = jnp.where(at == 0, hi, jnp.where(at == 1, mid, jnp.where(at == 2, lo, 0.0)))
    return parts.astype(BF16)


def kernel(
    sizes,
    q_hbm,
    k_hbm,
    v_hbm,
    out_ref,
    q_ref,
    k_ref,
    v_ref,
    k_parts,
    s_ref,
    f_ref,
    g_ref,
    lhs_row,
    lhs_col,
    val_lhs,
    k2_ref,
    v2_ref,
    pair_ref,
    wide_ref,
    row_log,
    log_send,
    log_recv,
    part_send,
    part_recv,
    side_recv,
    cmax_ref,
    row_send,
    row_recv,
    sum_send,
    sum_recv,
    col_send,
    col_recv,
    row_vec,
    col_vec,
    out_send,
    out_recv,
    head_send,
    head_recv,
    load_sem,
    first_sem,
    row_ssem,
    row_rsem,
    col_ssem,
    col_rsem,
    out_sem,
    head_sem,
    pair_ssem,
    pair_rsem,
    side_sem,
):
    nx, ny = sizes
    rows, width = q_ref.shape
    cols = k_ref.shape[0]
    row_tiles, col_tiles = rows // LANES, cols // LANES
    nz = ny // 2
    gz, gx, gy = lax.axis_index("gz"), lax.axis_index("gx"), lax.axis_index("gy")
    z, xl = gy // 2, lax.rem(gy, 2)
    y, xh = gx // 2, lax.rem(gx, 2)
    scale = math.log2(math.e) / math.sqrt(width)

    row_peers = [(dz, dx) for dz in far_first(nz) for dx in (1, 0) if (dz, dx) != (0, 0)]
    col_peers = [(dy, dx) for dy in far_first(nx // 2) for dx in (1, 0) if (dy, dx) != (0, 0)]

    def row_peer(dz, dx):
        return lax.rem(z + dz, nz) * 2 + lax.rem(xl + dx, 2)

    def col_peer(dy, dx):
        return lax.rem(y + dy, nx // 2) * 2 + lax.rem(xh + dx, 2)

    loads = [
        pltpu.make_async_copy(q_hbm, q_ref, load_sem.at[0]),
        pltpu.make_async_copy(k_hbm, k_parts.at[:, pl.ds(0, width)], load_sem.at[1]),
        pltpu.make_async_copy(v_hbm, v_ref, load_sem.at[2]),
        pltpu.make_async_copy(k_hbm, k_parts.at[:, pl.ds(width, width)], load_sem.at[3]),
        pltpu.make_async_copy(k_hbm, k_ref, load_sem.at[4]),
    ]
    for n in (1, 3, 0, 4, 2):
        loads[n].start()

    barrier = pltpu.get_barrier_semaphore()
    for dz, dx in row_peers:
        pl.semaphore_signal(
            barrier, inc=1, device_id={"gy": row_peer(dz, dx)}, device_id_type=MESH
        )
    for dy, dx in col_peers:
        pl.semaphore_signal(
            barrier, inc=1, device_id={"gx": col_peer(dy, dx)}, device_id_type=MESH
        )
    pl.semaphore_signal(barrier, inc=1, device_id={"gz": 1 - gz}, device_id_type=MESH)
    beside = z * 2 + 1 - xl
    for dy, dx in col_peers:
        pl.semaphore_signal(
            barrier,
            inc=1,
            device_id={"gx": col_peer(dy, dx), "gy": beside},
            device_id_type=MESH,
        )

    def send_all(source, target, ssem, rsem, peers):
        for slot, device in peers:
            pltpu.make_async_remote_copy(
                src_ref=source,
                dst_ref=target.at[slot],
                send_sem=ssem,
                recv_sem=rsem,
                device_id=device,
                device_id_type=MESH,
            ).start()

    def wait_all(target, sem):
        everything = target.at[pl.ds(1, target.shape[0] - 1)]
        pltpu.make_async_copy(everything, everything, sem).wait()

    row_to = [(dz * 2 + dx, {"gy": row_peer(dz, dx)}) for dz, dx in row_peers]
    col_to = [(dy * 2 + dx, {"gx": col_peer(dy, dx)}) for dy, dx in col_peers]
    side_to = [
        (dy * 2 + dx, {"gx": col_peer(dy, dx), "gy": beside}) for dy, dx in [*col_peers, (0, 0)]
    ]

    def to_pair(source, target, number):
        return pltpu.make_async_remote_copy(
            src_ref=source,
            dst_ref=target,
            send_sem=pair_ssem.at[number],
            recv_sem=pair_rsem.at[number],
            device_id={"gy": beside},
            device_id_type=MESH,
        )

    half = cols // 2
    halves = [pl.ds(0, half), pl.ds(half, half)]
    pair_keys = [to_pair(k_ref.at[h], k2_ref.at[h], n) for n, h in enumerate(halves)]
    pair_values = [to_pair(v_ref.at[h], v2_ref.at[h], 2 + n) for n, h in enumerate(halves)]
    pair_log = to_pair(log_send, log_recv, 4)
    pair_part = to_pair(part_send, part_recv, 5)

    def ranked(n):
        return jnp.where(n < nz // 2, n, nz + nz // 2 - 1 - n)

    targets = [ranked(jnp.where(n >= ranked(z), n + 1, n)) for n in range(nz - 1)] + [z]

    def log_total(own, received):
        biggest = own
        for other in received:
            biggest = jnp.maximum(biggest, other)
        total = jnp.exp2(own - biggest)
        for other in received:
            total = total + jnp.exp2(other - biggest)
        return biggest + jnp.log2(total)

    def plain_total(own, received):
        total = own
        for other in received:
            total = total + other
        return total

    loads[1].wait()
    loads[3].wait()
    loads[0].wait()

    def scaled_parts(x):
        scaled = scale * x.astype(F32)
        high = scaled.astype(BF16)
        return jnp.concatenate([high, (scaled - high.astype(F32)).astype(BF16)], axis=1)

    def send_rows(side_of):
        send_all(
            row_send.at[side_of],
            row_recv.at[side_of],
            first_sem.at[2 + side_of],
            first_sem.at[side_of],
            row_to,
        )

    block = 2 * LANES
    for b in range(rows // block):
        lanes = slice(b * block, (b + 1) * block)
        scores = lax.dot_general(
            k_parts[...],
            scaled_parts(q_ref[lanes, :]),
            (((1,), (1,)), ((), ())),
            preferred_element_type=F32,
        )
        s_ref[:, lanes] = scores
        tops, sums = [], []
        for jb in range(col_tiles):
            part = scores[jb * LANES : (jb + 1) * LANES].reshape(LANES // 8, 8, block)
            top = jnp.max(part, axis=0)
            tops.append(top)
            sums.append(jnp.sum(jnp.exp2(part - top[None]), axis=0))
        biggest = functools.reduce(jnp.maximum, tops)
        summed = sum(total * jnp.exp2(top - biggest) for top, total in zip(tops, sums))
        top = jnp.max(biggest, axis=0, keepdims=True)
        summed = jnp.sum(summed * jnp.exp2(biggest - top), axis=0, keepdims=True)
        local = top + jnp.log2(summed)
        for t in range(block // LANES):
            side_of, line = divmod(b * (block // LANES) + t, row_tiles // 2)
            row_send[side_of, pl.ds(line, 1), :] = local[:, t * LANES : (t + 1) * LANES]
        if b + 1 == rows // block // 2:
            pl.semaphore_wait(barrier, len(row_peers) + 2 * len(col_peers) + 1)
            send_rows(0)

    send_rows(1)
    loads[4].wait()
    pair_keys[0].start()
    loads[2].wait()
    for side_of in range(2):
        wait_all(row_recv.at[side_of], first_sem.at[side_of])
        row_log[side_of * (row_tiles // 2) : (side_of + 1) * (row_tiles // 2), :] = -log_total(
            row_send[side_of], [row_recv[side_of, slot] for slot in range(1, ny)]
        )

    eye = lax.broadcasted_iota(jnp.int32, (LANES, LANES), 0) == lax.broadcasted_iota(
        jnp.int32, (LANES, LANES), 1
    )

    def across(column):
        return jnp.sum(
            jnp.where(eye, jnp.broadcast_to(column, (LANES, LANES)), 0.0), axis=0, keepdims=True
        )

    tiles = [slice(t * LANES, (t + 1) * LANES) for t in range(row_tiles)]
    for jb in range(col_tiles):
        down = slice(jb * LANES, (jb + 1) * LANES)
        biggest = None
        for t in range(row_tiles):
            shifted = s_ref[down, tiles[t]] + row_log[t : t + 1, :]
            s_ref[down, tiles[t]] = shifted
            biggest = shifted if biggest is None else jnp.maximum(biggest, shifted)
        biggest = jnp.max(biggest, axis=1, keepdims=True)
        wide = jnp.broadcast_to(biggest, (LANES, LANES))
        summed = jnp.zeros((LANES, LANES), F32)
        for t in range(row_tiles):
            part = jnp.exp2(s_ref[down, tiles[t]] - wide)
            f_ref[down, tiles[t]] = part.astype(BF16)
            summed = summed + part
        summed = jnp.sum(summed, axis=1, keepdims=True)
        cmax_ref[pl.ds(jb, 1), :] = across(biggest)
        col_send[0, pl.ds(jb, 1), :] = across(biggest + jnp.log2(summed))

    send_all(col_send.at[0], col_recv.at[0], col_ssem.at[0], col_rsem.at[0], col_to)
    pair_keys[1].start()
    for t in range(col_tiles):
        down = slice(t * LANES, (t + 1) * LANES)
        val_lhs[0:width, down] = v_ref[down, :].astype(F32).T.astype(BF16)
        for i in range(row_tiles):
            g_ref[tiles[i], down] = f_ref[down, tiles[i]].T
    wait_all(col_recv.at[0], col_rsem.at[0])
    total = log_total(col_send[0], [col_recv[0, slot] for slot in range(1, nx)])
    log_send[...] = -total
    pair_log.start()
    col_vec[...] = jnp.exp2(cmax_ref[...] - total)

    def for_pair():
        pair_keys[0].wait_recv()
        pair_keys[1].wait_recv()
        k_parts[:, 0:width] = k2_ref[...]
        k_parts[:, width:] = k2_ref[...]
        pair_log.wait_recv()
        for t in range(col_tiles):
            line = jnp.broadcast_to(log_recv[t : t + 1, :], (LANES, LANES))
            column = jnp.sum(jnp.where(eye, line, 0.0), axis=1, keepdims=True)
            wide_ref[t * LANES : (t + 1) * LANES, :] = jnp.broadcast_to(column, (LANES, LANES))
        for m in range(nz // 2):
            chunks = [to * 2 + xl for to in targets[2 * m : 2 * m + 2]]
            q_block = jnp.concatenate(
                [q_ref[pl.ds(pl.multiple_of(c * LANES, LANES), LANES), :] for c in chunks], axis=0
            )
            scores = lax.dot_general(
                k_parts[...],
                scaled_parts(q_block),
                (((1,), (1,)), ((), ())),
                preferred_element_type=F32,
            )
            for n, c in enumerate(chunks):
                across_lanes = slice((2 * m + n) * LANES, (2 * m + n + 1) * LANES)
                part = scores[:, n * LANES : (n + 1) * LANES] + wide_ref[...]
                pair_ref[cols:, across_lanes] = jnp.exp2(part + row_log[pl.ds(c, 1), :]).astype(BF16)

    def values_of_pair():
        pair_values[0].wait_recv()
        pair_values[1].wait_recv()
        for t in range(col_tiles):
            down = slice(t * LANES, (t + 1) * LANES)
            val_lhs[0:width, cols + t * LANES : cols + (t + 1) * LANES] = (
                v2_ref[down, :].astype(F32).T.astype(BF16)
            )

    def own_half():
        for n, to in enumerate(targets):
            c = to * 2 + xl
            pair_ref[0:cols, n * LANES : (n + 1) * LANES] = f_ref[
                :, pl.ds(pl.multiple_of(c * LANES, LANES), LANES)
            ]

    def row_step(turn):
        for t in range(col_tiles):
            lhs_row[:, t * LANES : (t + 1) * LANES] = split_lhs(col_vec[t : t + 1, :])
        sums = jnp.sum(
            lax.dot_general(
                lhs_row[...], f_ref[...], (((1,), (0,)), ((), ())), preferred_element_type=F32
            ),
            axis=0,
            keepdims=True,
        )
        for t in range(row_tiles):
            row_vec[pl.ds(t, 1), :] = sums[:, t * LANES : (t + 1) * LANES]
        own = row_vec[...].astype(BF16)
        sum_send[turn - 1] = own
        send_all(
            sum_send.at[turn - 1], sum_recv.at[turn - 1], row_ssem.at[turn - 1], row_rsem.at[turn - 1], row_to
        )
        if turn == 1:
            pair_values[0].start()
            for_pair()
        else:
            values_of_pair()
        wait_all(sum_recv.at[turn - 1], row_rsem.at[turn - 1])
        row_vec[...] = 1.0 / plain_total(
            own.astype(F32), [sum_recv[turn - 1, slot].astype(F32) for slot in range(1, ny)]
        )

    def col_step(turn):
        for t in range(row_tiles):
            lhs_col[:, t * LANES : (t + 1) * LANES] = split_lhs(row_vec[t : t + 1, :])
        sums = jnp.sum(
            lax.dot_general(
                lhs_col[...], g_ref[...], (((1,), (0,)), ((), ())), preferred_element_type=F32
            ),
            axis=0,
            keepdims=True,
        )
        for t in range(col_tiles):
            col_send[turn, pl.ds(t, 1), :] = (
                sums[:, t * LANES : (t + 1) * LANES] * col_vec[t : t + 1, :]
            )
        send_all(
            col_send.at[turn], col_recv.at[turn], col_ssem.at[turn], col_rsem.at[turn], col_to
        )
        if turn == 1:
            pair_values[1].start()
            own_half()
        if turn == SWEEPS - 1:
            send_all(col_send.at[turn], side_recv, side_sem.at[0], side_sem.at[1], side_to)
        wait_all(col_recv.at[turn], col_rsem.at[turn])
        inverse = 1.0 / plain_total(
            col_send[turn], [col_recv[turn, slot] for slot in range(1, nx)]
        )
        col_vec[...] = col_vec[...] * inverse
        if turn == 1:
            part_send[...] = inverse
            pair_part.start()

    for turn in range(1, SWEEPS):
        row_step(turn)
        col_step(turn)

    pltpu.make_async_copy(side_recv, side_recv, side_sem.at[1]).wait()
    pair_part.wait_recv()
    side = part_recv[...] / plain_total(side_recv[0], [side_recv[slot] for slot in range(1, nx)])
    for t in range(2 * col_tiles):
        lanes = slice(t * LANES, (t + 1) * LANES)
        if t < col_tiles:
            line = col_vec[t : t + 1, :]
        else:
            line = side[t - col_tiles : t - col_tiles + 1, :]
        val_lhs[0:width, lanes] = (val_lhs[0:width, lanes].astype(F32) * line).astype(BF16)
        val_lhs[width : width + 16, lanes] = split_lhs(line)
    tail = lax.broadcasted_iota(jnp.int32, (16, LANES), 0)

    def product(m):
        return jnp.dot(
            val_lhs[...],
            pair_ref[:, m * 2 * LANES : (m + 1) * 2 * LANES],
            preferred_element_type=F32,
        )

    ahead = product(0)
    for m in range(nz // 2):
        both = ahead
        if m + 1 < nz // 2:
            ahead = product(m + 1)
        for x in range(2):
            n = 2 * m + x
            piece = both[:, x * LANES : (x + 1) * LANES]
            out_send[n, 0:width, :] = piece[0:width].astype(BF16)
            weight = jnp.sum(piece[width:], axis=0, keepdims=True)
            high = weight.astype(BF16).astype(F32)
            out_send[n, width : width + 16, :] = jnp.where(
                tail == 0, high, jnp.where(tail == 1, weight - high, 0.0)
            ).astype(BF16)
            if n != nz - 1:
                pltpu.make_async_remote_copy(
                    src_ref=out_send.at[n],
                    dst_ref=out_recv.at[lax.rem(z - targets[n] + nz, nz)],
                    send_sem=out_sem.at[0],
                    recv_sem=out_sem.at[1],
                    device_id={"gy": targets[n] * 2 + xl},
                    device_id_type=MESH,
                ).start()
    wait_all(out_recv, out_sem.at[1])
    total = out_send[nz - 1].astype(F32)
    for slot in range(1, nz):
        total = total + out_recv[slot].astype(F32)
    weight = jnp.sum(total[width:], axis=0, keepdims=True)
    head = (total[0:width] / weight).T.astype(BF16)
    head_send[...] = head
    swap = pltpu.make_async_remote_copy(
        src_ref=head_send,
        dst_ref=head_recv,
        send_sem=head_sem.at[0],
        recv_sem=head_sem.at[1],
        device_id={"gz": 1 - gz},
        device_id_type=MESH,
    )
    swap.start()
    out_ref[:, pl.ds(pl.multiple_of(gz * width, width), width)] = head
    for side_of in range(2):
        wait_all(row_recv.at[side_of], first_sem.at[2 + side_of])
    wait_all(col_recv.at[0], col_ssem.at[0])
    for turn in range(1, SWEEPS):
        wait_all(sum_recv.at[turn - 1], row_ssem.at[turn - 1])
        wait_all(col_recv.at[turn], col_ssem.at[turn])
    wait_all(out_recv, out_sem.at[0])
    pltpu.make_async_copy(side_recv, side_recv, side_sem.at[0]).wait()
    for copy in [*pair_keys, *pair_values, pair_log, pair_part]:
        copy.wait_send()
    swap.wait()
    out_ref[:, pl.ds(pl.multiple_of((1 - gz) * width, width), width)] = head_recv[...]


def solution(mesh):
    nx, ny = mesh.shape["gx"], mesh.shape["gy"]

    def body(queries, keys, values, w_out):
        _, rows, width = queries.shape
        cols = keys.shape[1]
        columns = w_out.shape[1] // lax.axis_size("gz")
        row_tiles, col_tiles = rows // LANES, cols // LANES
        anywhere = pl.BlockSpec(memory_space=pltpu.HBM)
        dma = pltpu.SemaphoreType.DMA
        heads = pl.pallas_call(
            functools.partial(kernel, (nx, ny)),
            out_shape=jax.ShapeDtypeStruct((rows // ny, 2 * width), BF16),
            in_specs=[anywhere] * 3,
            out_specs=pl.BlockSpec(memory_space=pltpu.VMEM),
            scratch_shapes=[
                pltpu.VMEM((rows, width), BF16),
                pltpu.VMEM((cols, width), BF16),
                pltpu.VMEM((cols, width), BF16),
                pltpu.VMEM((cols, 2 * width), BF16),
                pltpu.VMEM((cols, rows), F32),
                pltpu.VMEM((cols, rows), BF16),
                pltpu.VMEM((rows, cols), BF16),
                pltpu.VMEM((16, cols), BF16),
                pltpu.VMEM((16, rows), BF16),
                pltpu.VMEM((width + 16, 2 * cols), BF16),
                pltpu.VMEM((cols, width), BF16),
                pltpu.VMEM((cols, width), BF16),
                pltpu.VMEM((2 * cols, rows // 2), BF16),
                pltpu.VMEM((cols, LANES), F32),
                pltpu.VMEM((row_tiles, LANES), F32),
                pltpu.VMEM((col_tiles, LANES), F32),
                pltpu.VMEM((col_tiles, LANES), F32),
                pltpu.VMEM((col_tiles, LANES), F32),
                pltpu.VMEM((col_tiles, LANES), F32),
                pltpu.VMEM((nx, col_tiles, LANES), F32),
                pltpu.VMEM((col_tiles, LANES), F32),
                pltpu.VMEM((2, row_tiles // 2, LANES), F32),
                pltpu.VMEM((2, ny, row_tiles // 2, LANES), F32),
                pltpu.VMEM((SWEEPS - 1, row_tiles, LANES), BF16),
                pltpu.VMEM((SWEEPS - 1, ny, row_tiles, LANES), BF16),
                pltpu.VMEM((SWEEPS, col_tiles, LANES), F32),
                pltpu.VMEM((SWEEPS, nx, col_tiles, LANES), F32),
                pltpu.VMEM((row_tiles, LANES), F32),
                pltpu.VMEM((col_tiles, LANES), F32),
                pltpu.VMEM((ny // 2, width + 16, LANES), BF16),
                pltpu.VMEM((ny // 2, width + 16, LANES), BF16),
                pltpu.VMEM((LANES, width), BF16),
                pltpu.VMEM((LANES, width), BF16),
                dma((5,)),
                dma((4,)),
                dma((SWEEPS - 1,)),
                dma((SWEEPS - 1,)),
                dma((SWEEPS,)),
                dma((SWEEPS,)),
                dma((2,)),
                dma((2,)),
                dma((6,)),
                dma((6,)),
                dma((2,)),
            ],
            compiler_params=pltpu.CompilerParams(
                collective_id=0, has_side_effects=True, vmem_limit_bytes=44 * 1024 * 1024
            ),
        )(
            *(
                pltpu.with_memory_space_constraint(x.reshape(-1, width), pltpu.HBM)
                for x in (queries, keys, values)
            )
        )
        w_columns = lax.dynamic_slice_in_dim(
            w_out, lax.axis_index("gz") * columns, columns, 1
        )
        return jnp.dot(heads, w_columns, preferred_element_type=F32).astype(BF16)

    return jax.shard_map(
        body,
        mesh=mesh,
        in_specs=(P("gz", "gx", None), P("gz", "gy", None), P("gz", "gy", None), P()),
        out_specs=P(("gx", "gy"), "gz"),
        check_vma=False,
    )
```

```python
import functools
import math

import jax
import jax.numpy as jnp
from jax import lax
from jax.experimental import pallas as pl
from jax.experimental.pallas import tpu as pltpu
from jax.sharding import PartitionSpec as P

SWEEPS = 3
LANES = 128
MESH = pl.DeviceIdType.MESH
F32 = jnp.float32
BF16 = jnp.bfloat16


def far_first(count):
    return sorted(range(count), key=lambda d: -min(d, count - d))


def in_pairs(combine, parts):
    while len(parts) > 1:
        joined = [combine(*parts[n : n + 2]) for n in range(0, len(parts) - 1, 2)]
        parts = joined + parts[len(parts) // 2 * 2 :]
    return parts[0]


def split_lhs(x):
    rows = jnp.broadcast_to(x, (16, x.shape[1]))
    hi = rows.astype(BF16).astype(F32)
    rest = rows - hi
    mid = rest.astype(BF16).astype(F32)
    lo = rest - mid
    at = lax.broadcasted_iota(jnp.int32, rows.shape, 0)
    parts = jnp.where(at == 0, hi, jnp.where(at == 1, mid, jnp.where(at == 2, lo, 0.0)))
    return parts.astype(BF16)


def kernel(
    sizes,
    q_hbm,
    k_hbm,
    v_hbm,
    out_ref,
    q_ref,
    k_ref,
    v_ref,
    k_parts,
    s_ref,
    f_ref,
    g_ref,
    lhs_row,
    lhs_col,
    val_lhs,
    k2_ref,
    v2_ref,
    pair_ref,
    wide_ref,
    row_log,
    log_send,
    log_recv,
    part_send,
    part_recv,
    side_recv,
    cmax_ref,
    row_send,
    row_recv,
    sum_send,
    sum_recv,
    col_send,
    col_recv,
    row_vec,
    col_vec,
    out_send,
    out_recv,
    head_send,
    head_recv,
    load_sem,
    row_ssem,
    row_rsem,
    col_ssem,
    col_rsem,
    out_sem,
    head_sem,
    pair_ssem,
    pair_rsem,
    side_sem,
):
    nx, ny = sizes
    rows, width = q_ref.shape
    cols = k_ref.shape[0]
    row_tiles, col_tiles = rows // LANES, cols // LANES
    nz = ny // 2
    gz, gx, gy = lax.axis_index("gz"), lax.axis_index("gx"), lax.axis_index("gy")
    z, xl = gy // 2, lax.rem(gy, 2)
    y, xh = gx // 2, lax.rem(gx, 2)
    scale = math.log2(math.e) / math.sqrt(width)

    row_peers = [(dz, dx) for dz in far_first(nz) for dx in (1, 0) if (dz, dx) != (0, 0)]
    col_peers = [(dy, dx) for dy in far_first(nx // 2) for dx in (1, 0) if (dy, dx) != (0, 0)]

    def row_peer(dz, dx):
        return lax.rem(z + dz, nz) * 2 + lax.rem(xl + dx, 2)

    def col_peer(dy, dx):
        return lax.rem(y + dy, nx // 2) * 2 + lax.rem(xh + dx, 2)

    loads = [
        pltpu.make_async_copy(q_hbm, q_ref, load_sem.at[0]),
        pltpu.make_async_copy(k_hbm, k_parts.at[:, pl.ds(0, width)], load_sem.at[1]),
        pltpu.make_async_copy(v_hbm, v_ref, load_sem.at[2]),
        pltpu.make_async_copy(k_hbm, k_parts.at[:, pl.ds(width, width)], load_sem.at[3]),
        pltpu.make_async_copy(k_hbm, k_ref, load_sem.at[4]),
    ]
    for n in (1, 3, 0, 4, 2):
        loads[n].start()

    barrier = pltpu.get_barrier_semaphore()
    for dz, dx in row_peers:
        pl.semaphore_signal(
            barrier, inc=1, device_id={"gy": row_peer(dz, dx)}, device_id_type=MESH
        )
    for dy, dx in col_peers:
        pl.semaphore_signal(
            barrier, inc=1, device_id={"gx": col_peer(dy, dx)}, device_id_type=MESH
        )
    pl.semaphore_signal(barrier, inc=1, device_id={"gz": 1 - gz}, device_id_type=MESH)
    for dz in range(1, nz):
        pl.semaphore_signal(
            barrier,
            inc=1,
            device_id={"gy": row_peer(dz, 0), "gz": 1 - gz},
            device_id_type=MESH,
        )
    beside = z * 2 + 1 - xl
    for dy, dx in col_peers:
        pl.semaphore_signal(
            barrier,
            inc=1,
            device_id={"gx": col_peer(dy, dx), "gy": beside},
            device_id_type=MESH,
        )

    def send_all(source, target, ssem, rsem, peers):
        for slot, device in peers:
            pltpu.make_async_remote_copy(
                src_ref=source,
                dst_ref=target.at[slot],
                send_sem=ssem,
                recv_sem=rsem,
                device_id=device,
                device_id_type=MESH,
            ).start()

    def wait_all(target, sem):
        everything = target.at[pl.ds(1, target.shape[0] - 1)]
        pltpu.make_async_copy(everything, everything, sem).wait()

    row_to = [(dz * 2 + dx, {"gy": row_peer(dz, dx)}) for dz, dx in row_peers]
    col_to = [(dy * 2 + dx, {"gx": col_peer(dy, dx)}) for dy, dx in col_peers]
    side_to = [
        (dy * 2 + dx, {"gx": col_peer(dy, dx), "gy": beside}) for dy, dx in [*col_peers, (0, 0)]
    ]

    def to_pair(source, target, number):
        return pltpu.make_async_remote_copy(
            src_ref=source,
            dst_ref=target,
            send_sem=pair_ssem.at[number],
            recv_sem=pair_rsem.at[number],
            device_id={"gy": beside},
            device_id_type=MESH,
        )

    half = cols // 2
    halves = [pl.ds(0, half), pl.ds(half, half)]
    pair_keys = [to_pair(k_ref.at[h], k2_ref.at[h], n) for n, h in enumerate(halves)]
    pair_values = [to_pair(v_ref.at[h], v2_ref.at[h], 2 + n) for n, h in enumerate(halves)]
    pair_log = to_pair(log_send, log_recv, 4)
    pair_part = to_pair(part_send, part_recv, 5)

    turned = 3 if nz >= 8 else 1

    def ranked(n, shift):
        late = jnp.where(n < nz // 2, n, nz + nz // 2 - 1 - n)
        return jnp.where(n < turned, lax.rem(n + shift, turned), late)

    rank = ranked(z, turned - 1)
    targets = [ranked(jnp.where(n >= rank, n + 1, n), 1) for n in range(nz - 1)] + [z]

    def log_total(own, received):
        biggest = in_pairs(jnp.maximum, [own, *received])
        return biggest + jnp.log2(in_pairs(jnp.add, [jnp.exp2(x - biggest) for x in [own, *received]]))

    def plain_total(own, received):
        return in_pairs(jnp.add, [own, *received])

    loads[1].wait()
    loads[3].wait()
    loads[0].wait()

    def scaled_parts(x):
        scaled = scale * x.astype(F32)
        high = scaled.astype(BF16)
        return jnp.concatenate([high, (scaled - high.astype(F32)).astype(BF16)], axis=1)

    block = 2 * LANES
    for b in range(rows // block):
        lanes = slice(b * block, (b + 1) * block)
        scores = lax.dot_general(
            k_parts[...],
            scaled_parts(q_ref[lanes, :]),
            (((1,), (1,)), ((), ())),
            preferred_element_type=F32,
        )
        s_ref[:, lanes] = scores
        tops, sums = [], []
        for jb in range(col_tiles):
            part = scores[jb * LANES : (jb + 1) * LANES].reshape(LANES // 8, 8, block)
            top = jnp.max(part, axis=0)
            tops.append(top)
            sums.append(jnp.sum(jnp.exp2(part - top[None]), axis=0))
        biggest = in_pairs(jnp.maximum, tops)
        summed = in_pairs(
            jnp.add, [total * jnp.exp2(top - biggest) for top, total in zip(tops, sums)]
        )
        top = jnp.max(biggest, axis=0, keepdims=True)
        summed = jnp.sum(summed * jnp.exp2(biggest - top), axis=0, keepdims=True)
        local = top + jnp.log2(summed)
        for t in range(block // LANES):
            row_send[pl.ds(b * (block // LANES) + t, 1), :] = local[:, t * LANES : (t + 1) * LANES]

    pl.semaphore_wait(barrier, len(row_peers) + 2 * len(col_peers) + nz)
    send_all(row_send, row_recv, row_ssem.at[0], row_rsem.at[0], row_to)
    loads[4].wait()
    pair_keys[0].start()
    loads[2].wait()
    wait_all(row_recv, row_rsem.at[0])
    row_log[...] = -log_total(row_send[...], [row_recv[slot] for slot in range(1, ny)])

    eye = lax.broadcasted_iota(jnp.int32, (LANES, LANES), 0) == lax.broadcasted_iota(
        jnp.int32, (LANES, LANES), 1
    )

    def across(column):
        return jnp.sum(
            jnp.where(eye, jnp.broadcast_to(column, (LANES, LANES)), 0.0), axis=0, keepdims=True
        )

    tiles = [slice(t * LANES, (t + 1) * LANES) for t in range(row_tiles)]
    for jb in range(col_tiles):
        down = slice(jb * LANES, (jb + 1) * LANES)
        biggest = None
        for t in range(row_tiles):
            shifted = s_ref[down, tiles[t]] + row_log[t : t + 1, :]
            s_ref[down, tiles[t]] = shifted
            biggest = shifted if biggest is None else jnp.maximum(biggest, shifted)
        biggest = jnp.max(biggest, axis=1, keepdims=True)
        wide = jnp.broadcast_to(biggest, (LANES, LANES))
        summed = jnp.zeros((LANES, LANES), F32)
        for t in range(row_tiles):
            part = jnp.exp2(s_ref[down, tiles[t]] - wide)
            f_ref[down, tiles[t]] = part.astype(BF16)
            summed = summed + part
        summed = jnp.sum(summed, axis=1, keepdims=True)
        cmax_ref[pl.ds(jb, 1), :] = across(biggest)
        col_send[0, pl.ds(jb, 1), :] = across(biggest + jnp.log2(summed))

    send_all(col_send.at[0], col_recv.at[0], col_ssem.at[0], col_rsem.at[0], col_to)
    pair_keys[1].start()
    for t in range(col_tiles):
        down = slice(t * LANES, (t + 1) * LANES)
        val_lhs[0:width, down] = v_ref[down, :].astype(F32).T.astype(BF16)
        for i in range(row_tiles):
            g_ref[tiles[i], down] = f_ref[down, tiles[i]].T
    wait_all(col_recv.at[0], col_rsem.at[0])
    total = log_total(col_send[0], [col_recv[0, slot] for slot in range(1, nx)])
    log_send[...] = -total
    pair_log.start()
    col_vec[...] = jnp.exp2(cmax_ref[...] - total)

    def for_pair():
        pair_keys[0].wait_recv()
        pair_keys[1].wait_recv()
        k_parts[:, 0:width] = k2_ref[...]
        k_parts[:, width:] = k2_ref[...]
        pair_log.wait_recv()
        for t in range(col_tiles):
            line = jnp.broadcast_to(log_recv[t : t + 1, :], (LANES, LANES))
            column = jnp.sum(jnp.where(eye, line, 0.0), axis=1, keepdims=True)
            wide_ref[t * LANES : (t + 1) * LANES, :] = jnp.broadcast_to(column, (LANES, LANES))
        for m in range(nz // 2):
            chunks = [to * 2 + xl for to in targets[2 * m : 2 * m + 2]]
            q_block = jnp.concatenate(
                [q_ref[pl.ds(pl.multiple_of(c * LANES, LANES), LANES), :] for c in chunks], axis=0
            )
            scores = lax.dot_general(
                k_parts[...],
                scaled_parts(q_block),
                (((1,), (1,)), ((), ())),
                preferred_element_type=F32,
            )
            for n, c in enumerate(chunks):
                across_lanes = slice((2 * m + n) * LANES, (2 * m + n + 1) * LANES)
                part = scores[:, n * LANES : (n + 1) * LANES] + wide_ref[...]
                pair_ref[cols:, across_lanes] = jnp.exp2(part + row_log[pl.ds(c, 1), :]).astype(BF16)

    def values_of_pair():
        pair_values[0].wait_recv()
        pair_values[1].wait_recv()
        for t in range(col_tiles):
            down = slice(t * LANES, (t + 1) * LANES)
            val_lhs[0:width, cols + t * LANES : cols + (t + 1) * LANES] = (
                v2_ref[down, :].astype(F32).T.astype(BF16)
            )

    def own_half():
        for n, to in enumerate(targets):
            c = to * 2 + xl
            pair_ref[0:cols, n * LANES : (n + 1) * LANES] = f_ref[
                :, pl.ds(pl.multiple_of(c * LANES, LANES), LANES)
            ]

    def row_step(turn):
        for t in range(col_tiles):
            lhs_row[:, t * LANES : (t + 1) * LANES] = split_lhs(col_vec[t : t + 1, :])
        sums = jnp.sum(
            lax.dot_general(
                lhs_row[...], f_ref[...], (((1,), (0,)), ((), ())), preferred_element_type=F32
            ),
            axis=0,
            keepdims=True,
        )
        for t in range(row_tiles):
            row_vec[pl.ds(t, 1), :] = sums[:, t * LANES : (t + 1) * LANES]
        own = row_vec[...].astype(BF16)
        sum_send[turn - 1] = own
        send_all(
            sum_send.at[turn - 1], sum_recv.at[turn - 1], row_ssem.at[turn], row_rsem.at[turn], row_to
        )
        if turn == 1:
            pair_values[0].start()
            for_pair()
        else:
            values_of_pair()
        wait_all(sum_recv.at[turn - 1], row_rsem.at[turn])
        row_vec[...] = 1.0 / plain_total(
            own.astype(F32), [sum_recv[turn - 1, slot].astype(F32) for slot in range(1, ny)]
        )

    def col_step(turn):
        for t in range(row_tiles):
            lhs_col[:, t * LANES : (t + 1) * LANES] = split_lhs(row_vec[t : t + 1, :])
        sums = jnp.sum(
            lax.dot_general(
                lhs_col[...], g_ref[...], (((1,), (0,)), ((), ())), preferred_element_type=F32
            ),
            axis=0,
            keepdims=True,
        )
        for t in range(col_tiles):
            col_send[turn, pl.ds(t, 1), :] = (
                sums[:, t * LANES : (t + 1) * LANES] * col_vec[t : t + 1, :]
            )
        send_all(
            col_send.at[turn], col_recv.at[turn], col_ssem.at[turn], col_rsem.at[turn], col_to
        )
        if turn == 1:
            pair_values[1].start()
            own_half()
        if turn == SWEEPS - 1:
            send_all(col_send.at[turn], side_recv, side_sem.at[0], side_sem.at[1], side_to)
        wait_all(col_recv.at[turn], col_rsem.at[turn])
        inverse = 1.0 / plain_total(
            col_send[turn], [col_recv[turn, slot] for slot in range(1, nx)]
        )
        col_vec[...] = col_vec[...] * inverse
        if turn == 1:
            part_send[...] = inverse
            pair_part.start()

    for turn in range(1, SWEEPS):
        row_step(turn)
        col_step(turn)

    pltpu.make_async_copy(side_recv, side_recv, side_sem.at[1]).wait()
    pair_part.wait_recv()
    side = part_recv[...] / plain_total(side_recv[0], [side_recv[slot] for slot in range(1, nx)])
    for t in range(2 * col_tiles):
        lanes = slice(t * LANES, (t + 1) * LANES)
        if t < col_tiles:
            line = col_vec[t : t + 1, :]
        else:
            line = side[t - col_tiles : t - col_tiles + 1, :]
        val_lhs[0:width, lanes] = (val_lhs[0:width, lanes].astype(F32) * line).astype(BF16)
        val_lhs[width : width + 16, lanes] = split_lhs(line)
    tail = lax.broadcasted_iota(jnp.int32, (16, LANES), 0)

    def product(m):
        return jnp.dot(
            val_lhs[...],
            pair_ref[:, m * 2 * LANES : (m + 1) * 2 * LANES],
            preferred_element_type=F32,
        )

    ahead = product(0)
    for m in range(nz // 2):
        both = ahead
        if m + 1 < nz // 2:
            ahead = product(m + 1)
        for x in range(2):
            n = 2 * m + x
            piece = both[:, x * LANES : (x + 1) * LANES]
            out_send[n, 0:width, :] = piece[0:width].astype(BF16)
            weight = jnp.sum(piece[width:], axis=0, keepdims=True)
            high = weight.astype(BF16).astype(F32)
            out_send[n, width : width + 16, :] = jnp.where(
                tail == 0, high, jnp.where(tail == 1, weight - high, 0.0)
            ).astype(BF16)
            if n != nz - 1:
                pltpu.make_async_remote_copy(
                    src_ref=out_send.at[n],
                    dst_ref=out_recv.at[gz, lax.rem(z - targets[n] + nz, nz)],
                    send_sem=out_sem.at[2],
                    recv_sem=out_sem.at[gz],
                    device_id={"gy": targets[n] * 2 + xl, "gz": 1},
                    device_id_type=MESH,
                ).start()
    def all_waited(view, sem):
        pltpu.make_async_copy(view, view, sem).wait()

    def head_of(pieces):
        total = in_pairs(jnp.add, [piece.astype(F32) for piece in pieces])
        weight = jnp.sum(total[width:], axis=0, keepdims=True)
        return (total[0:width] / weight).T.astype(BF16)

    others = out_recv.at[1, pl.ds(1, nz - 1)]

    @pl.when(gz == 0)
    def _():
        own = pltpu.make_async_remote_copy(
            src_ref=out_send.at[nz - 1],
            dst_ref=out_recv.at[0, 0],
            send_sem=head_sem.at[0],
            recv_sem=out_sem.at[0],
            device_id={"gz": 1},
            device_id_type=MESH,
        )
        own.start()
        own.wait_send()
        all_waited(head_recv, head_sem.at[1])
        out_ref[...] = head_recv[...]

    @pl.when(gz == 1)
    def _():
        all_waited(others, out_sem.at[1])
        head_send[:, width:] = head_of(
            [out_send[nz - 1], *(out_recv[1, slot] for slot in range(1, nz))]
        )
        all_waited(out_recv.at[0], out_sem.at[0])
        head_send[:, 0:width] = head_of([out_recv[0, slot] for slot in range(nz)])
        swap = pltpu.make_async_remote_copy(
            src_ref=head_send,
            dst_ref=head_recv,
            send_sem=head_sem.at[0],
            recv_sem=head_sem.at[1],
            device_id={"gz": 0},
            device_id_type=MESH,
        )
        swap.start()
        out_ref[...] = head_send[...]
        swap.wait_send()

    wait_all(row_recv, row_ssem.at[0])
    wait_all(col_recv.at[0], col_ssem.at[0])
    for turn in range(1, SWEEPS):
        wait_all(sum_recv.at[turn - 1], row_ssem.at[turn])
        wait_all(col_recv.at[turn], col_ssem.at[turn])
    all_waited(others, out_sem.at[2])
    pltpu.make_async_copy(side_recv, side_recv, side_sem.at[0]).wait()
    for copy in [*pair_keys, *pair_values, pair_log, pair_part]:
        copy.wait_send()


def solution(mesh):
    nx, ny = mesh.shape["gx"], mesh.shape["gy"]

    def body(queries, keys, values, w_out):
        _, rows, width = queries.shape
        cols = keys.shape[1]
        columns = w_out.shape[1] // lax.axis_size("gz")
        row_tiles, col_tiles = rows // LANES, cols // LANES
        anywhere = pl.BlockSpec(memory_space=pltpu.HBM)
        dma = pltpu.SemaphoreType.DMA
        heads = pl.pallas_call(
            functools.partial(kernel, (nx, ny)),
            out_shape=jax.ShapeDtypeStruct((rows // ny, 2 * width), BF16),
            in_specs=[anywhere] * 3,
            out_specs=pl.BlockSpec(memory_space=pltpu.VMEM),
            scratch_shapes=[
                pltpu.VMEM((rows, width), BF16),
                pltpu.VMEM((cols, width), BF16),
                pltpu.VMEM((cols, width), BF16),
                pltpu.VMEM((cols, 2 * width), BF16),
                pltpu.VMEM((cols, rows), F32),
                pltpu.VMEM((cols, rows), BF16),
                pltpu.VMEM((rows, cols), BF16),
                pltpu.VMEM((16, cols), BF16),
                pltpu.VMEM((16, rows), BF16),
                pltpu.VMEM((width + 16, 2 * cols), BF16),
                pltpu.VMEM((cols, width), BF16),
                pltpu.VMEM((cols, width), BF16),
                pltpu.VMEM((2 * cols, rows // 2), BF16),
                pltpu.VMEM((cols, LANES), F32),
                pltpu.VMEM((row_tiles, LANES), F32),
                pltpu.VMEM((col_tiles, LANES), F32),
                pltpu.VMEM((col_tiles, LANES), F32),
                pltpu.VMEM((col_tiles, LANES), F32),
                pltpu.VMEM((col_tiles, LANES), F32),
                pltpu.VMEM((nx, col_tiles, LANES), F32),
                pltpu.VMEM((col_tiles, LANES), F32),
                pltpu.VMEM((row_tiles, LANES), F32),
                pltpu.VMEM((ny, row_tiles, LANES), F32),
                pltpu.VMEM((SWEEPS - 1, row_tiles, LANES), BF16),
                pltpu.VMEM((SWEEPS - 1, ny, row_tiles, LANES), BF16),
                pltpu.VMEM((SWEEPS, col_tiles, LANES), F32),
                pltpu.VMEM((SWEEPS, nx, col_tiles, LANES), F32),
                pltpu.VMEM((row_tiles, LANES), F32),
                pltpu.VMEM((col_tiles, LANES), F32),
                pltpu.VMEM((ny // 2, width + 16, LANES), BF16),
                pltpu.VMEM((2, ny // 2, width + 16, LANES), BF16),
                pltpu.VMEM((LANES, 2 * width), BF16),
                pltpu.VMEM((LANES, 2 * width), BF16),
                dma((5,)),
                dma((SWEEPS,)),
                dma((SWEEPS,)),
                dma((SWEEPS,)),
                dma((SWEEPS,)),
                dma((3,)),
                dma((2,)),
                dma((6,)),
                dma((6,)),
                dma((2,)),
            ],
            compiler_params=pltpu.CompilerParams(
                collective_id=0, has_side_effects=True, vmem_limit_bytes=44 * 1024 * 1024
            ),
        )(
            *(
                pltpu.with_memory_space_constraint(x.reshape(-1, width), pltpu.HBM)
                for x in (queries, keys, values)
            )
        )
        w_columns = lax.dynamic_slice_in_dim(
            w_out, lax.axis_index("gz") * columns, columns, 1
        )
        return jnp.dot(heads, w_columns, preferred_element_type=F32).astype(BF16)

    return jax.shard_map(
        body,
        mesh=mesh,
        in_specs=(P("gz", "gx", None), P("gz", "gy", None), P("gz", "gy", None), P()),
        out_specs=P(("gx", "gy"), "gz"),
        check_vma=False,
    )
```

```python
import functools
import math

import jax
import jax.numpy as jnp
from jax import lax
from jax.experimental import pallas as pl
from jax.experimental.pallas import tpu as pltpu
from jax.sharding import PartitionSpec as P

SWEEPS = 3
LANES = 128
MESH = pl.DeviceIdType.MESH
F32 = jnp.float32
BF16 = jnp.bfloat16


def far_first(count):
    return sorted(range(count), key=lambda d: -min(d, count - d))


def in_pairs(combine, parts):
    while len(parts) > 1:
        joined = [combine(*parts[n : n + 2]) for n in range(0, len(parts) - 1, 2)]
        parts = joined + parts[len(parts) // 2 * 2 :]
    return parts[0]


def split_lhs(x):
    rows = jnp.broadcast_to(x, (16, x.shape[1]))
    hi = rows.astype(BF16).astype(F32)
    rest = rows - hi
    mid = rest.astype(BF16).astype(F32)
    lo = rest - mid
    at = lax.broadcasted_iota(jnp.int32, rows.shape, 0)
    parts = jnp.where(at == 0, hi, jnp.where(at == 1, mid, jnp.where(at == 2, lo, 0.0)))
    return parts.astype(BF16)


def kernel(
    sizes,
    q_hbm,
    k_hbm,
    v_hbm,
    out_ref,
    q_ref,
    k_ref,
    v_ref,
    k_parts,
    s_ref,
    f_ref,
    g_ref,
    lhs_row,
    lhs_col,
    val_lhs,
    k2_ref,
    v2_ref,
    pair_ref,
    wide_ref,
    row_log,
    log_send,
    log_recv,
    part_send,
    part_recv,
    side_recv,
    cmax_ref,
    row_send,
    row_recv,
    sum_send,
    sum_recv,
    col_send,
    col_recv,
    row_vec,
    col_vec,
    out_send,
    out_recv,
    head_send,
    head_recv,
    load_sem,
    row_ssem,
    row_rsem,
    col_ssem,
    col_rsem,
    out_sem,
    head_sem,
    pair_ssem,
    pair_rsem,
    side_sem,
):
    nx, ny = sizes
    rows, width = q_ref.shape
    cols = k_ref.shape[0]
    row_tiles, col_tiles = rows // LANES, cols // LANES
    nz = ny // 2
    gz, gx, gy = lax.axis_index("gz"), lax.axis_index("gx"), lax.axis_index("gy")
    z, xl = gy // 2, lax.rem(gy, 2)
    y, xh = gx // 2, lax.rem(gx, 2)
    scale = math.log2(math.e) / math.sqrt(width)

    row_peers = [(dz, dx) for dz in far_first(nz) for dx in (1, 0) if (dz, dx) != (0, 0)]
    col_peers = [(dy, dx) for dy in far_first(nx // 2) for dx in (1, 0) if (dy, dx) != (0, 0)]

    def row_peer(dz, dx):
        return lax.rem(z + dz, nz) * 2 + lax.rem(xl + dx, 2)

    def col_peer(dy, dx):
        return lax.rem(y + dy, nx // 2) * 2 + lax.rem(xh + dx, 2)

    loads = [
        pltpu.make_async_copy(q_hbm, q_ref, load_sem.at[0]),
        pltpu.make_async_copy(k_hbm, k_parts.at[:, pl.ds(0, width)], load_sem.at[1]),
        pltpu.make_async_copy(v_hbm, v_ref, load_sem.at[2]),
        pltpu.make_async_copy(k_hbm, k_parts.at[:, pl.ds(width, width)], load_sem.at[3]),
        pltpu.make_async_copy(k_hbm, k_ref, load_sem.at[4]),
    ]
    for n in (1, 3, 0, 4, 2):
        loads[n].start()

    barrier = pltpu.get_barrier_semaphore()
    for dz, dx in row_peers:
        pl.semaphore_signal(
            barrier, inc=1, device_id={"gy": row_peer(dz, dx)}, device_id_type=MESH
        )
    for dy, dx in col_peers:
        pl.semaphore_signal(
            barrier, inc=1, device_id={"gx": col_peer(dy, dx)}, device_id_type=MESH
        )
    pl.semaphore_signal(barrier, inc=1, device_id={"gz": 1 - gz}, device_id_type=MESH)
    beside = z * 2 + 1 - xl
    for dy, dx in col_peers:
        pl.semaphore_signal(
            barrier,
            inc=1,
            device_id={"gx": col_peer(dy, dx), "gy": beside},
            device_id_type=MESH,
        )

    def send_all(source, target, ssem, rsem, peers):
        for slot, device in peers:
            pltpu.make_async_remote_copy(
                src_ref=source,
                dst_ref=target.at[slot],
                send_sem=ssem,
                recv_sem=rsem,
                device_id=device,
                device_id_type=MESH,
            ).start()

    def wait_all(target, sem):
        everything = target.at[pl.ds(1, target.shape[0] - 1)]
        pltpu.make_async_copy(everything, everything, sem).wait()

    row_to = [(dz * 2 + dx, {"gy": row_peer(dz, dx)}) for dz, dx in row_peers]
    col_to = [(dy * 2 + dx, {"gx": col_peer(dy, dx)}) for dy, dx in col_peers]
    side_to = [
        (dy * 2 + dx, {"gx": col_peer(dy, dx), "gy": beside}) for dy, dx in [*col_peers, (0, 0)]
    ]

    def to_pair(source, target, number):
        return pltpu.make_async_remote_copy(
            src_ref=source,
            dst_ref=target,
            send_sem=pair_ssem.at[number],
            recv_sem=pair_rsem.at[number],
            device_id={"gy": beside},
            device_id_type=MESH,
        )

    half = cols // 2
    halves = [pl.ds(0, half), pl.ds(half, half)]
    pair_keys = [to_pair(k_ref.at[h], k2_ref.at[h], n) for n, h in enumerate(halves)]
    pair_values = [to_pair(v_ref.at[h], v2_ref.at[h], 2 + n) for n, h in enumerate(halves)]
    pair_log = to_pair(log_send, log_recv, 4)
    pair_part = to_pair(part_send, part_recv, 5)

    def ranked(n):
        return jnp.where(n < nz // 2, n, nz + nz // 2 - 1 - n)

    targets = [ranked(jnp.where(n >= ranked(z), n + 1, n)) for n in range(nz - 1)] + [z]

    def log_total(own, received):
        biggest = in_pairs(jnp.maximum, [own, *received])
        return biggest + jnp.log2(in_pairs(jnp.add, [jnp.exp2(x - biggest) for x in [own, *received]]))

    def plain_total(own, received):
        return in_pairs(jnp.add, [own, *received])

    loads[1].wait()
    loads[3].wait()
    loads[0].wait()

    def scaled_parts(x):
        scaled = scale * x.astype(F32)
        high = scaled.astype(BF16)
        return jnp.concatenate([high, (scaled - high.astype(F32)).astype(BF16)], axis=1)

    block = 2 * LANES
    for b in range(rows // block):
        lanes = slice(b * block, (b + 1) * block)
        scores = lax.dot_general(
            k_parts[...],
            scaled_parts(q_ref[lanes, :]),
            (((1,), (1,)), ((), ())),
            preferred_element_type=F32,
        )
        s_ref[:, lanes] = scores
        tops, sums = [], []
        for jb in range(col_tiles):
            part = scores[jb * LANES : (jb + 1) * LANES].reshape(LANES // 8, 8, block)
            top = jnp.max(part, axis=0)
            tops.append(top)
            sums.append(jnp.sum(jnp.exp2(part - top[None]), axis=0))
        biggest = in_pairs(jnp.maximum, tops)
        summed = in_pairs(
            jnp.add, [total * jnp.exp2(top - biggest) for top, total in zip(tops, sums)]
        )
        top = jnp.max(biggest, axis=0, keepdims=True)
        summed = jnp.sum(summed * jnp.exp2(biggest - top), axis=0, keepdims=True)
        local = top + jnp.log2(summed)
        for t in range(block // LANES):
            row_send[pl.ds(b * (block // LANES) + t, 1), :] = local[:, t * LANES : (t + 1) * LANES]

    pl.semaphore_wait(barrier, len(row_peers) + 2 * len(col_peers) + 1)
    send_all(row_send, row_recv, row_ssem.at[0], row_rsem.at[0], row_to)
    loads[4].wait()
    pair_keys[0].start()
    loads[2].wait()
    wait_all(row_recv, row_rsem.at[0])
    row_log[...] = -log_total(row_send[...], [row_recv[slot] for slot in range(1, ny)])

    eye = lax.broadcasted_iota(jnp.int32, (LANES, LANES), 0) == lax.broadcasted_iota(
        jnp.int32, (LANES, LANES), 1
    )

    def across(column):
        return jnp.sum(
            jnp.where(eye, jnp.broadcast_to(column, (LANES, LANES)), 0.0), axis=0, keepdims=True
        )

    tiles = [slice(t * LANES, (t + 1) * LANES) for t in range(row_tiles)]
    for jb in range(col_tiles):
        down = slice(jb * LANES, (jb + 1) * LANES)
        biggest = None
        for t in range(row_tiles):
            shifted = s_ref[down, tiles[t]] + row_log[t : t + 1, :]
            s_ref[down, tiles[t]] = shifted
            biggest = shifted if biggest is None else jnp.maximum(biggest, shifted)
        biggest = jnp.max(biggest, axis=1, keepdims=True)
        wide = jnp.broadcast_to(biggest, (LANES, LANES))
        summed = jnp.zeros((LANES, LANES), F32)
        for t in range(row_tiles):
            part = jnp.exp2(s_ref[down, tiles[t]] - wide)
            f_ref[down, tiles[t]] = part.astype(BF16)
            summed = summed + part
        summed = jnp.sum(summed, axis=1, keepdims=True)
        cmax_ref[pl.ds(jb, 1), :] = across(biggest)
        col_send[0, pl.ds(jb, 1), :] = across(biggest + jnp.log2(summed))

    send_all(col_send.at[0], col_recv.at[0], col_ssem.at[0], col_rsem.at[0], col_to)
    pair_keys[1].start()
    for t in range(col_tiles):
        down = slice(t * LANES, (t + 1) * LANES)
        val_lhs[0:width, down] = v_ref[down, :].astype(F32).T.astype(BF16)
        for i in range(row_tiles):
            g_ref[tiles[i], down] = f_ref[down, tiles[i]].T
    wait_all(col_recv.at[0], col_rsem.at[0])
    total = log_total(col_send[0], [col_recv[0, slot] for slot in range(1, nx)])
    log_send[...] = -total
    pair_log.start()
    col_vec[...] = jnp.exp2(cmax_ref[...] - total)

    def for_pair():
        pair_keys[0].wait_recv()
        pair_keys[1].wait_recv()
        k_parts[:, 0:width] = k2_ref[...]
        k_parts[:, width:] = k2_ref[...]
        pair_log.wait_recv()
        for t in range(col_tiles):
            line = jnp.broadcast_to(log_recv[t : t + 1, :], (LANES, LANES))
            column = jnp.sum(jnp.where(eye, line, 0.0), axis=1, keepdims=True)
            wide_ref[t * LANES : (t + 1) * LANES, :] = jnp.broadcast_to(column, (LANES, LANES))
        for m in range(nz // 2):
            chunks = [to * 2 + xl for to in targets[2 * m : 2 * m + 2]]
            q_block = jnp.concatenate(
                [q_ref[pl.ds(pl.multiple_of(c * LANES, LANES), LANES), :] for c in chunks], axis=0
            )
            scores = lax.dot_general(
                k_parts[...],
                scaled_parts(q_block),
                (((1,), (1,)), ((), ())),
                preferred_element_type=F32,
            )
            for n, c in enumerate(chunks):
                across_lanes = slice((2 * m + n) * LANES, (2 * m + n + 1) * LANES)
                part = scores[:, n * LANES : (n + 1) * LANES] + wide_ref[...]
                pair_ref[cols:, across_lanes] = jnp.exp2(part + row_log[pl.ds(c, 1), :]).astype(BF16)

    def values_of_pair():
        pair_values[0].wait_recv()
        pair_values[1].wait_recv()
        for t in range(col_tiles):
            down = slice(t * LANES, (t + 1) * LANES)
            val_lhs[0:width, cols + t * LANES : cols + (t + 1) * LANES] = (
                v2_ref[down, :].astype(F32).T.astype(BF16)
            )

    def own_half():
        for n, to in enumerate(targets):
            c = to * 2 + xl
            pair_ref[0:cols, n * LANES : (n + 1) * LANES] = f_ref[
                :, pl.ds(pl.multiple_of(c * LANES, LANES), LANES)
            ]

    def row_step(turn):
        for t in range(col_tiles):
            lhs_row[:, t * LANES : (t + 1) * LANES] = split_lhs(col_vec[t : t + 1, :])
        sums = jnp.sum(
            lax.dot_general(
                lhs_row[...], f_ref[...], (((1,), (0,)), ((), ())), preferred_element_type=F32
            ),
            axis=0,
            keepdims=True,
        )
        for t in range(row_tiles):
            row_vec[pl.ds(t, 1), :] = sums[:, t * LANES : (t + 1) * LANES]
        own = row_vec[...].astype(BF16)
        sum_send[turn - 1] = own
        send_all(
            sum_send.at[turn - 1], sum_recv.at[turn - 1], row_ssem.at[turn], row_rsem.at[turn], row_to
        )
        if turn == 1:
            pair_values[0].start()
            for_pair()
        else:
            values_of_pair()
        wait_all(sum_recv.at[turn - 1], row_rsem.at[turn])
        row_vec[...] = 1.0 / plain_total(
            own.astype(F32), [sum_recv[turn - 1, slot].astype(F32) for slot in range(1, ny)]
        )

    def col_step(turn):
        for t in range(row_tiles):
            lhs_col[:, t * LANES : (t + 1) * LANES] = split_lhs(row_vec[t : t + 1, :])
        sums = jnp.sum(
            lax.dot_general(
                lhs_col[...], g_ref[...], (((1,), (0,)), ((), ())), preferred_element_type=F32
            ),
            axis=0,
            keepdims=True,
        )
        for t in range(col_tiles):
            col_send[turn, pl.ds(t, 1), :] = (
                sums[:, t * LANES : (t + 1) * LANES] * col_vec[t : t + 1, :]
            )
        send_all(
            col_send.at[turn], col_recv.at[turn], col_ssem.at[turn], col_rsem.at[turn], col_to
        )
        if turn == 1:
            pair_values[1].start()
            own_half()
        if turn == SWEEPS - 1:
            send_all(col_send.at[turn], side_recv, side_sem.at[0], side_sem.at[1], side_to)
        wait_all(col_recv.at[turn], col_rsem.at[turn])
        inverse = 1.0 / plain_total(
            col_send[turn], [col_recv[turn, slot] for slot in range(1, nx)]
        )
        col_vec[...] = col_vec[...] * inverse
        if turn == 1:
            part_send[...] = inverse
            pair_part.start()

    for turn in range(1, SWEEPS):
        row_step(turn)
        col_step(turn)

    pltpu.make_async_copy(side_recv, side_recv, side_sem.at[1]).wait()
    pair_part.wait_recv()
    side = part_recv[...] / plain_total(side_recv[0], [side_recv[slot] for slot in range(1, nx)])
    for t in range(2 * col_tiles):
        lanes = slice(t * LANES, (t + 1) * LANES)
        if t < col_tiles:
            line = col_vec[t : t + 1, :]
        else:
            line = side[t - col_tiles : t - col_tiles + 1, :]
        val_lhs[0:width, lanes] = (val_lhs[0:width, lanes].astype(F32) * line).astype(BF16)
        val_lhs[width : width + 16, lanes] = split_lhs(line)
    tail = lax.broadcasted_iota(jnp.int32, (16, LANES), 0)

    def product(m):
        return jnp.dot(
            val_lhs[...],
            pair_ref[:, m * 2 * LANES : (m + 1) * 2 * LANES],
            preferred_element_type=F32,
        )

    ahead = product(0)
    for m in range(nz // 2):
        both = ahead
        if m + 1 < nz // 2:
            ahead = product(m + 1)
        for x in range(2):
            n = 2 * m + x
            piece = both[:, x * LANES : (x + 1) * LANES]
            out_send[n, 0:width, :] = piece[0:width].astype(BF16)
            weight = jnp.sum(piece[width:], axis=0, keepdims=True)
            high = weight.astype(BF16).astype(F32)
            out_send[n, width : width + 16, :] = jnp.where(
                tail == 0, high, jnp.where(tail == 1, weight - high, 0.0)
            ).astype(BF16)
            if n != nz - 1:
                pltpu.make_async_remote_copy(
                    src_ref=out_send.at[n],
                    dst_ref=out_recv.at[lax.rem(z - targets[n] + nz, nz)],
                    send_sem=out_sem.at[0],
                    recv_sem=out_sem.at[1],
                    device_id={"gy": targets[n] * 2 + xl},
                    device_id_type=MESH,
                ).start()
    wait_all(out_recv, out_sem.at[1])
    total = out_send[nz - 1].astype(F32)
    for slot in range(1, nz):
        total = total + out_recv[slot].astype(F32)
    weight = jnp.sum(total[width:], axis=0, keepdims=True)
    head = (total[0:width] / weight).T.astype(BF16)
    head_send[...] = head
    swap = pltpu.make_async_remote_copy(
        src_ref=head_send,
        dst_ref=head_recv,
        send_sem=head_sem.at[0],
        recv_sem=head_sem.at[1],
        device_id={"gz": 1 - gz},
        device_id_type=MESH,
    )
    swap.start()
    out_ref[:, pl.ds(pl.multiple_of(gz * width, width), width)] = head
    wait_all(row_recv, row_ssem.at[0])
    wait_all(col_recv.at[0], col_ssem.at[0])
    for turn in range(1, SWEEPS):
        wait_all(sum_recv.at[turn - 1], row_ssem.at[turn])
        wait_all(col_recv.at[turn], col_ssem.at[turn])
    wait_all(out_recv, out_sem.at[0])
    pltpu.make_async_copy(side_recv, side_recv, side_sem.at[0]).wait()
    for copy in [*pair_keys, *pair_values, pair_log, pair_part]:
        copy.wait_send()
    swap.wait()
    out_ref[:, pl.ds(pl.multiple_of((1 - gz) * width, width), width)] = head_recv[...]


def solution(mesh):
    nx, ny = mesh.shape["gx"], mesh.shape["gy"]

    def body(queries, keys, values, w_out):
        _, rows, width = queries.shape
        cols = keys.shape[1]
        columns = w_out.shape[1] // lax.axis_size("gz")
        row_tiles, col_tiles = rows // LANES, cols // LANES
        anywhere = pl.BlockSpec(memory_space=pltpu.HBM)
        dma = pltpu.SemaphoreType.DMA
        heads = pl.pallas_call(
            functools.partial(kernel, (nx, ny)),
            out_shape=jax.ShapeDtypeStruct((rows // ny, 2 * width), BF16),
            in_specs=[anywhere] * 3,
            out_specs=pl.BlockSpec(memory_space=pltpu.VMEM),
            scratch_shapes=[
                pltpu.VMEM((rows, width), BF16),
                pltpu.VMEM((cols, width), BF16),
                pltpu.VMEM((cols, width), BF16),
                pltpu.VMEM((cols, 2 * width), BF16),
                pltpu.VMEM((cols, rows), F32),
                pltpu.VMEM((cols, rows), BF16),
                pltpu.VMEM((rows, cols), BF16),
                pltpu.VMEM((16, cols), BF16),
                pltpu.VMEM((16, rows), BF16),
                pltpu.VMEM((width + 16, 2 * cols), BF16),
                pltpu.VMEM((cols, width), BF16),
                pltpu.VMEM((cols, width), BF16),
                pltpu.VMEM((2 * cols, rows // 2), BF16),
                pltpu.VMEM((cols, LANES), F32),
                pltpu.VMEM((row_tiles, LANES), F32),
                pltpu.VMEM((col_tiles, LANES), F32),
                pltpu.VMEM((col_tiles, LANES), F32),
                pltpu.VMEM((col_tiles, LANES), F32),
                pltpu.VMEM((col_tiles, LANES), F32),
                pltpu.VMEM((nx, col_tiles, LANES), F32),
                pltpu.VMEM((col_tiles, LANES), F32),
                pltpu.VMEM((row_tiles, LANES), F32),
                pltpu.VMEM((ny, row_tiles, LANES), F32),
                pltpu.VMEM((SWEEPS - 1, row_tiles, LANES), BF16),
                pltpu.VMEM((SWEEPS - 1, ny, row_tiles, LANES), BF16),
                pltpu.VMEM((SWEEPS, col_tiles, LANES), F32),
                pltpu.VMEM((SWEEPS, nx, col_tiles, LANES), F32),
                pltpu.VMEM((row_tiles, LANES), F32),
                pltpu.VMEM((col_tiles, LANES), F32),
                pltpu.VMEM((ny // 2, width + 16, LANES), BF16),
                pltpu.VMEM((ny // 2, width + 16, LANES), BF16),
                pltpu.VMEM((LANES, width), BF16),
                pltpu.VMEM((LANES, width), BF16),
                dma((5,)),
                dma((SWEEPS,)),
                dma((SWEEPS,)),
                dma((SWEEPS,)),
                dma((SWEEPS,)),
                dma((2,)),
                dma((2,)),
                dma((6,)),
                dma((6,)),
                dma((2,)),
            ],
            compiler_params=pltpu.CompilerParams(
                collective_id=0, has_side_effects=True, vmem_limit_bytes=44 * 1024 * 1024
            ),
        )(
            *(
                pltpu.with_memory_space_constraint(x.reshape(-1, width), pltpu.HBM)
                for x in (queries, keys, values)
            )
        )
        w_columns = lax.dynamic_slice_in_dim(
            w_out, lax.axis_index("gz") * columns, columns, 1
        )
        return jnp.dot(heads, w_columns, preferred_element_type=F32).astype(BF16)

    return jax.shard_map(
        body,
        mesh=mesh,
        in_specs=(P("gz", "gx", None), P("gz", "gy", None), P("gz", "gy", None), P()),
        out_specs=P(("gx", "gy"), "gz"),
        check_vma=False,
    )
```

```python
import functools
import math

import jax
import jax.numpy as jnp
from jax import lax
from jax.experimental import pallas as pl
from jax.experimental.pallas import tpu as pltpu
from jax.sharding import PartitionSpec as P

SWEEPS = 3
LANES = 128
MESH = pl.DeviceIdType.MESH
F32 = jnp.float32
BF16 = jnp.bfloat16


def far_first(count):
    return sorted(range(count), key=lambda d: -min(d, count - d))


def split_lhs(x):
    rows = jnp.broadcast_to(x, (16, x.shape[1]))
    hi = rows.astype(BF16).astype(F32)
    rest = rows - hi
    mid = rest.astype(BF16).astype(F32)
    lo = rest - mid
    at = lax.broadcasted_iota(jnp.int32, rows.shape, 0)
    parts = jnp.where(at == 0, hi, jnp.where(at == 1, mid, jnp.where(at == 2, lo, 0.0)))
    return parts.astype(BF16)


def kernel(
    sizes,
    q_hbm,
    k_hbm,
    v_hbm,
    out_ref,
    q_ref,
    k_ref,
    v_ref,
    k_parts,
    s_ref,
    f_ref,
    g_ref,
    lhs_row,
    lhs_col,
    val_lhs,
    k2_ref,
    v2_ref,
    pair_ref,
    wide_ref,
    row_log,
    log_send,
    log_recv,
    part_send,
    part_recv,
    side_recv,
    cmax_ref,
    row_send,
    row_recv,
    sum_send,
    sum_recv,
    col_send,
    col_recv,
    row_vec,
    col_vec,
    out_send,
    out_recv,
    head_send,
    head_recv,
    load_sem,
    row_ssem,
    row_rsem,
    col_ssem,
    col_rsem,
    out_sem,
    head_sem,
    pair_ssem,
    pair_rsem,
    side_sem,
):
    nx, ny = sizes
    rows, width = q_ref.shape
    cols = k_ref.shape[0]
    row_tiles, col_tiles = rows // LANES, cols // LANES
    nz = ny // 2
    gz, gx, gy = lax.axis_index("gz"), lax.axis_index("gx"), lax.axis_index("gy")
    z, xl = gy // 2, lax.rem(gy, 2)
    y, xh = gx // 2, lax.rem(gx, 2)
    scale = math.log2(math.e) / math.sqrt(width)

    row_peers = [(dz, dx) for dz in far_first(nz) for dx in (1, 0) if (dz, dx) != (0, 0)]
    col_peers = [(dy, dx) for dy in far_first(nx // 2) for dx in (1, 0) if (dy, dx) != (0, 0)]

    def row_peer(dz, dx):
        return lax.rem(z + dz, nz) * 2 + lax.rem(xl + dx, 2)

    def col_peer(dy, dx):
        return lax.rem(y + dy, nx // 2) * 2 + lax.rem(xh + dx, 2)

    loads = [
        pltpu.make_async_copy(q_hbm, q_ref, load_sem.at[0]),
        pltpu.make_async_copy(k_hbm, k_parts.at[:, pl.ds(0, width)], load_sem.at[1]),
        pltpu.make_async_copy(v_hbm, v_ref, load_sem.at[2]),
        pltpu.make_async_copy(k_hbm, k_parts.at[:, pl.ds(width, width)], load_sem.at[3]),
        pltpu.make_async_copy(k_hbm, k_ref, load_sem.at[4]),
    ]
    for n in (1, 3, 0, 4, 2):
        loads[n].start()

    barrier = pltpu.get_barrier_semaphore()
    for dz, dx in row_peers:
        pl.semaphore_signal(
            barrier, inc=1, device_id={"gy": row_peer(dz, dx)}, device_id_type=MESH
        )
    for dy, dx in col_peers:
        pl.semaphore_signal(
            barrier, inc=1, device_id={"gx": col_peer(dy, dx)}, device_id_type=MESH
        )
    pl.semaphore_signal(barrier, inc=1, device_id={"gz": 1 - gz}, device_id_type=MESH)
    beside = z * 2 + 1 - xl
    for dy, dx in col_peers:
        pl.semaphore_signal(
            barrier,
            inc=1,
            device_id={"gx": col_peer(dy, dx), "gy": beside},
            device_id_type=MESH,
        )

    def send_all(source, target, ssem, rsem, peers):
        for slot, device in peers:
            pltpu.make_async_remote_copy(
                src_ref=source,
                dst_ref=target.at[slot],
                send_sem=ssem,
                recv_sem=rsem,
                device_id=device,
                device_id_type=MESH,
            ).start()

    def wait_all(target, sem):
        everything = target.at[pl.ds(1, target.shape[0] - 1)]
        pltpu.make_async_copy(everything, everything, sem).wait()

    row_to = [(dz * 2 + dx, {"gy": row_peer(dz, dx)}) for dz, dx in row_peers]
    col_to = [(dy * 2 + dx, {"gx": col_peer(dy, dx)}) for dy, dx in col_peers]
    side_to = [
        (dy * 2 + dx, {"gx": col_peer(dy, dx), "gy": beside}) for dy, dx in [*col_peers, (0, 0)]
    ]

    def to_pair(source, target, number):
        return pltpu.make_async_remote_copy(
            src_ref=source,
            dst_ref=target,
            send_sem=pair_ssem.at[number],
            recv_sem=pair_rsem.at[number],
            device_id={"gy": beside},
            device_id_type=MESH,
        )

    half = cols // 2
    halves = [pl.ds(0, half), pl.ds(half, half)]
    pair_keys = [to_pair(k_ref.at[h], k2_ref.at[h], n) for n, h in enumerate(halves)]
    pair_values = [to_pair(v_ref.at[h], v2_ref.at[h], 2 + n) for n, h in enumerate(halves)]
    pair_log = to_pair(log_send, log_recv, 4)
    pair_part = to_pair(part_send, part_recv, 5)

    def ranked(n):
        return jnp.where(n < nz // 2, n, nz + nz // 2 - 1 - n)

    targets = [ranked(jnp.where(n >= ranked(z), n + 1, n)) for n in range(nz - 1)] + [z]

    def log_total(own, received):
        biggest = own
        for other in received:
            biggest = jnp.maximum(biggest, other)
        total = jnp.exp2(own - biggest)
        for other in received:
            total = total + jnp.exp2(other - biggest)
        return biggest + jnp.log2(total)

    def plain_total(own, received):
        total = own
        for other in received:
            total = total + other
        return total

    loads[1].wait()
    loads[3].wait()
    loads[0].wait()

    def scaled_parts(x):
        scaled = scale * x.astype(F32)
        high = scaled.astype(BF16)
        return jnp.concatenate([high, (scaled - high.astype(F32)).astype(BF16)], axis=1)

    block = 2 * LANES
    for b in range(rows // block):
        lanes = slice(b * block, (b + 1) * block)
        scores = lax.dot_general(
            k_parts[...],
            scaled_parts(q_ref[lanes, :]),
            (((1,), (1,)), ((), ())),
            preferred_element_type=F32,
        )
        s_ref[:, lanes] = scores
        biggest, summed = None, None
        for jb in range(col_tiles):
            part = scores[jb * LANES : (jb + 1) * LANES].reshape(LANES // 8, 8, block)
            top = jnp.max(part, axis=0)
            total = jnp.sum(jnp.exp2(part - top[None]), axis=0)
            if biggest is None:
                biggest, summed = top, total
            else:
                larger = jnp.maximum(biggest, top)
                summed = summed * jnp.exp2(biggest - larger) + total * jnp.exp2(top - larger)
                biggest = larger
        top = jnp.max(biggest, axis=0, keepdims=True)
        summed = jnp.sum(summed * jnp.exp2(biggest - top), axis=0, keepdims=True)
        local = top + jnp.log2(summed)
        for t in range(block // LANES):
            row_send[pl.ds(b * (block // LANES) + t, 1), :] = local[:, t * LANES : (t + 1) * LANES]

    pl.semaphore_wait(barrier, len(row_peers) + 2 * len(col_peers) + 1)
    send_all(row_send, row_recv, row_ssem.at[0], row_rsem.at[0], row_to)
    loads[4].wait()
    pair_keys[0].start()
    loads[2].wait()
    wait_all(row_recv, row_rsem.at[0])
    row_log[...] = -log_total(row_send[...], [row_recv[slot] for slot in range(1, ny)])

    eye = lax.broadcasted_iota(jnp.int32, (LANES, LANES), 0) == lax.broadcasted_iota(
        jnp.int32, (LANES, LANES), 1
    )

    def across(column):
        return jnp.sum(
            jnp.where(eye, jnp.broadcast_to(column, (LANES, LANES)), 0.0), axis=0, keepdims=True
        )

    tiles = [slice(t * LANES, (t + 1) * LANES) for t in range(row_tiles)]
    for jb in range(col_tiles):
        down = slice(jb * LANES, (jb + 1) * LANES)
        biggest = None
        for t in range(row_tiles):
            shifted = s_ref[down, tiles[t]] + row_log[t : t + 1, :]
            s_ref[down, tiles[t]] = shifted
            biggest = shifted if biggest is None else jnp.maximum(biggest, shifted)
        biggest = jnp.max(biggest, axis=1, keepdims=True)
        wide = jnp.broadcast_to(biggest, (LANES, LANES))
        summed = jnp.zeros((LANES, LANES), F32)
        for t in range(row_tiles):
            part = jnp.exp2(s_ref[down, tiles[t]] - wide)
            f_ref[down, tiles[t]] = part.astype(BF16)
            summed = summed + part
        summed = jnp.sum(summed, axis=1, keepdims=True)
        cmax_ref[pl.ds(jb, 1), :] = across(biggest)
        col_send[0, pl.ds(jb, 1), :] = across(biggest + jnp.log2(summed))

    send_all(col_send.at[0], col_recv.at[0], col_ssem.at[0], col_rsem.at[0], col_to)
    pair_keys[1].start()
    for t in range(col_tiles):
        down = slice(t * LANES, (t + 1) * LANES)
        val_lhs[0:width, down] = v_ref[down, :].astype(F32).T.astype(BF16)
        for i in range(row_tiles):
            g_ref[tiles[i], down] = f_ref[down, tiles[i]].T
    wait_all(col_recv.at[0], col_rsem.at[0])
    total = log_total(col_send[0], [col_recv[0, slot] for slot in range(1, nx)])
    log_send[...] = -total
    pair_log.start()
    col_vec[...] = jnp.exp2(cmax_ref[...] - total)

    def for_pair():
        pair_keys[0].wait_recv()
        pair_keys[1].wait_recv()
        k_parts[:, 0:width] = k2_ref[...]
        k_parts[:, width:] = k2_ref[...]
        pair_log.wait_recv()
        for t in range(col_tiles):
            line = jnp.broadcast_to(log_recv[t : t + 1, :], (LANES, LANES))
            column = jnp.sum(jnp.where(eye, line, 0.0), axis=1, keepdims=True)
            wide_ref[t * LANES : (t + 1) * LANES, :] = jnp.broadcast_to(column, (LANES, LANES))
        for m in range(nz // 2):
            chunks = [to * 2 + xl for to in targets[2 * m : 2 * m + 2]]
            q_block = jnp.concatenate(
                [q_ref[pl.ds(pl.multiple_of(c * LANES, LANES), LANES), :] for c in chunks], axis=0
            )
            scores = lax.dot_general(
                k_parts[...],
                scaled_parts(q_block),
                (((1,), (1,)), ((), ())),
                preferred_element_type=F32,
            )
            for n, c in enumerate(chunks):
                across_lanes = slice((2 * m + n) * LANES, (2 * m + n + 1) * LANES)
                part = scores[:, n * LANES : (n + 1) * LANES] + wide_ref[...]
                pair_ref[cols:, across_lanes] = jnp.exp2(part + row_log[pl.ds(c, 1), :]).astype(BF16)

    def values_of_pair():
        pair_values[0].wait_recv()
        pair_values[1].wait_recv()
        for t in range(col_tiles):
            down = slice(t * LANES, (t + 1) * LANES)
            val_lhs[0:width, cols + t * LANES : cols + (t + 1) * LANES] = (
                v2_ref[down, :].astype(F32).T.astype(BF16)
            )

    def own_half():
        for n, to in enumerate(targets):
            c = to * 2 + xl
            pair_ref[0:cols, n * LANES : (n + 1) * LANES] = f_ref[
                :, pl.ds(pl.multiple_of(c * LANES, LANES), LANES)
            ]

    def row_step(turn):
        for t in range(col_tiles):
            lhs_row[:, t * LANES : (t + 1) * LANES] = split_lhs(col_vec[t : t + 1, :])
        sums = jnp.sum(
            lax.dot_general(
                lhs_row[...], f_ref[...], (((1,), (0,)), ((), ())), preferred_element_type=F32
            ),
            axis=0,
            keepdims=True,
        )
        for t in range(row_tiles):
            row_vec[pl.ds(t, 1), :] = sums[:, t * LANES : (t + 1) * LANES]
        own = row_vec[...].astype(BF16)
        sum_send[turn - 1] = own
        send_all(
            sum_send.at[turn - 1], sum_recv.at[turn - 1], row_ssem.at[turn], row_rsem.at[turn], row_to
        )
        if turn == 1:
            pair_values[0].start()
            for_pair()
        else:
            values_of_pair()
        wait_all(sum_recv.at[turn - 1], row_rsem.at[turn])
        row_vec[...] = 1.0 / plain_total(
            own.astype(F32), [sum_recv[turn - 1, slot].astype(F32) for slot in range(1, ny)]
        )

    def col_step(turn):
        for t in range(row_tiles):
            lhs_col[:, t * LANES : (t + 1) * LANES] = split_lhs(row_vec[t : t + 1, :])
        sums = jnp.sum(
            lax.dot_general(
                lhs_col[...], g_ref[...], (((1,), (0,)), ((), ())), preferred_element_type=F32
            ),
            axis=0,
            keepdims=True,
        )
        for t in range(col_tiles):
            col_send[turn, pl.ds(t, 1), :] = (
                sums[:, t * LANES : (t + 1) * LANES] * col_vec[t : t + 1, :]
            )
        send_all(
            col_send.at[turn], col_recv.at[turn], col_ssem.at[turn], col_rsem.at[turn], col_to
        )
        if turn == 1:
            pair_values[1].start()
            own_half()
        if turn == SWEEPS - 1:
            send_all(col_send.at[turn], side_recv, side_sem.at[0], side_sem.at[1], side_to)
        wait_all(col_recv.at[turn], col_rsem.at[turn])
        inverse = 1.0 / plain_total(
            col_send[turn], [col_recv[turn, slot] for slot in range(1, nx)]
        )
        col_vec[...] = col_vec[...] * inverse
        if turn == 1:
            part_send[...] = inverse
            pair_part.start()

    for turn in range(1, SWEEPS):
        row_step(turn)
        col_step(turn)

    pltpu.make_async_copy(side_recv, side_recv, side_sem.at[1]).wait()
    pair_part.wait_recv()
    side = part_recv[...] / plain_total(side_recv[0], [side_recv[slot] for slot in range(1, nx)])
    for t in range(2 * col_tiles):
        lanes = slice(t * LANES, (t + 1) * LANES)
        if t < col_tiles:
            line = col_vec[t : t + 1, :]
        else:
            line = side[t - col_tiles : t - col_tiles + 1, :]
        rounded = line.astype(BF16)
        val_lhs[0:width, lanes] = val_lhs[0:width, lanes] * rounded
        val_lhs[width : width + 16, lanes] = split_lhs(rounded.astype(F32))
    tail = lax.broadcasted_iota(jnp.int32, (16, LANES), 0)

    def product(m):
        return jnp.dot(
            val_lhs[...],
            pair_ref[:, m * 2 * LANES : (m + 1) * 2 * LANES],
            preferred_element_type=F32,
        )

    ahead = product(0)
    for m in range(nz // 2):
        both = ahead
        if m + 1 < nz // 2:
            ahead = product(m + 1)
        for x in range(2):
            n = 2 * m + x
            piece = both[:, x * LANES : (x + 1) * LANES]
            out_send[n, 0:width, :] = piece[0:width].astype(BF16)
            weight = jnp.sum(piece[width:], axis=0, keepdims=True)
            high = weight.astype(BF16).astype(F32)
            out_send[n, width : width + 16, :] = jnp.where(
                tail == 0, high, jnp.where(tail == 1, weight - high, 0.0)
            ).astype(BF16)
            if n != nz - 1:
                pltpu.make_async_remote_copy(
                    src_ref=out_send.at[n],
                    dst_ref=out_recv.at[lax.rem(z - targets[n] + nz, nz)],
                    send_sem=out_sem.at[0],
                    recv_sem=out_sem.at[1],
                    device_id={"gy": targets[n] * 2 + xl},
                    device_id_type=MESH,
                ).start()
    wait_all(out_recv, out_sem.at[1])
    total = out_send[nz - 1].astype(F32)
    for slot in range(1, nz):
        total = total + out_recv[slot].astype(F32)
    weight = jnp.sum(total[width:], axis=0, keepdims=True)
    head = (total[0:width] / weight).T.astype(BF16)
    head_send[...] = head
    swap = pltpu.make_async_remote_copy(
        src_ref=head_send,
        dst_ref=head_recv,
        send_sem=head_sem.at[0],
        recv_sem=head_sem.at[1],
        device_id={"gz": 1 - gz},
        device_id_type=MESH,
    )
    swap.start()
    out_ref[:, pl.ds(pl.multiple_of(gz * width, width), width)] = head
    wait_all(row_recv, row_ssem.at[0])
    wait_all(col_recv.at[0], col_ssem.at[0])
    for turn in range(1, SWEEPS):
        wait_all(sum_recv.at[turn - 1], row_ssem.at[turn])
        wait_all(col_recv.at[turn], col_ssem.at[turn])
    wait_all(out_recv, out_sem.at[0])
    pltpu.make_async_copy(side_recv, side_recv, side_sem.at[0]).wait()
    for copy in [*pair_keys, *pair_values, pair_log, pair_part]:
        copy.wait_send()
    swap.wait()
    out_ref[:, pl.ds(pl.multiple_of((1 - gz) * width, width), width)] = head_recv[...]


def solution(mesh):
    nx, ny = mesh.shape["gx"], mesh.shape["gy"]

    def body(queries, keys, values, w_out):
        _, rows, width = queries.shape
        cols = keys.shape[1]
        columns = w_out.shape[1] // lax.axis_size("gz")
        row_tiles, col_tiles = rows // LANES, cols // LANES
        anywhere = pl.BlockSpec(memory_space=pltpu.HBM)
        dma = pltpu.SemaphoreType.DMA
        heads = pl.pallas_call(
            functools.partial(kernel, (nx, ny)),
            out_shape=jax.ShapeDtypeStruct((rows // ny, 2 * width), BF16),
            in_specs=[anywhere] * 3,
            out_specs=pl.BlockSpec(memory_space=pltpu.VMEM),
            scratch_shapes=[
                pltpu.VMEM((rows, width), BF16),
                pltpu.VMEM((cols, width), BF16),
                pltpu.VMEM((cols, width), BF16),
                pltpu.VMEM((cols, 2 * width), BF16),
                pltpu.VMEM((cols, rows), F32),
                pltpu.VMEM((cols, rows), BF16),
                pltpu.VMEM((rows, cols), BF16),
                pltpu.VMEM((16, cols), BF16),
                pltpu.VMEM((16, rows), BF16),
                pltpu.VMEM((width + 16, 2 * cols), BF16),
                pltpu.VMEM((cols, width), BF16),
                pltpu.VMEM((cols, width), BF16),
                pltpu.VMEM((2 * cols, rows // 2), BF16),
                pltpu.VMEM((cols, LANES), F32),
                pltpu.VMEM((row_tiles, LANES), F32),
                pltpu.VMEM((col_tiles, LANES), F32),
                pltpu.VMEM((col_tiles, LANES), F32),
                pltpu.VMEM((col_tiles, LANES), F32),
                pltpu.VMEM((col_tiles, LANES), F32),
                pltpu.VMEM((nx, col_tiles, LANES), F32),
                pltpu.VMEM((col_tiles, LANES), F32),
                pltpu.VMEM((row_tiles, LANES), F32),
                pltpu.VMEM((ny, row_tiles, LANES), F32),
                pltpu.VMEM((SWEEPS - 1, row_tiles, LANES), BF16),
                pltpu.VMEM((SWEEPS - 1, ny, row_tiles, LANES), BF16),
                pltpu.VMEM((SWEEPS, col_tiles, LANES), F32),
                pltpu.VMEM((SWEEPS, nx, col_tiles, LANES), F32),
                pltpu.VMEM((row_tiles, LANES), F32),
                pltpu.VMEM((col_tiles, LANES), F32),
                pltpu.VMEM((ny // 2, width + 16, LANES), BF16),
                pltpu.VMEM((ny // 2, width + 16, LANES), BF16),
                pltpu.VMEM((LANES, width), BF16),
                pltpu.VMEM((LANES, width), BF16),
                dma((5,)),
                dma((SWEEPS,)),
                dma((SWEEPS,)),
                dma((SWEEPS,)),
                dma((SWEEPS,)),
                dma((2,)),
                dma((2,)),
                dma((6,)),
                dma((6,)),
                dma((2,)),
            ],
            compiler_params=pltpu.CompilerParams(
                collective_id=0, has_side_effects=True, vmem_limit_bytes=44 * 1024 * 1024
            ),
        )(
            *(
                pltpu.with_memory_space_constraint(x.reshape(-1, width), pltpu.HBM)
                for x in (queries, keys, values)
            )
        )
        w_columns = lax.dynamic_slice_in_dim(
            w_out, lax.axis_index("gz") * columns, columns, 1
        )
        return jnp.dot(heads, w_columns, preferred_element_type=F32).astype(BF16)

    return jax.shard_map(
        body,
        mesh=mesh,
        in_specs=(P("gz", "gx", None), P("gz", "gy", None), P("gz", "gy", None), P()),
        out_specs=P(("gx", "gy"), "gz"),
        check_vma=False,
    )
```
